32 devices in a mesh: slab: 8 (over y, x, core), cross: 4 (over z).
Axes of the slice: x: 2, y: 2, z: 4, core: 2. Of those that a mesh axis runs over, the one named last changes fastest.
Arguments:
- populations: float32 [19, 32, 32, 128], P(None, 'slab', 'cross'), may hold values from 0 to 1, as said below
- fluid_mask: int32 [32, 32, 128], P('slab', 'cross'), may hold values 0 or 1
- relaxation: float32 [32, 32, 128], P('slab', 'cross'), may hold values from 0.8 to 1.7
- positions: int32 [3, 128, 642], P(None, 'slab'), may hold values from -1 to 127, as said below
- triangles: int32 [3, 1280], replicated, may hold values from 0 to 641, as said below
- tension: float32 [128, 1280], P('slab'), may hold values from 0.0003 to 0.003
- coarse_moments: float32 [4, 4096], P(None, 'slab'), may hold values from -0.2 to 1.2, as said below
- interface: int32 [3, 4096], P(None, ('slab', 'cross')), may hold values from -1 to 4095, as said below
Outputs:
- populations_next: float32 [19, 32, 32, 128], P(None, 'slab', 'cross')
- flow: float32 [3, 32, 32, 128], P(None, 'slab', 'cross')
The draws below stay inside these ranges and needn't reach their ends.
Inputs may be any that keep to these rules, and one draw needn't show every extreme that they name: `positions`: nodes of membrane m lie in planes 4 * (m // 16) - 1 to 4 * (m // 16) + 4, columns 0 to 31 and rows 0 to 127. `triangles`: each triangle names three different nodes of a membrane. `interface`: in each block of 128 columns (one device's, slab major), row 0 names different cells of that device's block, numbered (plane * 8 + column) * 128 + row, or -1 for an unused slot; rows 1 and 2 name coarse cells. `populations`: populations are positive. `coarse_moments`: row 0 is a positive density, rows 1 to 3 a velocity.
All inputs are finite; a program needn't handle non-finite values. No bound on the sum of `fluid_mask` on one device may be relied on, other than what follows from the above.
Results may differ from the reference program's by a relative error of at most 0.0001.
Values sent between devices are 32-bit elements; how exact they have to be, the bound alone decides.
A program may use at most 128 MiB of HBM per device.

```python
import math
import jax
import jax.numpy as jnp
import numpy as np
from jax import lax

PL = 4
SX = 8
NY = 128
MEMB_DEV = 16
MNODES = 642
MTRI = 1280
IF_DEV = 128
STEPS = 4
NZ = 32
NX = 32
MEMBS = 128
NCOARSE = 4096
IFACES = 4096


LATTICE_VECTORS = [(0, 0, 0), (1, 0, 0), (-1, 0, 0), (0, 1, 0), (0, -1, 0), (0, 0, 1), (0, 0, -1), (1, 1, 0), (-1, -1, 0), (1, -1, 0), (-1, 1, 0), (1, 0, 1), (-1, 0, -1), (1, 0, -1), (-1, 0, 1), (0, 1, 1), (0, -1, -1), (0, 1, -1), (0, -1, 1)]


LATTICE_WEIGHTS = [1.0 / 3.0] + [1.0 / 18.0] * 6 + [1.0 / 36.0] * 12


def equilibrium_draw(density, velocity):
    squared = velocity[0] * velocity[0] + velocity[1] * velocity[1] + velocity[2] * velocity[2]
    planes = []
    for member, vector in enumerate(LATTICE_VECTORS):
        projected = vector[0] * velocity[0] + vector[1] * velocity[1] + vector[2] * velocity[2]
        planes.append(LATTICE_WEIGHTS[member] * density * (1.0 + 3.0 * projected + 4.5 * projected * projected - 1.5 * squared))
    return jnp.stack(planes)


def draw_populations(key, part):
    subkeys = jax.random.split(jax.random.fold_in(key, 3), 3)
    grid = (NZ, NX, NY)
    density = jax.random.uniform(subkeys[0], grid, jnp.float32, 0.9, 1.1)
    velocity = jnp.clip(0.05 * jax.random.normal(subkeys[1], (3,) + grid, jnp.float32), -0.15, 0.15)
    spread = 0.1
    noise = jax.random.uniform(subkeys[2], (19,) + grid, jnp.float32, -1.0, 1.0)
    return equilibrium_draw(density, velocity) * (1.0 + spread * noise)


def draw_coarse_moments(key, part):
    subkeys = jax.random.split(jax.random.fold_in(key, 4), 2)
    density = jax.random.uniform(subkeys[0], (1, NCOARSE), jnp.float32, 0.9, 1.1)
    velocity = jnp.clip(0.05 * jax.random.normal(subkeys[1], (3, NCOARSE), jnp.float32), -0.15, 0.15)
    return jnp.concatenate([density, velocity], axis=0)


def draw_positions(key, part):
    subkeys = jax.random.split(jax.random.fold_in(key, 5), 5)
    membrane = jnp.arange(MEMBS, dtype=jnp.int32)[:, None]
    slab_owner = membrane // MEMB_DEV
    plane_ids = slab_owner * PL - 1 + jax.random.randint(subkeys[0], (MEMBS, MNODES), 0, PL + 2)
    centre_column = jax.random.randint(subkeys[1], (MEMBS, 1), 3, NX - 3)
    column_ids = jnp.clip(centre_column + jax.random.randint(subkeys[2], (MEMBS, MNODES), -3, 4), 0, NX - 1)
    centre_row = jax.random.randint(subkeys[3], (MEMBS, 1), 3, NY - 3)
    row_ids = centre_row + jax.random.randint(subkeys[4], (MEMBS, MNODES), -3, 4)
    return jnp.stack([plane_ids, column_ids, row_ids]).astype(jnp.int32)


def draw_triangles(key, part):
    subkeys = jax.random.split(jax.random.fold_in(key, 7), 3)
    vertex_one = jax.random.randint(subkeys[0], (MTRI,), 0, MNODES)
    step_one = jax.random.randint(subkeys[1], (MTRI,), 1, MNODES)
    step_two = jax.random.randint(subkeys[2], (MTRI,), 1, MNODES - 1)
    step_two = step_two + (step_two >= step_one).astype(jnp.int32)
    return jnp.stack([vertex_one, (vertex_one + step_one) % MNODES, (vertex_one + step_two) % MNODES]).astype(jnp.int32)


def draw_interface(key, part):
    subkeys = jax.random.split(jax.random.fold_in(key, 9), 5)
    devices = IFACES // IF_DEV
    cell_total = PL * SX * NY

    def choose_cells(device_key):
        return jax.random.permutation(device_key, cell_total)[:IF_DEV]
    chosen = jax.vmap(choose_cells)(jax.random.split(subkeys[0], devices))
    counts = jax.random.randint(subkeys[1], (devices,), max(IF_DEV // 4, 1), IF_DEV + 1)
    fullest = jax.random.randint(subkeys[2], (), 0, devices)
    counts = jnp.where(jnp.arange(devices, dtype=jnp.int32) == fullest, IF_DEV, counts)
    slots = jnp.arange(IF_DEV, dtype=jnp.int32)
    cell_ids = jnp.where(slots[None, :] < counts[:, None], chosen, -1).reshape(-1)
    coarse_one = jax.random.randint(subkeys[3], (IFACES,), 0, NCOARSE)
    coarse_two = jax.random.randint(subkeys[4], (IFACES,), 0, NCOARSE)
    return jnp.stack([cell_ids, coarse_one, coarse_two]).astype(jnp.int32)


def touch_ends(entries, stream_key, least, high):
    longest = entries.shape.index(max(entries.shape))
    spots = []
    for shift in (0, 1):
        where = [jax.random.randint(jax.random.fold_in(stream_key, axis), (), 0, length) for axis, length in enumerate(entries.shape)]
        where[longest] = (where[longest] + shift) % entries.shape[longest]
        spots.append(tuple(where))
    return entries.at[spots[0]].set(least).at[spots[1]].set(high)


def steps_of(rng, extent, shards, smallest, top_value):
    def one(axis_at, blocks):
        heights = jax.random.uniform(jax.random.fold_in(jax.random.fold_in(rng, 6), axis_at), (blocks,), jnp.float32, smallest / len(shards), top_value / len(shards))
        return jnp.repeat(jnp.exp(heights), extent[axis_at] // blocks).reshape((-1,) + (1,) * (len(extent) - axis_at - 1))

    gain = one(*shards[0])
    for cut in shards[1:]:
        gain = gain * one(*cut)
    return gain


def setup_inputs(seed: int = 0) -> dict:
    streams_of = jax.random.split(jax.random.key(seed), 9)
    populations = draw_populations(jax.random.fold_in(streams_of[8], 71), 0)
    fluid_mask = touch_ends((jax.random.randint(streams_of[1], (NZ, NX, NY), 0, 8) < 7).astype(jnp.int32), jax.random.fold_in(streams_of[1], 1), 0, 1)
    relaxation = jnp.clip(jnp.exp(math.log(1.7) - 0.75377182 * jax.random.uniform(streams_of[2], (NZ, NX, NY), jnp.float32) ** steps_of(streams_of[2], (NZ, NX, NY), ((0, 8), (1, 4)), -0.2, 0.2)), 0.8, 1.7)
    positions = draw_positions(jax.random.fold_in(streams_of[8], 71), 0)
    triangles = draw_triangles(jax.random.fold_in(streams_of[8], 71), 0)
    tension = jnp.clip(jnp.exp(math.log(0.003) - 2.3025851 * jax.random.uniform(streams_of[5], (MEMBS, MTRI), jnp.float32) ** steps_of(streams_of[5], (MEMBS, MTRI), ((0, 8),), -0.2, 0.2)), 0.0003, 0.003)
    coarse_moments = draw_coarse_moments(jax.random.fold_in(streams_of[8], 71), 0)
    interface = draw_interface(jax.random.fold_in(streams_of[8], 71), 0)
    return {"populations": populations, "fluid_mask": fluid_mask, "relaxation": relaxation, "positions": positions, "triangles": triangles, "tension": tension, "coarse_moments": coarse_moments, "interface": interface}


LATTICE_VECTORS = [(0, 0, 0), (1, 0, 0), (-1, 0, 0), (0, 1, 0), (0, -1, 0), (0, 0, 1), (0, 0, -1), (1, 1, 0), (-1, -1, 0), (1, -1, 0), (-1, 1, 0), (1, 0, 1), (-1, 0, -1), (1, 0, -1), (-1, 0, 1), (0, 1, 1), (0, -1, -1), (0, 1, -1), (0, -1, 1)]
LATTICE_WEIGHTS = [1.0 / 3.0] + [1.0 / 18.0] * 6 + [1.0 / 36.0] * 12
OPPOSITE = [0] + [member + 1 if member % 2 == 1 else member - 1 for member in range(1, 19)]
ROOT_THREE = math.sqrt(3.0)

def equilibrium(density, velocity):
    lattice = jnp.asarray(LATTICE_VECTORS, jnp.float32)
    weights = jnp.asarray(LATTICE_WEIGHTS, jnp.float32).reshape((19,) + (1,) * density.ndim)
    projected = jnp.einsum('qk,k...->q...', lattice, velocity, precision=lax.Precision.HIGHEST)
    squared = lax.optimization_barrier(jnp.sum(velocity * velocity, axis=0))
    return weights * density * (1.0 + 3.0 * projected + 4.5 * projected * projected - 1.5 * squared)

def moments(fields):
    lattice = jnp.asarray(LATTICE_VECTORS, jnp.float32)
    density = lax.optimization_barrier(jnp.sum(fields, axis=0))
    momentum = jnp.einsum('qk,q...->k...', lattice, fields, precision=lax.Precision.HIGHEST)
    return (density, momentum)

def collide(fields, body_force, relaxation, fluid_mask):
    density, momentum = moments(fields)
    shifted = momentum / density + body_force / (relaxation * density)
    relaxed = fields + relaxation * (equilibrium(density, shifted) - fields)
    reversed_fields = fields[np.array(OPPOSITE)]
    return jnp.where(fluid_mask[None] == 1, relaxed, reversed_fields)

def stream(padded, plane_count, column_count):
    wrapped = jnp.concatenate([padded[..., -1:], padded, padded[..., :1]], axis=-1)
    across = padded.shape[-1]
    planes = []
    for member, vector in enumerate(LATTICE_VECTORS):
        step_plane, step_column, step_row = vector
        planes.append(wrapped[member, 1 - step_plane:1 - step_plane + plane_count, 1 - step_column:1 - step_column + column_count, 1 - step_row:1 - step_row + across])
    return jnp.stack(planes)

def node_force(positions, triangles, tension):
    coords = positions.astype(jnp.float32)
    vertex_one = coords[:, :, triangles[0]]
    vertex_two = coords[:, :, triangles[1]]
    vertex_three = coords[:, :, triangles[2]]
    scaled = tension[None]
    running = jnp.zeros(coords.shape, jnp.float32)
    running = running.at[:, :, triangles[0]].add(scaled * (vertex_two + vertex_three - 2.0 * vertex_one))
    running = running.at[:, :, triangles[1]].add(scaled * (vertex_one + vertex_three - 2.0 * vertex_two))
    running = running.at[:, :, triangles[2]].add(scaled * (vertex_one + vertex_two - 2.0 * vertex_three))
    return running

def spread_global(positions, nodal_force):
    force_field = jnp.zeros((3, NZ + 4, NX + 2, NY), jnp.float32)
    kernel = (0.25, 0.5, 0.25)
    for offset_plane in (-1, 0, 1):
        for offset_column in (-1, 0, 1):
            for offset_row in (-1, 0, 1):
                weight = kernel[offset_plane + 1] * kernel[offset_column + 1] * kernel[offset_row + 1]
                plane_ids = positions[0] + 2 + offset_plane
                column_ids = positions[1] + 1 + offset_column
                row_ids = (positions[2] + offset_row) % NY
                force_field = force_field.at[:, plane_ids, column_ids, row_ids].add(weight * nodal_force)
    return force_field[:, 2:NZ + 2, 1:NX + 1]

def reference(populations, fluid_mask, relaxation, positions, triangles, tension, coarse_moments, interface):
    body_force = spread_global(positions, node_force(positions, triangles, tension))
    blended = 0.75 * coarse_moments[:, interface[1]] + 0.25 * coarse_moments[:, interface[2]]
    boundary = equilibrium(blended[0], blended[1:4])
    local_cell = interface[0]
    device = jnp.arange(IFACES, dtype=jnp.int32) // IF_DEV
    crosses = NX // SX
    slab_owner = device // crosses
    cross_owner = device % crosses
    plane_ids = slab_owner * PL + local_cell // (SX * NY)
    column_ids = cross_owner * SX + local_cell // NY % SX
    row_ids = local_cell % NY
    target = jnp.where(local_cell >= 0, (plane_ids * NX + column_ids) * NY + row_ids, NZ * NX * NY).astype(jnp.int32)
    fields = populations
    for iteration in range(STEPS):
        relaxed = collide(fields, body_force, relaxation, fluid_mask)
        padded = jnp.pad(relaxed, ((0, 0), (1, 1), (1, 1), (0, 0)))
        passed = stream(padded, NZ, NX)
        fields = passed.reshape(19, -1).at[:, target].set(boundary, mode='drop').reshape(passed.shape)
    density, momentum = moments(fields)
    return (fields, ROOT_THREE * momentum / density)
```

```python
import functools
import math

import jax
import jax.numpy as jnp
from jax import lax
from jax.experimental import pallas as pl
from jax.experimental.pallas import tpu as pltpu
from jax.sharding import PartitionSpec as P

STEPS = 4
MESH = pl.DeviceIdType.MESH
LATTICE_VECTORS = [
    (0, 0, 0),
    (1, 0, 0),
    (-1, 0, 0),
    (0, 1, 0),
    (0, -1, 0),
    (0, 0, 1),
    (0, 0, -1),
    (1, 1, 0),
    (-1, -1, 0),
    (1, -1, 0),
    (-1, 1, 0),
    (1, 0, 1),
    (-1, 0, -1),
    (1, 0, -1),
    (-1, 0, 1),
    (0, 1, 1),
    (0, -1, -1),
    (0, 1, -1),
    (0, -1, 1),
]
LATTICE_WEIGHTS = [1.0 / 3.0] + [1.0 / 18.0] * 6 + [1.0 / 36.0] * 12
OPPOSITE = [0] + [q + 1 if q % 2 == 1 else q - 1 for q in range(1, 19)]
ROOT_THREE = math.sqrt(3.0)
DIRECTIONS = [(1, 0), (-1, 0), (0, 1), (0, -1), (1, 1), (-1, -1), (1, -1), (-1, 1)]
NT = (((1,), (1,)), ((), ()))
F32, BF16, I32 = jnp.float32, jnp.bfloat16, jnp.int32


def round_up(value, unit):
    return (value + unit - 1) // unit * unit


def split(value, parts):
    pieces = []
    for _ in range(parts):
        piece = value.astype(BF16).astype(F32)
        pieces.append(piece)
        value = value - piece
    return pieces


def nodal_stage(plane_count, columns, rows, pos_ref, tri_ref, ten_ref, xs, inc, force):
    dims, membranes, nodes = pos_ref.shape
    padded = xs.shape[2]
    triangles = tri_ref.shape[1]
    slab = lax.axis_index("slab")
    cross = lax.axis_index("cross")

    xs[...] = jnp.zeros_like(xs)
    xs[0, :, :nodes] = (pos_ref[0] - slab * plane_count).astype(F32)
    xs[1, :, :nodes] = (pos_ref[1] - cross * columns).astype(F32)
    xs[2, :, :nodes] = (pos_ref[2] - rows // 2).astype(F32)

    corners = [tri_ref[pl.ds(corner, 1), :] for corner in range(3)]
    chunk = 128

    @pl.loop(0, padded // chunk)
    def _(i):
        ids = lax.broadcasted_iota(I32, (chunk, triangles), 0) + i * chunk
        hit = (ids == corners[0]) | (ids == corners[1]) | (ids == corners[2])
        inc[pl.ds(pl.multiple_of(i * chunk, chunk), chunk), :] = jnp.where(hit, 1.0, 0.0).astype(BF16)

    coords = xs[...].reshape(dims * membranes, padded)
    sums = jnp.dot(coords.astype(BF16), inc[...], preferred_element_type=F32)
    tension = ten_ref[...]
    terms = jnp.concatenate(
        [sums[k * membranes : (k + 1) * membranes] * tension for k in range(3)] + [tension], axis=0
    )
    stacked = jnp.concatenate(split(terms, 3), axis=0).astype(BF16)
    gathered = lax.dot_general(stacked, inc[...], NT, preferred_element_type=F32)
    count = terms.shape[0]
    total = gathered[:count] + (gathered[count : 2 * count] + gathered[2 * count :])
    weight = total[3 * membranes :]
    for k in range(3):
        force[k] = total[k * membranes : (k + 1) * membranes] - 3.0 * xs[k] * weight


def spread_stage(xs, force, acc, out_ref):
    _, membranes, padded = xs.shape
    _, planes, columns, rows = out_ref.shape
    plane_count = planes - 4
    half = (columns + 2) // 2
    cells = acc.shape[0] // 6
    acc[...] = jnp.zeros_like(acc)
    unroll = 4 if membranes % 4 == 0 else 1

    @pl.loop(0, membranes // unroll)
    def _(i):
        running = None
        for inner in range(unroll):
            m = pl.ds(i * unroll + inner, 1)
            plane = xs[0, m, :].astype(I32) + 1
            column = xs[1, m, :].astype(I32) + 1
            row = xs[2, m, :].astype(I32) + rows // 2
            inside = (column >= 0) & (column < 2 * half)
            upper = column >= half
            cell = plane * half + jnp.where(upper, column - half, column)
            cell = jnp.where(inside, cell, -1)
            lane = row + jnp.where(upper, rows, 0)
            mask = lax.broadcasted_iota(I32, (cells, padded), 0) == cell
            values = [split(force[k, m, :], 2) for k in range(3)]
            left = jnp.concatenate(
                [jnp.where(mask, values[k][part], 0.0) for part in range(2) for k in range(3)], axis=0
            ).astype(BF16)
            right = jnp.where(
                lax.broadcasted_iota(I32, (2 * rows, padded), 0) == lane, 1.0, 0.0
            ).astype(BF16)
            product = lax.dot_general(left, right, NT, preferred_element_type=F32)
            running = product if running is None else running + product
        acc[...] += running

    for k in range(3):
        value = acc[k * cells : (k + 1) * cells] + acc[(3 + k) * cells : (4 + k) * cells]
        halves = []
        for part in range(2):
            b = value[:, part * rows : (part + 1) * rows]
            halves.append(0.5 * b + 0.25 * (pltpu.roll(b, 1, 1) + pltpu.roll(b, rows - 1, 1)))
        smooth = []
        for p in range(plane_count + 2):
            b = jnp.concatenate([h[p * half : (p + 1) * half] for h in halves], axis=0)
            smooth.append(
                0.5 * b[1 : columns + 1] + 0.25 * (b[:columns] + b[2 : columns + 2])
            )
        for j in range(planes):
            total_plane = jnp.zeros((columns, rows), F32)
            for source, w in ((j - 2, 0.25), (j - 1, 0.5), (j, 0.25)):
                if 0 <= source < plane_count + 2:
                    total_plane = total_plane + w * smooth[source]
            out_ref[k, j] = total_plane


def equilibrium_pairs(density, velocity):
    squared = velocity[0] * velocity[0] + velocity[1] * velocity[1] + velocity[2] * velocity[2]
    base = 1.0 - 1.5 * squared
    result = [None] * 19
    result[0] = LATTICE_WEIGHTS[0] * density * base
    scaled = {w: w * density for w in (1.0 / 18.0, 1.0 / 36.0)}
    for q in range(1, 19, 2):
        projected = None
        for c, v in zip(LATTICE_VECTORS[q], velocity):
            if c == 0:
                continue
            if projected is None:
                projected = v if c == 1 else -v
            else:
                projected = projected + v if c == 1 else projected - v
        even = base + 4.5 * projected * projected
        odd = 3.0 * projected
        weight = scaled[LATTICE_WEIGHTS[q]]
        result[q] = weight * (even + odd)
        result[q + 1] = weight * (even - odd)
    return result


def moments_of(fields):
    density = functools.reduce(lambda a, b: a + b, fields)
    momentum = []
    for k in range(3):
        plus = [fields[q] for q in range(19) if LATTICE_VECTORS[q][k] == 1]
        minus = [fields[q] for q in range(19) if LATTICE_VECTORS[q][k] == -1]
        momentum.append(functools.reduce(lambda a, b: a + b, [a - b for a, b in zip(plus, minus)]))
    return density, momentum


def moving(dim, sign):
    return [q for q in range(19) if LATTICE_VECTORS[q][dim] == sign]


def lattice_kernel(
    slabs, crosses,
    tri_hbm, pos_hbm, ten_hbm, coarse_hbm, face_hbm, relax_hbm, fluid_hbm, pop_hbm,
    next_ref,
    tri_ref, pos_ref, ten_ref, coarse_ref, face_ref, relax_ref, fluid_ref, pop_ref,
    xs, inc, nodal, acc, force_ref,
    relaxed, pushed, rim, used_ref, coarse_all, parts,
    force_in, zsend, zrecv, xsend, xrecv, csend, crecv,
    load_sems, coarse_sems, force_sems, send_sems, recv_sems,
):
    _, plane_count, columns, rows = pop_ref.shape
    slab = lax.axis_index("slab")
    cross = lax.axis_index("cross")

    def beside(direction, sign):
        dz, dx = direction[0] * sign, direction[1] * sign
        conditions = []
        if dz == 1:
            conditions.append(slab < slabs - 1)
        if dz == -1:
            conditions.append(slab > 0)
        if dx == 1:
            conditions.append(cross < crosses - 1)
        if dx == -1:
            conditions.append(cross > 0)
        return functools.reduce(jnp.logical_and, conditions)

    def target(direction):
        return {"slab": slab + direction[0], "cross": cross + direction[1]}

    loads = [
        pltpu.make_async_copy(source, sink, load_sems.at[i])
        for i, (source, sink) in enumerate(
            (
                (tri_hbm, tri_ref),
                (pos_hbm, pos_ref),
                (ten_hbm, ten_ref),
                (coarse_hbm, coarse_ref),
                (face_hbm, face_ref),
                (relax_hbm, relax_ref),
                (fluid_hbm, fluid_ref),
                (pop_hbm, pop_ref),
            )
        )
    ]
    for load in loads:
        load.start()

    force_in[...] = jnp.zeros_like(force_in)
    zrecv[...] = jnp.zeros_like(zrecv)
    xrecv[...] = jnp.zeros_like(xrecv)
    crecv[...] = jnp.zeros_like(crecv)
    parts[...] = jnp.zeros_like(parts)

    barrier = pltpu.get_barrier_semaphore()

    @pl.loop(1, slabs)
    def _(d):
        peer = lax.rem(slab + d, slabs)
        pl.semaphore_signal(
            barrier, inc=1, device_id={"slab": peer, "cross": cross}, device_id_type=MESH
        )

    expected = slabs - 1
    for direction in DIRECTIONS:
        if direction[1] == 0:
            continue
        there = beside(direction, 1)
        expected = expected + jnp.where(there, 1, 0)

        @pl.when(there)
        def _():
            pl.semaphore_signal(
                barrier, inc=1, device_id=target(direction), device_id_type=MESH
            )

    for load in loads[:3]:
        load.wait()
    nodal_stage(plane_count, columns, rows, pos_ref, tri_ref, ten_ref, xs, inc, nodal)
    loads[3].wait()
    pl.semaphore_wait(barrier, expected)
    coarse_all[slab] = coarse_ref[...]

    def coarse_copy(d):
        return pltpu.make_async_remote_copy(
            src_ref=coarse_ref,
            dst_ref=coarse_all.at[slab],
            send_sem=coarse_sems.at[0, d],
            recv_sem=coarse_sems.at[1, d],
            device_id={"slab": lax.rem(slab + d, slabs), "cross": cross},
            device_id_type=MESH,
        )

    @pl.loop(1, slabs)
    def _(d):
        coarse_copy(d).start()

    spread_stage(xs, nodal, acc, force_ref)

    def force_copy(index):
        start = plane_count + 2 if index == 0 else 0
        return pltpu.make_async_remote_copy(
            src_ref=force_ref.at[:, pl.ds(start, 2)],
            dst_ref=force_in.at[index],
            send_sem=force_sems.at[0, index],
            recv_sem=force_sems.at[1, index],
            device_id=target(DIRECTIONS[index]),
            device_id_type=MESH,
        )

    for index in range(2):

        @pl.when(beside(DIRECTIONS[index], 1))
        def _():
            force_copy(index).start()

    for load in loads[4:]:
        load.wait()

    cell = face_ref[pl.ds(0, 1), :]
    slots = cell.shape[1]
    used = cell >= 0
    place = jnp.where(used, cell // rows, -1)
    lane = jnp.where(used, cell % rows, -1)
    first = face_ref[pl.ds(1, 1), :]
    second = face_ref[pl.ds(2, 1), :]
    width = coarse_ref.shape[1]

    @pl.loop(1, slabs)
    def _(d):
        pltpu.make_async_remote_copy(
            src_ref=coarse_ref,
            dst_ref=coarse_all.at[lax.rem(slab + slabs - d, slabs)],
            send_sem=coarse_sems.at[0, d],
            recv_sem=coarse_sems.at[1, d],
            device_id={"slab": lax.rem(slab + d, slabs), "cross": cross},
            device_id_type=MESH,
        ).wait_recv()

    def blend(j, running):
        for i, piece in enumerate(split(coarse_all[j], 3)):
            parts[pl.ds(8 * i, 4), :] = piece
        ids = lax.broadcasted_iota(I32, (width, slots), 0) + j * width
        table = jnp.where(ids == first, 0.75, 0.0) + jnp.where(ids == second, 0.25, 0.0)
        return running + jnp.dot(
            parts[...].astype(BF16), table.astype(BF16), preferred_element_type=F32
        )

    mixed = lax.fori_loop(0, slabs, blend, jnp.zeros((24, slots), F32))
    blended = mixed[0:4] + (mixed[8:12] + mixed[16:20])

    cells = plane_count * columns
    mask = lax.broadcasted_iota(I32, (cells, slots), 0) == place
    pieces = split(blended, 3)
    left = [jnp.where(mask, piece[m : m + 1], 0.0) for m in range(4) for piece in pieces]
    left.append(jnp.where(mask, 1.0, 0.0))
    right = jnp.where(lax.broadcasted_iota(I32, (rows, slots), 0) == lane, 1.0, 0.0)
    placed = lax.dot_general(
        jnp.concatenate(left, axis=0).astype(BF16), right.astype(BF16), NT, preferred_element_type=F32
    )

    def placed_at(index, p):
        start = index * cells + p * columns
        return placed[start : start + columns]

    for p in range(plane_count):
        filled = [
            placed_at(3 * m, p) + (placed_at(3 * m + 1, p) + placed_at(3 * m + 2, p)) for m in range(4)
        ]
        used_ref[p] = placed_at(12, p)
        for q, value in enumerate(equilibrium_pairs(filled[0], filled[1:])):
            rim[q, p] = value

    for index in range(2):

        @pl.when(beside(DIRECTIONS[index], -1))
        def _():
            force_copy(index).wait_recv()

    for k in range(3):
        for p in range(plane_count):
            value = force_ref[k, p + 2]
            if p < 2:
                value = value + force_in[0, k, p]
            if p >= plane_count - 2:
                value = value + force_in[1, k, p - plane_count + 2]
            pushed[k, p] = value / relax_ref[p]

    sublane = lax.broadcasted_iota(I32, (columns, rows), 0)
    ups, downs = moving(0, 1), moving(0, -1)
    rights, lefts = moving(1, 1), moving(1, -1)
    corner_of = {7: 0, 8: 1, 9: 2, 10: 3}

    def halo_copy(step, index):
        if index < 2:
            source, sink = zsend.at[step, index], zrecv.at[step, index]
        elif index < 4:
            source, sink = xsend.at[step, index - 2], xrecv.at[step, index - 2]
        else:
            source, sink = csend.at[step, index - 4], crecv.at[step, index - 4]
        return pltpu.make_async_remote_copy(
            src_ref=source,
            dst_ref=sink,
            send_sem=send_sems.at[step % 2, index],
            recv_sem=recv_sems.at[step % 2, index],
            device_id=target(DIRECTIONS[index]),
            device_id_type=MESH,
        )

    for step in range(STEPS):
        fields_ref = pop_ref if step == 0 else next_ref
        for p in range(plane_count):
            fields = [fields_ref[q, p] for q in range(19)]
            density, momentum = moments_of(fields)
            inverse = 1.0 / density
            shifted = [(momentum[k] + pushed[k, p]) * inverse for k in range(3)]
            rate = relax_ref[p]
            fluid = fluid_ref[p] == 1
            for q, goal in enumerate(equilibrium_pairs(density, shifted)):
                value = fields[q] + rate * (goal - fields[q])
                value = jnp.where(fluid, value, fields[OPPOSITE[q]])
                relaxed[q, p] = value
                if p == plane_count - 1 and q in ups:
                    zsend[step, 0, ups.index(q)] = value
                if p == 0 and q in downs:
                    zsend[step, 1, downs.index(q)] = value
                if q in rights:
                    xsend[step, 0, rights.index(q), p : p + 1] = value[columns - 1 :]
                if q in lefts:
                    xsend[step, 1, lefts.index(q), p : p + 1] = value[:1]
                if q in corner_of:
                    cz, cx, _ = LATTICE_VECTORS[q]
                    if p == (plane_count - 1 if cz == 1 else 0):
                        edge = value[columns - 1 :] if cx == 1 else value[:1]
                        csend[step, corner_of[q]] = edge
        for index in (4, 5, 6, 7, 0, 1, 2, 3):

            @pl.when(beside(DIRECTIONS[index], 1))
            def _():
                if step >= 2:
                    halo_copy(step - 2, index).wait_send()
                halo_copy(step, index).start()

        for index in range(8):

            @pl.when(beside(DIRECTIONS[index], -1))
            def _():
                halo_copy(step, index).wait_recv()

        for p in range(plane_count):
            fixed = used_ref[p] > 0.5
            for q, (cz, cx, cy) in enumerate(LATTICE_VECTORS):
                source = p - cz
                within = 0 <= source < plane_count
                if within:
                    value = relaxed[q, source]
                elif cz == 1:
                    value = zrecv[step, 0, ups.index(q)]
                else:
                    value = zrecv[step, 1, downs.index(q)]
                if cx != 0:
                    side, members = (0, rights) if cx == 1 else (1, lefts)
                    if within:
                        edge = xrecv[step, side, members.index(q), source : source + 1]
                    else:
                        edge = crecv[step, corner_of[q]]
                    value = pltpu.roll(value, cx % columns, 0)
                    at = 0 if cx == 1 else columns - 1
                    value = jnp.where(sublane == at, edge, value)
                if cy != 0:
                    value = pltpu.roll(value, cy % rows, 1)
                next_ref[q, p] = jnp.where(fixed, rim[q, p], value)

    @pl.loop(1, slabs)
    def _(d):
        coarse_copy(d).wait_send()

    for index in range(2):

        @pl.when(beside(DIRECTIONS[index], 1))
        def _():
            force_copy(index).wait_send()

    for index in range(8):

        @pl.when(beside(DIRECTIONS[index], 1))
        def _():
            for step in range(max(0, STEPS - 2), STEPS):
                halo_copy(step, index).wait_send()


def flow_kernel(fields_ref, next_ref, flow_ref, flow, sems):
    whole = pltpu.make_async_copy(fields_ref, next_ref, sems.at[0])
    whole.start()
    for p in range(fields_ref.shape[1]):
        fields = [fields_ref[q, p] for q in range(19)]
        density, momentum = moments_of(fields)
        inverse = ROOT_THREE / density
        for k in range(3):
            flow[k, p] = momentum[k] * inverse
    part = pltpu.make_async_copy(flow, flow_ref, sems.at[1])
    part.start()
    whole.wait()
    part.wait()


def on_device(
    slabs, crosses,
    populations, fluid_mask, relaxation, positions, triangles, tension, coarse_moments, interface,
):
    _, plane_count, columns, rows = populations.shape
    _, membranes, nodes = positions.shape
    padded = round_up(nodes, 128)
    corners = triangles.shape[1]
    half = (columns + 2) // 2
    cells = round_up((plane_count + 2) * half, 16)
    vmem = pl.BlockSpec(memory_space=pltpu.VMEM)
    block = (19, plane_count, columns, rows)
    operands = (
        triangles, positions, tension, coarse_moments, interface, relaxation, fluid_mask, populations,
    )
    fields = pl.pallas_call(
        functools.partial(lattice_kernel, slabs, crosses),
        name="lattice_steps",
        out_shape=pltpu.VMEM(block, F32),
        in_specs=[pl.BlockSpec(memory_space=pl.ANY)] * 8,
        out_specs=vmem,
        scratch_shapes=[pltpu.VMEM(operand.shape, operand.dtype) for operand in operands]
        + [
            pltpu.VMEM((3, membranes, padded), F32),
            pltpu.VMEM((padded, corners), BF16),
            pltpu.VMEM((3, membranes, padded), F32),
            pltpu.VMEM((6 * cells, 2 * rows), F32),
            pltpu.VMEM((3, plane_count + 4, columns, rows), F32),
            pltpu.VMEM(block, F32),
            pltpu.VMEM((3,) + block[1:], F32),
            pltpu.VMEM(block, F32),
            pltpu.VMEM(block[1:], F32),
            pltpu.VMEM((slabs,) + coarse_moments.shape, F32),
            pltpu.VMEM((24, coarse_moments.shape[1]), F32),
            pltpu.VMEM((2, 3, 2, columns, rows), F32),
            pltpu.VMEM((STEPS, 2, 5, columns, rows), F32),
            pltpu.VMEM((STEPS, 2, 5, columns, rows), F32),
            pltpu.VMEM((STEPS, 2, 5, plane_count, rows), F32),
            pltpu.VMEM((STEPS, 2, 5, plane_count, rows), F32),
            pltpu.VMEM((STEPS, 4, 1, rows), F32),
            pltpu.VMEM((STEPS, 4, 1, rows), F32),
            pltpu.SemaphoreType.DMA((8,)),
            pltpu.SemaphoreType.DMA((2, slabs)),
            pltpu.SemaphoreType.DMA((2, 2)),
            pltpu.SemaphoreType.DMA((2, 8)),
            pltpu.SemaphoreType.DMA((2, 8)),
        ],
        compiler_params=pltpu.CompilerParams(collective_id=0, has_side_effects=True),
    )(*operands)
    return pl.pallas_call(
        flow_kernel,
        name="flow",
        out_shape=(
            jax.ShapeDtypeStruct(block, F32),
            jax.ShapeDtypeStruct((3,) + block[1:], F32),
        ),
        in_specs=[vmem],
        out_specs=(pl.BlockSpec(memory_space=pl.ANY),) * 2,
        scratch_shapes=[pltpu.VMEM((3,) + block[1:], F32), pltpu.SemaphoreType.DMA((2,))],
    )(pltpu.with_memory_space_constraint(fields, pltpu.VMEM))


def solution(mesh):
    in_specs = (
        P(None, "slab", "cross", None),
        P("slab", "cross", None),
        P("slab", "cross", None),
        P(None, "slab", None),
        P(),
        P("slab", None),
        P(None, "slab"),
        P(None, ("slab", "cross")),
    )
    out_specs = (P(None, "slab", "cross", None), P(None, "slab", "cross", None))
    return jax.shard_map(
        functools.partial(on_device, mesh.shape["slab"], mesh.shape["cross"]),
        mesh=mesh, in_specs=in_specs, out_specs=out_specs, check_vma=False,
    )
```

```python
import functools
import math

import jax
import jax.numpy as jnp
from jax import lax
from jax.experimental import pallas as pl
from jax.experimental.pallas import tpu as pltpu
from jax.sharding import PartitionSpec as P

STEPS = 4
MESH = pl.DeviceIdType.MESH
LATTICE_VECTORS = [
    (0, 0, 0),
    (1, 0, 0),
    (-1, 0, 0),
    (0, 1, 0),
    (0, -1, 0),
    (0, 0, 1),
    (0, 0, -1),
    (1, 1, 0),
    (-1, -1, 0),
    (1, -1, 0),
    (-1, 1, 0),
    (1, 0, 1),
    (-1, 0, -1),
    (1, 0, -1),
    (-1, 0, 1),
    (0, 1, 1),
    (0, -1, -1),
    (0, 1, -1),
    (0, -1, 1),
]
LATTICE_WEIGHTS = [1.0 / 3.0] + [1.0 / 18.0] * 6 + [1.0 / 36.0] * 12
OPPOSITE = [0] + [q + 1 if q % 2 == 1 else q - 1 for q in range(1, 19)]
ROOT_THREE = math.sqrt(3.0)
DIRECTIONS = [(1, 0), (-1, 0), (0, 1), (0, -1), (1, 1), (-1, -1), (1, -1), (-1, 1)]
NT = (((1,), (1,)), ((), ()))
F32, BF16, I32, I16 = jnp.float32, jnp.bfloat16, jnp.int32, jnp.int16
HALO = 2
SLAB_MOVES = [
    [(q, depth) for depth in (1, 2) for q in range(19) if LATTICE_VECTORS[q][0] * sign >= depth - 1]
    for sign in (1, -1)
]
CROSS_MOVES = [
    [(q, depth) for depth in (1, 2) for q in range(19) if LATTICE_VECTORS[q][1] * sign >= depth - 1]
    for sign in (1, -1)
]
CORNER_MOVES = [
    [
        (q, dz, dx)
        for dz in (1, 2)
        for dx in (1, 2)
        for q in range(19)
        if LATTICE_VECTORS[q][0] * sz >= dz - 1 and LATTICE_VECTORS[q][1] * sx >= dx - 1
    ]
    for sz, sx in DIRECTIONS[4:]
]


def round_up(value, unit):
    return (value + unit - 1) // unit * unit


def split(value, parts):
    pieces = []
    for _ in range(parts):
        piece = value.astype(BF16).astype(F32)
        pieces.append(piece)
        value = value - piece
    return pieces


def incidence_stage(tri_ref, inc, nodes):
    triangles = tri_ref.shape[1]
    tiles = triangles // 128
    corners = [
        [
            jnp.broadcast_to(tri_ref[pl.ds(k, 1), t * 128 : (t + 1) * 128], (16, 128)).astype(I16)
            for t in range(tiles)
        ]
        for k in range(3)
    ]
    iota = lax.broadcasted_iota(I32, (16, 128), 0)

    def rows_at(start):
        ids = (iota + start).astype(I16)
        for t in range(tiles):
            hit = (ids == corners[0][t]) | (ids == corners[1][t]) | (ids == corners[2][t])
            inc[pl.ds(start, 16), t * 128 : (t + 1) * 128] = jnp.where(
                hit, jnp.ones((), BF16), jnp.zeros((), BF16)
            )

    chunk = 128

    @pl.loop(0, nodes // chunk)
    def _(i):
        for r in range(chunk // 16):
            rows_at(pl.multiple_of(i * chunk + r * 16, 16))

    done = nodes // chunk * chunk
    while done < nodes:
        rows_at(done)
        done += 16
    if done < inc.shape[0]:
        inc[done:, :] = jnp.zeros((inc.shape[0] - done, triangles), BF16)


def nodal_stage(plane_count, columns, rows, pos_ref, ten_ref, inc, xs, cell_ref, lane_ref, force):
    dims, membranes, nodes = pos_ref.shape
    padded = xs.shape[2]
    slab = lax.axis_index("slab")
    cross = lax.axis_index("cross")
    planes, half = plane_count + 2, (columns + 6) // 2

    cell_ref[...] = jnp.full(cell_ref.shape, -1, I32)
    lane_ref[...] = jnp.full(lane_ref.shape, -1, I32)
    plane = pos_ref[0] - (slab * plane_count - 1)
    column = pos_ref[1] - (cross * columns - 3)
    row = pos_ref[2]
    inside = (column >= 0) & (column < 2 * half)
    upper = column >= half
    cell = jnp.where(upper, column - half, column) * planes + plane
    cell_ref[:, :nodes] = jnp.where(inside, cell, -1)
    lane_ref[:, :nodes] = row + jnp.where(upper, rows, 0)

    xs[...] = jnp.zeros_like(xs)
    for k in range(3):
        xs[k, :, :nodes] = (pos_ref[k] - pos_ref[k, :, 0:1]).astype(F32)

    coords = xs[...].reshape(dims * membranes, padded)
    sums = jnp.dot(coords.astype(BF16), inc[...], preferred_element_type=F32)
    tension = ten_ref[...]
    terms = jnp.concatenate(
        [sums[k * membranes : (k + 1) * membranes] * tension for k in range(3)] + [tension], axis=0
    )
    stacked = jnp.concatenate(split(terms, 2), axis=0).astype(BF16)
    gathered = lax.dot_general(stacked, inc[...], NT, preferred_element_type=F32)
    count = terms.shape[0]
    total = gathered[:count] + gathered[count:]
    weight = total[3 * membranes :]
    for k in range(3):
        force[k] = total[k * membranes : (k + 1) * membranes] - 3.0 * xs[k] * weight


def spread_stage(plane_count, columns, cell_ref, lane_ref, force, acc, along, across, out_ref):
    _, membranes, padded = force.shape
    rows = out_ref.shape[2]
    planes, half = plane_count + 2, (columns + 6) // 2
    extent = plane_count + 2 * HALO
    cells = acc.shape[0] // 6
    acc[...] = jnp.zeros_like(acc)
    unroll = 4 if membranes % 4 == 0 else 1
    zero, one = jnp.zeros((), BF16), jnp.ones((), BF16)

    @pl.loop(0, membranes // unroll)
    def _(i):
        running = None
        for inner in range(unroll):
            m = pl.ds(i * unroll + inner, 1)
            cell = cell_ref[m, :].astype(I16)
            lane = lane_ref[m, :].astype(I16)
            mask = lax.broadcasted_iota(I16, (cells, padded), 0) == cell
            values = [split(force[k, m, :], 2) for k in range(3)]
            left = jnp.concatenate(
                [
                    jnp.where(mask, values[k][part].astype(BF16), zero)
                    for part in range(2)
                    for k in range(3)
                ],
                axis=0,
            )
            right = jnp.where(lax.broadcasted_iota(I16, (2 * rows, padded), 0) == lane, one, zero)
            product = lax.dot_general(left, right, NT, preferred_element_type=F32)
            running = product if running is None else running + product
        acc[...] += running

    used = half * planes
    inner = (columns + 4) * planes
    step = lax.broadcasted_iota(I32, (extent, rows), 0)
    weights = [
        jnp.where((step >= 2 - shift) & (step < planes + 2 - shift), w, 0.0)
        for shift, w in ((0, 0.25), (1, 0.5), (2, 0.25))
    ]
    for k in range(3):
        value = acc[k * cells : (k + 1) * cells] + acc[(3 + k) * cells : (4 + k) * cells]
        for part in range(2):
            b = value[:, part * rows : (part + 1) * rows]
            b = 0.5 * b + 0.25 * (pltpu.roll(b, 1, 1) + pltpu.roll(b, rows - 1, 1))
            along[k, part * used : part * used + cells] = b
        across[k, 0:8] = jnp.zeros((8, rows), F32)
        across[k, 8 + inner : 16 + inner] = jnp.zeros((8, rows), F32)
        across[k, 8 : 8 + inner] = 0.5 * along[k, planes : planes + inner] + 0.25 * (
            along[k, 0:inner] + along[k, 2 * planes : 2 * planes + inner]
        )
        for c in range(columns + 4):
            start = 8 + c * planes
            out_ref[k, (c + 1) * extent : (c + 2) * extent] = (
                weights[0] * across[k, start - 2 : start - 2 + extent]
                + weights[1] * across[k, start - 1 : start - 1 + extent]
                + weights[2] * across[k, start : start + extent]
            )


def equilibrium_pairs(density, velocity):
    squared = velocity[0] * velocity[0] + velocity[1] * velocity[1] + velocity[2] * velocity[2]
    base = 1.0 - 1.5 * squared
    result = [None] * 19
    result[0] = LATTICE_WEIGHTS[0] * density * base
    scaled = {w: w * density for w in (1.0 / 18.0, 1.0 / 36.0)}
    for q in range(1, 19, 2):
        projected = None
        for c, v in zip(LATTICE_VECTORS[q], velocity):
            if c == 0:
                continue
            if projected is None:
                projected = v if c == 1 else -v
            else:
                projected = projected + v if c == 1 else projected - v
        even = base + 4.5 * projected * projected
        odd = 3.0 * projected
        weight = scaled[LATTICE_WEIGHTS[q]]
        result[q] = weight * (even + odd)
        result[q + 1] = weight * (even - odd)
    return result


def moments_of(fields):
    density = functools.reduce(lambda a, b: a + b, fields)
    momentum = []
    for k in range(3):
        plus = [fields[q] for q in range(19) if LATTICE_VECTORS[q][k] == 1]
        minus = [fields[q] for q in range(19) if LATTICE_VECTORS[q][k] == -1]
        momentum.append(functools.reduce(lambda a, b: a + b, [a - b for a, b in zip(plus, minus)]))
    return density, momentum


def collide(fields, rate, pushed):
    sums = [fields[q] + fields[q + 1] for q in range(1, 19, 2)]
    gaps = [fields[q] - fields[q + 1] for q in range(1, 19, 2)]
    density = functools.reduce(lambda a, b: a + b, sums) + fields[0]
    scale = 3.0 / density
    tripled = []
    for k in range(3):
        total = pushed[k]
        for pair in range(9):
            c = LATTICE_VECTORS[2 * pair + 1][k]
            if c:
                total = total + gaps[pair] if c == 1 else total - gaps[pair]
        tripled.append(total * scale)
    squared = tripled[0] * tripled[0] + tripled[1] * tripled[1] + tripled[2] * tripled[2]
    base = 1.0 - (1.0 / 6.0) * squared
    fluid = rate > 0.0
    keep = 1.0 - rate
    strength = rate * density
    scaled = {w: w * strength for w in (1.0 / 18.0, 1.0 / 36.0)}
    result = [None] * 19
    rest = keep * fields[0] + (LATTICE_WEIGHTS[0] * strength) * base
    result[0] = jnp.where(fluid, rest, fields[0])
    for q in range(1, 19, 2):
        projected = None
        for c, v in zip(LATTICE_VECTORS[q], tripled):
            if c == 0:
                continue
            if projected is None:
                projected = v if c == 1 else -v
            else:
                projected = projected + v if c == 1 else projected - v
        weight = scaled[LATTICE_WEIGHTS[q]]
        even = weight * (base + 0.5 * projected * projected)
        odd = weight * projected
        result[q] = jnp.where(fluid, keep * fields[q] + (even + odd), fields[q + 1])
        result[q + 1] = jnp.where(fluid, keep * fields[q + 1] + (even - odd), fields[q])
    return result


def lattice_kernel(
    slabs, crosses,
    tri_hbm, pop_hbm, relax_hbm, fluid_hbm, pos_hbm, ten_hbm, coarse_hbm, face_hbm,
    next_ref,
    tri_ref, pop_ref, relax_ref, fluid_ref, pos_ref, ten_ref, coarse_ref, face_ref,
    xs, inc, nodal, cell_ref, lane_ref, acc, along, across,
    raw, own_force, far_force, pushed, placed_ref, rim, post_one, post_two, post_three,
    coarse_all, parts,
    zsend, zrecv, xsend, xrecv, csend, crecv,
    load_sems, coarse_sems, raw_sems, force_sems, placed_sems, halo_sems,
):
    _, plane_count, columns, rows = pop_ref.shape
    extent, wide = plane_count + 2 * HALO, columns + 2 * HALO
    slab = lax.axis_index("slab")
    cross = lax.axis_index("cross")

    def beside(direction, sign):
        dz, dx = direction[0] * sign, direction[1] * sign
        conditions = []
        if dz == 1:
            conditions.append(slab < slabs - 1)
        if dz == -1:
            conditions.append(slab > 0)
        if dx == 1:
            conditions.append(cross < crosses - 1)
        if dx == -1:
            conditions.append(cross > 0)
        return functools.reduce(jnp.logical_and, conditions)

    def target(direction):
        return {"slab": slab + direction[0], "cross": cross + direction[1]}

    def cubed(ref):
        return ref.reshape(ref.shape[0], wide + 2, extent, rows)

    def spans(step, size, depth):
        if step == 1:
            return HALO + size - depth, HALO - depth, depth
        if step == -1:
            return HALO, HALO + size, depth
        return HALO, HALO, size

    def block_copy(ref, sems, index, depth):
        dz, dx = DIRECTIONS[index]
        z_from, z_to, z_size = spans(dz, plane_count, depth)
        x_from, x_to, x_size = spans(dx, columns, depth)
        whole = cubed(ref)
        return pltpu.make_async_remote_copy(
            src_ref=whole.at[:, pl.ds(1 + x_from, x_size), pl.ds(z_from, z_size)],
            dst_ref=whole.at[:, pl.ds(1 + x_to, x_size), pl.ds(z_to, z_size)],
            send_sem=sems.at[0, index],
            recv_sem=sems.at[1, index],
            device_id=target(DIRECTIONS[index]),
            device_id_type=MESH,
        )

    def column_rows(c):
        return pl.ds((c + 1) * extent, extent)

    def plane_rows(p, dz=0, dx=0):
        return pl.ds((HALO + 1 - dx) * extent + HALO + p - dz, columns, stride=extent)

    loads = [
        pltpu.make_async_copy(source, sink, load_sems.at[i])
        for i, (source, sink) in enumerate(
            (
                (tri_hbm, tri_ref),
                (pop_hbm, pop_ref),
                (relax_hbm, relax_ref),
                (fluid_hbm, fluid_ref),
                (pos_hbm, pos_ref),
                (ten_hbm, ten_ref),
                (coarse_hbm, coarse_ref),
                (face_hbm, face_ref),
            )
        )
    ]
    for load in loads:
        load.start()

    barrier = pltpu.get_barrier_semaphore()

    @pl.loop(1, slabs)
    def _(d):
        peer = lax.rem(slab + d, slabs)
        pl.semaphore_signal(
            barrier, inc=1, device_id={"slab": peer, "cross": cross}, device_id_type=MESH
        )

    expected = slabs - 1
    for direction in DIRECTIONS:
        if direction[1] == 0:
            continue
        there = beside(direction, 1)
        expected = expected + jnp.where(there, 1, 0)

        @pl.when(there)
        def _():
            pl.semaphore_signal(
                barrier, inc=1, device_id=target(direction), device_id_type=MESH
            )

    def clear(side):
        dz, dx = DIRECTIONS[side]
        for c in range(-1, wide + 1):
            if dx == 1 and c >= HALO or dx == -1 and c < HALO + columns:
                continue
            start = (c + 1) * extent
            if dz == 1:
                start, size = start, HALO
            elif dz == -1:
                start, size = start + HALO + plane_count, HALO
            else:
                size = extent
            for q in range(20):
                raw[q, pl.ds(start, size), :] = jnp.zeros((size, rows), F32)
            for q in range(5):
                placed_ref[q, pl.ds(start, size), :] = jnp.full((size, rows), 1.0 if q == 4 else 0.0, F32)
        if dx == 0:
            zrecv[side] = jnp.zeros(zrecv.shape[1:], F32)
            near = 0 if dz == 1 else extent // 2
            for c in range(wide):
                for k in range(3):
                    far_force[k, pl.ds((c + 1) * extent + near, extent // 2), :] = jnp.zeros(
                        (extent // 2, rows), F32
                    )
        else:
            xrecv[side - 2] = jnp.zeros(xrecv.shape[1:], F32)

    for side in range(4):

        @pl.when(jnp.logical_not(beside(DIRECTIONS[side], -1)))
        def _():
            clear(side)

    for index in range(4):

        @pl.when(jnp.logical_not(beside(DIRECTIONS[4 + index], -1)))
        def _():
            crecv[index] = jnp.zeros(crecv.shape[1:], F32)

    loads[0].wait()
    incidence_stage(tri_ref, inc, pos_ref.shape[2])
    for load in loads[1:4]:
        load.wait()
    for p in range(plane_count):
        for q in range(19):
            raw[q, plane_rows(p), :] = pop_ref[q, p]
        raw[19, plane_rows(p), :] = jnp.where(fluid_ref[p] == 1, relax_ref[p], 0.0)
    loads[6].wait()
    pl.semaphore_wait(barrier, expected)

    for index in (4, 5, 6, 7, 0, 1, 2, 3):

        @pl.when(beside(DIRECTIONS[index], 1))
        def _():
            block_copy(raw, raw_sems, index, HALO).start()

    coarse_all[slab] = coarse_ref[...]

    def coarse_copy(d):
        return pltpu.make_async_remote_copy(
            src_ref=coarse_ref,
            dst_ref=coarse_all.at[slab],
            send_sem=coarse_sems.at[0, d],
            recv_sem=coarse_sems.at[1, d],
            device_id={"slab": lax.rem(slab + d, slabs), "cross": cross},
            device_id_type=MESH,
        )

    @pl.loop(1, slabs)
    def _(d):
        coarse_copy(d).start()

    for load in loads[4:6]:
        load.wait()
    nodal_stage(
        plane_count, columns, rows, pos_ref, ten_ref, inc, xs, cell_ref, lane_ref, nodal
    )
    spread_stage(plane_count, columns, cell_ref, lane_ref, nodal, acc, along, across, own_force)

    def force_copy(index):
        part = extent // 2
        start = part if index == 0 else 0
        return pltpu.make_async_remote_copy(
            src_ref=cubed(own_force).at[:, pl.ds(1, wide), pl.ds(start, part)],
            dst_ref=cubed(far_force).at[:, pl.ds(1, wide), pl.ds(part - start, part)],
            send_sem=force_sems.at[0, index],
            recv_sem=force_sems.at[1, index],
            device_id=target(DIRECTIONS[index]),
            device_id_type=MESH,
        )

    for index in range(2):

        @pl.when(beside(DIRECTIONS[index], 1))
        def _():
            force_copy(index).start()

    loads[7].wait()
    cell = face_ref[pl.ds(0, 1), :]
    slots = cell.shape[1]
    used = cell >= 0
    place = cell // rows
    place = jnp.where(used, place % columns * plane_count + place // columns, -1)
    lane = jnp.where(used, cell % rows, -1)
    first = face_ref[pl.ds(1, 1), :]
    second = face_ref[pl.ds(2, 1), :]
    width = coarse_ref.shape[1]

    @pl.loop(1, slabs)
    def _(d):
        pltpu.make_async_remote_copy(
            src_ref=coarse_ref,
            dst_ref=coarse_all.at[lax.rem(slab + slabs - d, slabs)],
            send_sem=coarse_sems.at[0, d],
            recv_sem=coarse_sems.at[1, d],
            device_id={"slab": lax.rem(slab + d, slabs), "cross": cross},
            device_id_type=MESH,
        ).wait_recv()

    parts[...] = jnp.zeros_like(parts)
    zero = jnp.zeros((), BF16)

    def local(index, j):
        at = index - j * width
        return jnp.where((at >= 0) & (at < width), at, -1).astype(I16)

    def blend(j, running):
        for i, piece in enumerate(split(coarse_all[j], 2)):
            parts[pl.ds(8 * i, 4), :] = piece
        ids = lax.broadcasted_iota(I16, (width, slots), 0)
        table = jnp.where(ids == local(first, j), jnp.full((), 0.75, BF16), zero) + jnp.where(
            ids == local(second, j), jnp.full((), 0.25, BF16), zero
        )
        return running + jnp.dot(parts[...].astype(BF16), table, preferred_element_type=F32)

    mixed = lax.fori_loop(0, slabs, blend, jnp.zeros((16, slots), F32))
    blended = mixed[0:4] + mixed[8:12]

    cells = plane_count * columns
    mask = lax.broadcasted_iota(I32, (cells, slots), 0) == place
    pieces = split(blended, 2)
    left = [jnp.where(mask, piece[m : m + 1], 0.0) for m in range(4) for piece in pieces]
    left.append(jnp.where(mask, 1.0, 0.0))
    right = jnp.where(lax.broadcasted_iota(I32, (rows, slots), 0) == lane, 1.0, 0.0)
    placed = lax.dot_general(
        jnp.concatenate(left, axis=0).astype(BF16), right.astype(BF16), NT, preferred_element_type=F32
    )
    for m in range(5):
        value = placed[2 * m * cells : (2 * m + 1) * cells]
        if m < 4:
            value = value + placed[(2 * m + 1) * cells : (2 * m + 2) * cells]
        for c in range(columns):
            placed_ref[m, pl.ds((HALO + 1 + c) * extent + HALO, plane_count), :] = value[
                c * plane_count : (c + 1) * plane_count
            ]

    for index in (4, 5, 6, 7, 0, 1, 2, 3):

        @pl.when(beside(DIRECTIONS[index], 1))
        def _():
            block_copy(placed_ref, placed_sems, index, 1).start()

    for index in range(8):

        @pl.when(beside(DIRECTIONS[index], -1))
        def _():
            block_copy(placed_ref, placed_sems, index, 1).wait_recv()

    for c in range(1, wide - 1):
        at = column_rows(c)
        density = placed_ref[0, at, :]
        velocity = [placed_ref[k, at, :] for k in range(1, 4)]
        for q, value in enumerate(equilibrium_pairs(density, velocity)):
            rim[q, at, :] = value

    for index in range(2):

        @pl.when(beside(DIRECTIONS[index], -1))
        def _():
            force_copy(index).wait_recv()

    for index in range(8):

        @pl.when(beside(DIRECTIONS[index], -1))
        def _():
            block_copy(raw, raw_sems, index, HALO).wait_recv()

    def pulled(source, at, starts):
        fixed = placed_ref[4, at, :] > 0.5
        fields = []
        for q, (cz, cx, cy) in enumerate(LATTICE_VECTORS):
            value = source[q, starts(cz, cx), :]
            if cy != 0:
                value = pltpu.roll(value, cy % rows, 1)
            fields.append(jnp.where(fixed, rim[q, at, :], value))
        return fields

    def pulled_column(source, c):
        return pulled(
            source,
            column_rows(c),
            lambda cz, cx: pl.ds((c + 1 - cx) * extent - cz, extent),
        )

    def pulled_plane(source, p):
        return pulled(source, plane_rows(p), lambda cz, cx: plane_rows(p, cz, cx))

    for c in range(wide):
        at = column_rows(c)
        rate = raw[19, at, :]
        fluid = rate > 0.0
        inverse = 1.0 / rate
        push = []
        for k in range(3):
            value = jnp.where(fluid, (own_force[k, at, :] + far_force[k, at, :]) * inverse, 0.0)
            pushed[k, at, :] = value
            push.append(value)
        for q, value in enumerate(collide([raw[q, at, :] for q in range(19)], rate, push)):
            post_one[q, at, :] = value

    def collide_columns(source, sink):
        for c in range(1, wide - 1):
            at = column_rows(c)
            fields = pulled_column(source, c)
            push = [pushed[k, at, :] for k in range(3)]
            for q, value in enumerate(collide(fields, raw[19, at, :], push)):
                sink[q, at, :] = value

    collide_columns(post_one, post_two)

    for p in range(plane_count):
        at = plane_rows(p)
        fields = pulled_plane(post_two, p)
        push = [pushed[k, at, :] for k in range(3)]
        for q, value in enumerate(collide(fields, raw[19, at, :], push)):
            post_three[q, at, :] = value
            for side in range(2):
                depth = plane_count - p if side == 0 else p + 1
                if (q, depth) in SLAB_MOVES[side]:
                    zsend[side, SLAB_MOVES[side].index((q, depth))] = value

    def inner_row(step, depth, size):
        return HALO + (size - depth if step == 1 else depth - 1)

    def outer_row(step, depth, size):
        return HALO + (-depth if step == 1 else size - 1 + depth)

    for side in range(4):
        for e, (q, dz, dx) in enumerate(CORNER_MOVES[side]):
            sz, sx = DIRECTIONS[4 + side]
            row = (inner_row(sx, dx, columns) + 1) * extent + inner_row(sz, dz, plane_count)
            csend[side, pl.ds(e, 1), :] = post_three[q, pl.ds(row, 1), :]
    for side in range(2):
        for e, (q, depth) in enumerate(CROSS_MOVES[side]):
            row = (inner_row(DIRECTIONS[2 + side][1], depth, columns) + 1) * extent + HALO
            xsend[side, pl.ds(e * plane_count, plane_count), :] = post_three[
                q, pl.ds(row, plane_count), :
            ]

    def halo_copy(index):
        if index < 2:
            source, sink = zsend.at[index], zrecv.at[index]
        elif index < 4:
            source, sink = xsend.at[index - 2], xrecv.at[index - 2]
        else:
            source, sink = csend.at[index - 4], crecv.at[index - 4]
        return pltpu.make_async_remote_copy(
            src_ref=source,
            dst_ref=sink,
            send_sem=halo_sems.at[0, index],
            recv_sem=halo_sems.at[1, index],
            device_id=target(DIRECTIONS[index]),
            device_id_type=MESH,
        )

    for index in (4, 5, 6, 7, 0, 1, 2, 3):

        @pl.when(beside(DIRECTIONS[index], 1))
        def _():
            halo_copy(index).start()

    for index in range(8):

        @pl.when(beside(DIRECTIONS[index], -1))
        def _():
            halo_copy(index).wait_recv()

    for side in range(2):
        for e, (q, depth) in enumerate(SLAB_MOVES[side]):
            row = outer_row(DIRECTIONS[side][0], depth, plane_count)
            post_three[q, plane_rows(row - HALO), :] = zrecv[side, e]
        for e, (q, depth) in enumerate(CROSS_MOVES[side]):
            row = (outer_row(DIRECTIONS[2 + side][1], depth, columns) + 1) * extent + HALO
            post_three[q, pl.ds(row, plane_count), :] = xrecv[
                side, pl.ds(e * plane_count, plane_count), :
            ]
    for side in range(4):
        for e, (q, dz, dx) in enumerate(CORNER_MOVES[side]):
            sz, sx = DIRECTIONS[4 + side]
            row = (outer_row(sx, dx, columns) + 1) * extent + outer_row(sz, dz, plane_count)
            post_three[q, pl.ds(row, 1), :] = crecv[side, pl.ds(e, 1), :]

    collide_columns(post_three, post_one)

    for p in range(plane_count):
        for q, value in enumerate(pulled_plane(post_one, p)):
            next_ref[q, p] = value

    @pl.loop(1, slabs)
    def _(d):
        coarse_copy(d).wait_send()

    for index in range(8):

        @pl.when(beside(DIRECTIONS[index], 1))
        def _():
            block_copy(raw, raw_sems, index, HALO).wait_send()
            block_copy(placed_ref, placed_sems, index, 1).wait_send()
            halo_copy(index).wait_send()
            if index < 2:
                force_copy(index).wait_send()


def flow_kernel(fields_ref, next_ref, flow_ref, flow, sems):
    whole = pltpu.make_async_copy(fields_ref, next_ref, sems.at[0])
    whole.start()
    for p in range(fields_ref.shape[1]):
        fields = [fields_ref[q, p] for q in range(19)]
        density, momentum = moments_of(fields)
        inverse = ROOT_THREE / density
        for k in range(3):
            flow[k, p] = momentum[k] * inverse
    part = pltpu.make_async_copy(flow, flow_ref, sems.at[1])
    part.start()
    whole.wait()
    part.wait()


def on_device(
    slabs, crosses,
    populations, fluid_mask, relaxation, positions, triangles, tension, coarse_moments, interface,
):
    _, plane_count, columns, rows = populations.shape
    _, membranes, nodes = positions.shape
    padded = round_up(nodes, 128)
    corners = triangles.shape[1]
    half, planes = (columns + 6) // 2, plane_count + 2
    cells = round_up(planes * half, 16)
    flat = (columns + 2 * HALO + 2) * (plane_count + 2 * HALO)
    vmem = pl.BlockSpec(memory_space=pltpu.VMEM)
    block = (19, plane_count, columns, rows)
    operands = (
        triangles, populations, relaxation, fluid_mask, positions, tension, coarse_moments, interface,
    )
    fields = pl.pallas_call(
        functools.partial(lattice_kernel, slabs, crosses),
        name="lattice_steps",
        out_shape=pltpu.VMEM(block, F32),
        in_specs=[pl.BlockSpec(memory_space=pl.ANY)] * 8,
        out_specs=vmem,
        scratch_shapes=[pltpu.VMEM(operand.shape, operand.dtype) for operand in operands]
        + [
            pltpu.VMEM((3, membranes, padded), F32),
            pltpu.VMEM((padded, corners), BF16),
            pltpu.VMEM((3, membranes, padded), F32),
            pltpu.VMEM((membranes, padded), I32),
            pltpu.VMEM((membranes, padded), I32),
            pltpu.VMEM((6 * cells, 2 * rows), F32),
            pltpu.VMEM((3, half * planes + cells, rows), F32),
            pltpu.VMEM((3, (columns + 4) * planes + 16, rows), F32),
            pltpu.VMEM((20, flat, rows), F32),
            pltpu.VMEM((3, flat, rows), F32),
            pltpu.VMEM((3, flat, rows), F32),
            pltpu.VMEM((3, flat, rows), F32),
            pltpu.VMEM((5, flat, rows), F32),
            pltpu.VMEM((19, flat, rows), F32),
            pltpu.VMEM((19, flat, rows), F32),
            pltpu.VMEM((19, flat, rows), F32),
            pltpu.VMEM((19, flat, rows), F32),
            pltpu.VMEM((slabs,) + coarse_moments.shape, F32),
            pltpu.VMEM((16, coarse_moments.shape[1]), F32),
            pltpu.VMEM((2, 19, columns, rows), F32),
            pltpu.VMEM((2, 19, columns, rows), F32),
            pltpu.VMEM((2, round_up(19 * plane_count, 8), rows), F32),
            pltpu.VMEM((2, round_up(19 * plane_count, 8), rows), F32),
            pltpu.VMEM((4, 24, rows), F32),
            pltpu.VMEM((4, 24, rows), F32),
            pltpu.SemaphoreType.DMA((8,)),
            pltpu.SemaphoreType.DMA((2, slabs)),
            pltpu.SemaphoreType.DMA((2, 8)),
            pltpu.SemaphoreType.DMA((2, 2)),
            pltpu.SemaphoreType.DMA((2, 8)),
            pltpu.SemaphoreType.DMA((2, 8)),
        ],
        compiler_params=pltpu.CompilerParams(collective_id=0, has_side_effects=True),
    )(*operands)
    return pl.pallas_call(
        flow_kernel,
        name="flow",
        out_shape=(
            jax.ShapeDtypeStruct(block, F32),
            jax.ShapeDtypeStruct((3,) + block[1:], F32),
        ),
        in_specs=[vmem],
        out_specs=(pl.BlockSpec(memory_space=pl.ANY),) * 2,
        scratch_shapes=[pltpu.VMEM((3,) + block[1:], F32), pltpu.SemaphoreType.DMA((2,))],
    )(pltpu.with_memory_space_constraint(fields, pltpu.VMEM))


def solution(mesh):
    in_specs = (
        P(None, "slab", "cross", None),
        P("slab", "cross", None),
        P("slab", "cross", None),
        P(None, "slab", None),
        P(),
        P("slab", None),
        P(None, "slab"),
        P(None, ("slab", "cross")),
    )
    out_specs = (P(None, "slab", "cross", None), P(None, "slab", "cross", None))
    return jax.shard_map(
        functools.partial(on_device, mesh.shape["slab"], mesh.shape["cross"]),
        mesh=mesh, in_specs=in_specs, out_specs=out_specs, check_vma=False,
    )
```

```python
import functools
import math

import jax
import jax.numpy as jnp
from jax import lax
from jax.experimental import pallas as pl
from jax.experimental.pallas import tpu as pltpu
from jax.sharding import PartitionSpec as P

STEPS = 4
MESH = pl.DeviceIdType.MESH
LATTICE_VECTORS = [
    (0, 0, 0),
    (1, 0, 0),
    (-1, 0, 0),
    (0, 1, 0),
    (0, -1, 0),
    (0, 0, 1),
    (0, 0, -1),
    (1, 1, 0),
    (-1, -1, 0),
    (1, -1, 0),
    (-1, 1, 0),
    (1, 0, 1),
    (-1, 0, -1),
    (1, 0, -1),
    (-1, 0, 1),
    (0, 1, 1),
    (0, -1, -1),
    (0, 1, -1),
    (0, -1, 1),
]
LATTICE_WEIGHTS = [1.0 / 3.0] + [1.0 / 18.0] * 6 + [1.0 / 36.0] * 12
OPPOSITE = [0] + [q + 1 if q % 2 == 1 else q - 1 for q in range(1, 19)]
ROOT_THREE = math.sqrt(3.0)
DIRECTIONS = [(1, 0), (-1, 0), (0, 1), (0, -1), (1, 1), (-1, -1), (1, -1), (-1, 1)]
NT = (((1,), (1,)), ((), ()))
F32, BF16, I32, I16 = jnp.float32, jnp.bfloat16, jnp.int32, jnp.int16
HALO = 2
SLAB_MOVES = [
    [(q, depth) for depth in (1, 2) for q in range(19) if LATTICE_VECTORS[q][0] * sign >= depth - 1]
    for sign in (1, -1)
]
CROSS_MOVES = [
    [(q, depth) for depth in (1, 2) for q in range(19) if LATTICE_VECTORS[q][1] * sign >= depth - 1]
    for sign in (1, -1)
]
CORNER_MOVES = [
    [
        (q, dz, dx)
        for dz in (1, 2)
        for dx in (1, 2)
        for q in range(19)
        if LATTICE_VECTORS[q][0] * sz >= dz - 1 and LATTICE_VECTORS[q][1] * sx >= dx - 1
    ]
    for sz, sx in DIRECTIONS[4:]
]


def round_up(value, unit):
    return (value + unit - 1) // unit * unit


def split(value, parts):
    pieces = []
    for _ in range(parts):
        piece = value.astype(BF16).astype(F32)
        pieces.append(piece)
        value = value - piece
    return pieces


def incidence_stage(tri_ref, inc, nodes):
    triangles = tri_ref.shape[1]
    tiles = triangles // 128
    corners = [
        [
            jnp.broadcast_to(tri_ref[pl.ds(k, 1), t * 128 : (t + 1) * 128], (16, 128)).astype(I16)
            for t in range(tiles)
        ]
        for k in range(3)
    ]
    iota = lax.broadcasted_iota(I32, (16, 128), 0)

    def rows_at(start):
        ids = (iota + start).astype(I16)
        for t in range(tiles):
            hit = (ids == corners[0][t]) | (ids == corners[1][t]) | (ids == corners[2][t])
            inc[pl.ds(start, 16), t * 128 : (t + 1) * 128] = jnp.where(
                hit, jnp.ones((), BF16), jnp.zeros((), BF16)
            )

    chunk = 128

    @pl.loop(0, nodes // chunk)
    def _(i):
        for r in range(chunk // 16):
            rows_at(pl.multiple_of(i * chunk + r * 16, 16))

    done = nodes // chunk * chunk
    while done < nodes:
        rows_at(done)
        done += 16
    if done < inc.shape[0]:
        inc[done:, :] = jnp.zeros((inc.shape[0] - done, triangles), BF16)


def nodal_stage(plane_count, columns, rows, pos_ref, ten_ref, inc, xs, cell_ref, lane_ref, force):
    dims, membranes, nodes = pos_ref.shape
    padded = xs.shape[2]
    slab = lax.axis_index("slab")
    cross = lax.axis_index("cross")
    planes, half = plane_count + 2, (columns + 6) // 2

    cell_ref[...] = jnp.full(cell_ref.shape, -1, I32)
    lane_ref[...] = jnp.full(lane_ref.shape, -1, I32)
    plane = pos_ref[0] - (slab * plane_count - 1)
    column = pos_ref[1] - (cross * columns - 3)
    row = pos_ref[2]
    inside = (column >= 0) & (column < 2 * half)
    upper = column >= half
    cell = jnp.where(upper, column - half, column) * planes + plane
    cell_ref[:, :nodes] = jnp.where(inside, cell, -1)
    lane_ref[:, :nodes] = row + jnp.where(upper, rows, 0)

    xs[...] = jnp.zeros_like(xs)
    for k in range(3):
        xs[k, :, :nodes] = (pos_ref[k] - pos_ref[k, :, 0:1]).astype(F32)

    coords = xs[...].reshape(dims * membranes, padded)
    sums = jnp.dot(coords.astype(BF16), inc[...], preferred_element_type=F32)
    tension = ten_ref[...]
    terms = jnp.concatenate(
        [sums[k * membranes : (k + 1) * membranes] * tension for k in range(3)] + [tension], axis=0
    )
    stacked = jnp.concatenate(split(terms, 2), axis=0).astype(BF16)
    gathered = lax.dot_general(stacked, inc[...], NT, preferred_element_type=F32)
    count = terms.shape[0]
    total = gathered[:count] + gathered[count:]
    weight = total[3 * membranes :]
    for k in range(3):
        force[k] = total[k * membranes : (k + 1) * membranes] - 3.0 * xs[k] * weight


def spread_stage(plane_count, columns, cell_ref, lane_ref, force, acc, along, across, out_ref):
    _, membranes, padded = force.shape
    rows = out_ref.shape[2]
    planes, half = plane_count + 2, (columns + 6) // 2
    extent = plane_count + 2 * HALO
    cells = acc.shape[0] // 6
    acc[...] = jnp.zeros_like(acc)
    unroll = 4 if membranes % 4 == 0 else 1
    zero, one = jnp.zeros((), BF16), jnp.ones((), BF16)

    @pl.loop(0, membranes // unroll)
    def _(i):
        running = None
        for inner in range(unroll):
            m = pl.ds(i * unroll + inner, 1)
            cell = cell_ref[m, :].astype(I16)
            lane = lane_ref[m, :].astype(I16)
            mask = lax.broadcasted_iota(I16, (cells, padded), 0) == cell
            values = [split(force[k, m, :], 2) for k in range(3)]
            left = jnp.concatenate(
                [
                    jnp.where(mask, values[k][part].astype(BF16), zero)
                    for part in range(2)
                    for k in range(3)
                ],
                axis=0,
            )
            right = jnp.where(lax.broadcasted_iota(I16, (2 * rows, padded), 0) == lane, one, zero)
            product = lax.dot_general(left, right, NT, preferred_element_type=F32)
            running = product if running is None else running + product
        acc[...] += running

    used = half * planes
    inner = (columns + 4) * planes
    step = lax.broadcasted_iota(I32, (extent, rows), 0)
    weights = [
        jnp.where((step >= 2 - shift) & (step < planes + 2 - shift), w, 0.0)
        for shift, w in ((0, 0.25), (1, 0.5), (2, 0.25))
    ]
    for k in range(3):
        value = acc[k * cells : (k + 1) * cells] + acc[(3 + k) * cells : (4 + k) * cells]
        for part in range(2):
            b = value[:, part * rows : (part + 1) * rows]
            b = 0.5 * b + 0.25 * (pltpu.roll(b, 1, 1) + pltpu.roll(b, rows - 1, 1))
            along[k, part * used : part * used + cells] = b
        across[k, 0:8] = jnp.zeros((8, rows), F32)
        across[k, 8 + inner : 16 + inner] = jnp.zeros((8, rows), F32)
        across[k, 8 : 8 + inner] = 0.5 * along[k, planes : planes + inner] + 0.25 * (
            along[k, 0:inner] + along[k, 2 * planes : 2 * planes + inner]
        )
        for c in range(columns + 4):
            start = 8 + c * planes
            out_ref[k, (c + 1) * extent : (c + 2) * extent] = (
                weights[0] * across[k, start - 2 : start - 2 + extent]
                + weights[1] * across[k, start - 1 : start - 1 + extent]
                + weights[2] * across[k, start : start + extent]
            )


def equilibrium_pairs(density, velocity):
    squared = velocity[0] * velocity[0] + velocity[1] * velocity[1] + velocity[2] * velocity[2]
    base = 1.0 - 1.5 * squared
    result = [None] * 19
    result[0] = LATTICE_WEIGHTS[0] * density * base
    scaled = {w: w * density for w in (1.0 / 18.0, 1.0 / 36.0)}
    for q in range(1, 19, 2):
        projected = None
        for c, v in zip(LATTICE_VECTORS[q], velocity):
            if c == 0:
                continue
            if projected is None:
                projected = v if c == 1 else -v
            else:
                projected = projected + v if c == 1 else projected - v
        even = base + 4.5 * projected * projected
        odd = 3.0 * projected
        weight = scaled[LATTICE_WEIGHTS[q]]
        result[q] = weight * (even + odd)
        result[q + 1] = weight * (even - odd)
    return result


def moments_of(fields):
    density = functools.reduce(lambda a, b: a + b, fields)
    momentum = []
    for k in range(3):
        plus = [fields[q] for q in range(19) if LATTICE_VECTORS[q][k] == 1]
        minus = [fields[q] for q in range(19) if LATTICE_VECTORS[q][k] == -1]
        momentum.append(functools.reduce(lambda a, b: a + b, [a - b for a, b in zip(plus, minus)]))
    return density, momentum


def collide(fields, rate, pushed):
    sums = [fields[q] + fields[q + 1] for q in range(1, 19, 2)]
    gaps = [fields[q] - fields[q + 1] for q in range(1, 19, 2)]
    density = functools.reduce(lambda a, b: a + b, sums) + fields[0]
    scale = 3.0 / density
    tripled = []
    for k in range(3):
        total = pushed[k]
        for pair in range(9):
            c = LATTICE_VECTORS[2 * pair + 1][k]
            if c:
                total = total + gaps[pair] if c == 1 else total - gaps[pair]
        tripled.append(total * scale)
    squared = tripled[0] * tripled[0] + tripled[1] * tripled[1] + tripled[2] * tripled[2]
    base = 1.0 - (1.0 / 6.0) * squared
    fluid = rate > 0.0
    keep = 1.0 - rate
    strength = rate * density
    scaled = {w: w * strength for w in (1.0 / 18.0, 1.0 / 36.0)}
    result = [None] * 19
    rest = keep * fields[0] + (LATTICE_WEIGHTS[0] * strength) * base
    result[0] = jnp.where(fluid, rest, fields[0])
    for q in range(1, 19, 2):
        projected = None
        for c, v in zip(LATTICE_VECTORS[q], tripled):
            if c == 0:
                continue
            if projected is None:
                projected = v if c == 1 else -v
            else:
                projected = projected + v if c == 1 else projected - v
        weight = scaled[LATTICE_WEIGHTS[q]]
        even = weight * (base + 0.5 * projected * projected)
        odd = weight * projected
        result[q] = jnp.where(fluid, keep * fields[q] + (even + odd), fields[q + 1])
        result[q + 1] = jnp.where(fluid, keep * fields[q + 1] + (even - odd), fields[q])
    return result


def lattice_kernel(
    slabs, crosses,
    tri_hbm, pop_hbm, relax_hbm, fluid_hbm, pos_hbm, ten_hbm, coarse_hbm, face_hbm,
    next_ref,
    tri_ref, pop_ref, relax_ref, fluid_ref, pos_ref, ten_ref, coarse_ref, face_ref,
    xs, inc, nodal, cell_ref, lane_ref, acc, along, across,
    raw, own_force, far_force, pushed, placed_ref, rim, post_one, post_two, post_three,
    coarse_all, table, faces,
    zsend, zrecv, xsend, xrecv, csend, crecv,
    load_sems, coarse_sems, raw_sems, force_sems, face_sems, halo_sems,
):
    _, plane_count, columns, rows = pop_ref.shape
    extent, wide = plane_count + 2 * HALO, columns + 2 * HALO
    slab = lax.axis_index("slab")
    cross = lax.axis_index("cross")

    def beside(direction, sign):
        dz, dx = direction[0] * sign, direction[1] * sign
        conditions = []
        if dz == 1:
            conditions.append(slab < slabs - 1)
        if dz == -1:
            conditions.append(slab > 0)
        if dx == 1:
            conditions.append(cross < crosses - 1)
        if dx == -1:
            conditions.append(cross > 0)
        return functools.reduce(jnp.logical_and, conditions)

    def target(direction):
        return {"slab": slab + direction[0], "cross": cross + direction[1]}

    def cubed(ref):
        return ref.reshape(ref.shape[0], wide + 2, extent, rows)

    def spans(step, size, depth):
        if step == 1:
            return HALO + size - depth, HALO - depth, depth
        if step == -1:
            return HALO, HALO + size, depth
        return HALO, HALO, size

    def block_copy(ref, sems, index, depth):
        dz, dx = DIRECTIONS[index]
        z_from, z_to, z_size = spans(dz, plane_count, depth)
        x_from, x_to, x_size = spans(dx, columns, depth)
        whole = cubed(ref)
        return pltpu.make_async_remote_copy(
            src_ref=whole.at[:, pl.ds(1 + x_from, x_size), pl.ds(z_from, z_size)],
            dst_ref=whole.at[:, pl.ds(1 + x_to, x_size), pl.ds(z_to, z_size)],
            send_sem=sems.at[0, index],
            recv_sem=sems.at[1, index],
            device_id=target(DIRECTIONS[index]),
            device_id_type=MESH,
        )

    def column_rows(c):
        return pl.ds((c + 1) * extent, extent)

    def plane_rows(p, dz=0, dx=0):
        return pl.ds((HALO + 1 - dx) * extent + HALO + p - dz, columns, stride=extent)

    loads = [
        pltpu.make_async_copy(source, sink, load_sems.at[i])
        for i, (source, sink) in enumerate(
            (
                (tri_hbm, tri_ref),
                (pop_hbm, pop_ref),
                (relax_hbm, relax_ref),
                (fluid_hbm, fluid_ref),
                (pos_hbm, pos_ref),
                (ten_hbm, ten_ref),
                (coarse_hbm, coarse_ref),
                (face_hbm, face_ref),
            )
        )
    ]
    for load in loads:
        load.start()

    barrier = pltpu.get_barrier_semaphore()

    @pl.loop(1, slabs)
    def _(d):
        peer = lax.rem(slab + d, slabs)
        pl.semaphore_signal(
            barrier, inc=1, device_id={"slab": peer, "cross": cross}, device_id_type=MESH
        )

    expected = slabs - 1
    for direction in DIRECTIONS:
        if direction[1] == 0:
            continue
        there = beside(direction, 1)
        expected = expected + jnp.where(there, 1, 0)

        @pl.when(there)
        def _():
            pl.semaphore_signal(
                barrier, inc=1, device_id=target(direction), device_id_type=MESH
            )

    def clear(side):
        dz, dx = DIRECTIONS[side]
        for c in range(-1, wide + 1):
            if dx == 1 and c >= HALO or dx == -1 and c < HALO + columns:
                continue
            start = (c + 1) * extent
            if dz == 1:
                start, size = start, HALO
            elif dz == -1:
                start, size = start + HALO + plane_count, HALO
            else:
                size = extent
            for q in range(20):
                raw[q, pl.ds(start, size), :] = jnp.zeros((size, rows), F32)
        if dx == 0:
            zrecv[side] = jnp.zeros(zrecv.shape[1:], F32)
            near = 0 if dz == 1 else extent // 2
            for c in range(wide):
                for k in range(3):
                    far_force[k, pl.ds((c + 1) * extent + near, extent // 2), :] = jnp.zeros(
                        (extent // 2, rows), F32
                    )
        else:
            xrecv[side - 2] = jnp.zeros(xrecv.shape[1:], F32)

    for side in range(4):

        @pl.when(jnp.logical_not(beside(DIRECTIONS[side], -1)))
        def _():
            clear(side)

    for index in range(8):

        @pl.when(jnp.logical_not(beside(DIRECTIONS[index], -1)))
        def _():
            faces[index] = jnp.full(faces.shape[1:], -1, I32)
            if index >= 4:
                crecv[index - 4] = jnp.zeros(crecv.shape[1:], F32)

    loads[0].wait()
    incidence_stage(tri_ref, inc, pos_ref.shape[2])
    loads[6].wait()
    pl.semaphore_wait(barrier, expected)

    coarse_all[slab] = coarse_ref[...]

    def coarse_copy(d):
        return pltpu.make_async_remote_copy(
            src_ref=coarse_ref,
            dst_ref=coarse_all.at[slab],
            send_sem=coarse_sems.at[0, d],
            recv_sem=coarse_sems.at[1, d],
            device_id={"slab": lax.rem(slab + d, slabs), "cross": cross},
            device_id_type=MESH,
        )

    @pl.loop(1, slabs)
    def _(d):
        coarse_copy(d).start()

    loads[7].wait()

    def face_copy(index):
        return pltpu.make_async_remote_copy(
            src_ref=face_ref,
            dst_ref=faces.at[index],
            send_sem=face_sems.at[0, index],
            recv_sem=face_sems.at[1, index],
            device_id=target(DIRECTIONS[index]),
            device_id_type=MESH,
        )

    for index in (4, 5, 6, 7, 0, 1, 2, 3):

        @pl.when(beside(DIRECTIONS[index], 1))
        def _():
            face_copy(index).start()

    for load in loads[1:4]:
        load.wait()
    for p in range(plane_count):
        for q in range(19):
            raw[q, plane_rows(p), :] = pop_ref[q, p]
        raw[19, plane_rows(p), :] = jnp.where(fluid_ref[p] == 1, relax_ref[p], 0.0)
    for index in (4, 5, 6, 7, 0, 1, 2, 3):

        @pl.when(beside(DIRECTIONS[index], 1))
        def _():
            block_copy(raw, raw_sems, index, HALO).start()

    for load in loads[4:6]:
        load.wait()
    nodal_stage(
        plane_count, columns, rows, pos_ref, ten_ref, inc, xs, cell_ref, lane_ref, nodal
    )
    spread_stage(plane_count, columns, cell_ref, lane_ref, nodal, acc, along, across, own_force)

    def force_copy(index):
        part = extent // 2
        start = part if index == 0 else 0
        return pltpu.make_async_remote_copy(
            src_ref=cubed(own_force).at[:, pl.ds(1, wide), pl.ds(start, part)],
            dst_ref=cubed(far_force).at[:, pl.ds(1, wide), pl.ds(part - start, part)],
            send_sem=force_sems.at[0, index],
            recv_sem=force_sems.at[1, index],
            device_id=target(DIRECTIONS[index]),
            device_id_type=MESH,
        )

    for index in range(2):

        @pl.when(beside(DIRECTIONS[index], 1))
        def _():
            force_copy(index).start()

    @pl.loop(1, slabs)
    def _(d):
        pltpu.make_async_remote_copy(
            src_ref=coarse_ref,
            dst_ref=coarse_all.at[lax.rem(slab + slabs - d, slabs)],
            send_sem=coarse_sems.at[0, d],
            recv_sem=coarse_sems.at[1, d],
            device_id={"slab": lax.rem(slab + d, slabs), "cross": cross},
            device_id_type=MESH,
        ).wait_recv()

    for index in range(8):

        @pl.when(beside(DIRECTIONS[index], -1))
        def _():
            face_copy(index).wait_recv()

    slots = face_ref.shape[1]
    lanes = table.shape[1]
    chunks = coarse_ref.shape[1] // lanes
    together = table.shape[0] // (4 * chunks)
    groups = [[face_ref[pl.ds(k, 1), :] for k in range(3)]] + [
        [faces[index, pl.ds(k, 1), :] for k in range(3)] for index in range(8)
    ]
    wanted = [jnp.concatenate(group[1:], axis=1) for group in groups]
    one, zero = jnp.ones((), BF16), jnp.zeros((), BF16)
    picks = [
        jnp.where(
            lax.broadcasted_iota(I16, (lanes, 2 * slots), 0) == (index & (lanes - 1)).astype(I16),
            one, zero,
        )
        for index in wanted
    ]
    quarter = lax.shift_right_logical(
        lax.broadcasted_iota(I32, (table.shape[0], 2 * slots), 0), 2
    )

    def gather(base, found):
        for j in range(together):
            for chunk in range(chunks):
                table[pl.ds((j * chunks + chunk) * 4, 4), :] = coarse_all[
                    base * together + j, :, chunk * lanes : (chunk + 1) * lanes
                ]
        stacked = jnp.concatenate(split(table[...], 2), axis=0).astype(BF16)
        result = []
        for index, pick, total in zip(wanted, picks, found):
            both = jnp.dot(stacked, pick, preferred_element_type=F32)
            both = both[: table.shape[0]] + both[table.shape[0] :]
            high = lax.shift_right_logical(index, lanes.bit_length() - 1)
            both = jnp.where(quarter == high - base * (together * chunks), both, 0.0)
            for start in range(0, table.shape[0], 8):
                total = total + both[start : start + 8]
            result.append(total)
        return tuple(result)

    found = tuple(jnp.zeros((8, 2 * slots), F32) for _ in groups)
    if coarse_all.shape[0] == together:
        found = gather(0, found)
    else:
        found = lax.fori_loop(0, coarse_all.shape[0] // together, gather, found)
    blended = []
    for total in found:
        total = total[0:4] + total[4:8]
        blended.append(0.75 * total[:, :slots] + 0.25 * total[:, slots:])

    def spots(group):
        cell = group[0]
        used = cell >= 0
        line = cell // rows
        return used, line // columns, line % columns, jnp.where(used, cell % rows, -1)

    def put(size, goals, lane_rows, moments):
        mask = [lax.broadcasted_iota(I32, (size, slots), 0) == goal for goal in goals]
        pieces = [split(value, 2) for value in moments]
        left = [
            jnp.concatenate(
                [jnp.where(m, piece[part][k : k + 1], 0.0) for m, piece in zip(mask, pieces)], axis=1
            )
            for k in range(4)
            for part in range(2)
        ]
        left.append(jnp.concatenate([jnp.where(m, 1.0, 0.0) for m in mask], axis=1))
        right = jnp.concatenate(
            [
                jnp.where(lax.broadcasted_iota(I32, (rows, slots), 0) == lane, 1.0, 0.0)
                for lane in lane_rows
            ],
            axis=1,
        )
        out = lax.dot_general(
            jnp.concatenate(left, axis=0).astype(BF16), right.astype(BF16), NT,
            preferred_element_type=F32,
        )
        return [
            out[2 * k * size : (2 * k + 1) * size] + out[(2 * k + 1) * size : (2 * k + 2) * size]
            for k in range(4)
        ] + [out[8 * size : 9 * size]]

    used, plane, column, lane = spots(groups[0])
    goal = jnp.where(used, column * plane_count + plane, -1)
    for k, value in enumerate(put(columns * plane_count, [goal], [lane], blended[:1])):
        for c in range(columns):
            placed_ref[k, pl.ds((HALO + 1 + c) * extent + HALO, plane_count), :] = value[
                c * plane_count : (c + 1) * plane_count
            ]

    goals, lane_rows, offsets, offset = [], [], [], 0
    for index, (dz, dx) in enumerate(DIRECTIONS):
        used, plane, column, lane = spots(groups[1 + index])
        if dz:
            used = used & (plane == (plane_count - 1 if dz == 1 else 0))
        if dx:
            used = used & (column == (columns - 1 if dx == 1 else 0))
        along_edge = column if dx == 0 else plane if dz == 0 else jnp.zeros_like(plane)
        goals.append(jnp.where(used, along_edge + offset, -1))
        lane_rows.append(lane)
        offsets.append(offset)
        offset += columns if dx == 0 else plane_count if dz == 0 else 1
    for k, value in enumerate(put(round_up(offset, 16), goals, lane_rows, blended[1:])):
        for index, (dz, dx) in enumerate(DIRECTIONS):
            size = columns if dx == 0 else plane_count if dz == 0 else 1
            part = value[offsets[index] : offsets[index] + size]
            if k == 4:
                part = jnp.where(beside(DIRECTIONS[index], -1), part, 1.0)
            p = -1 if dz == 1 else plane_count
            c = HALO + (-1 if dx == 1 else columns)
            if dx == 0:
                placed_ref[k, plane_rows(p), :] = part
            elif dz == 0:
                placed_ref[k, pl.ds((c + 1) * extent + HALO, plane_count), :] = part
            else:
                placed_ref[k, pl.ds((c + 1) * extent + HALO + p, 1), :] = part

    for c in range(1, wide - 1):
        at = column_rows(c)
        density = placed_ref[0, at, :]
        velocity = [placed_ref[k, at, :] for k in range(1, 4)]
        for q, value in enumerate(equilibrium_pairs(density, velocity)):
            rim[q, at, :] = value

    for index in range(2):

        @pl.when(beside(DIRECTIONS[index], -1))
        def _():
            force_copy(index).wait_recv()

    for index in range(8):

        @pl.when(beside(DIRECTIONS[index], -1))
        def _():
            block_copy(raw, raw_sems, index, HALO).wait_recv()

    def pulled(source, at, starts):
        fixed = placed_ref[4, at, :] > 0.5
        fields = []
        for q, (cz, cx, cy) in enumerate(LATTICE_VECTORS):
            value = source[q, starts(cz, cx), :]
            if cy != 0:
                value = pltpu.roll(value, cy % rows, 1)
            fields.append(jnp.where(fixed, rim[q, at, :], value))
        return fields

    def pulled_column(source, c):
        return pulled(
            source,
            column_rows(c),
            lambda cz, cx: pl.ds((c + 1 - cx) * extent - cz, extent),
        )

    def pulled_plane(source, p):
        return pulled(source, plane_rows(p), lambda cz, cx: plane_rows(p, cz, cx))

    for c in range(wide):
        at = column_rows(c)
        rate = raw[19, at, :]
        fluid = rate > 0.0
        inverse = 1.0 / rate
        push = []
        for k in range(3):
            value = jnp.where(fluid, (own_force[k, at, :] + far_force[k, at, :]) * inverse, 0.0)
            pushed[k, at, :] = value
            push.append(value)
        for q, value in enumerate(collide([raw[q, at, :] for q in range(19)], rate, push)):
            post_one[q, at, :] = value

    def collide_columns(source, sink):
        for c in range(1, wide - 1):
            at = column_rows(c)
            fields = pulled_column(source, c)
            push = [pushed[k, at, :] for k in range(3)]
            for q, value in enumerate(collide(fields, raw[19, at, :], push)):
                sink[q, at, :] = value

    collide_columns(post_one, post_two)

    for p in range(plane_count):
        at = plane_rows(p)
        fields = pulled_plane(post_two, p)
        push = [pushed[k, at, :] for k in range(3)]
        for q, value in enumerate(collide(fields, raw[19, at, :], push)):
            post_three[q, at, :] = value
            for side in range(2):
                depth = plane_count - p if side == 0 else p + 1
                if (q, depth) in SLAB_MOVES[side]:
                    zsend[side, SLAB_MOVES[side].index((q, depth))] = value

    def inner_row(step, depth, size):
        return HALO + (size - depth if step == 1 else depth - 1)

    def outer_row(step, depth, size):
        return HALO + (-depth if step == 1 else size - 1 + depth)

    for side in range(4):
        for e, (q, dz, dx) in enumerate(CORNER_MOVES[side]):
            sz, sx = DIRECTIONS[4 + side]
            row = (inner_row(sx, dx, columns) + 1) * extent + inner_row(sz, dz, plane_count)
            csend[side, pl.ds(e, 1), :] = post_three[q, pl.ds(row, 1), :]
    for side in range(2):
        for e, (q, depth) in enumerate(CROSS_MOVES[side]):
            row = (inner_row(DIRECTIONS[2 + side][1], depth, columns) + 1) * extent + HALO
            xsend[side, pl.ds(e * plane_count, plane_count), :] = post_three[
                q, pl.ds(row, plane_count), :
            ]

    def halo_copy(index):
        if index < 2:
            source, sink = zsend.at[index], zrecv.at[index]
        elif index < 4:
            source, sink = xsend.at[index - 2], xrecv.at[index - 2]
        else:
            source, sink = csend.at[index - 4], crecv.at[index - 4]
        return pltpu.make_async_remote_copy(
            src_ref=source,
            dst_ref=sink,
            send_sem=halo_sems.at[0, index],
            recv_sem=halo_sems.at[1, index],
            device_id=target(DIRECTIONS[index]),
            device_id_type=MESH,
        )

    for index in (4, 5, 6, 7, 0, 1, 2, 3):

        @pl.when(beside(DIRECTIONS[index], 1))
        def _():
            halo_copy(index).start()

    for index in range(8):

        @pl.when(beside(DIRECTIONS[index], -1))
        def _():
            halo_copy(index).wait_recv()

    for side in range(2):
        for e, (q, depth) in enumerate(SLAB_MOVES[side]):
            row = outer_row(DIRECTIONS[side][0], depth, plane_count)
            post_three[q, plane_rows(row - HALO), :] = zrecv[side, e]
        for e, (q, depth) in enumerate(CROSS_MOVES[side]):
            row = (outer_row(DIRECTIONS[2 + side][1], depth, columns) + 1) * extent + HALO
            post_three[q, pl.ds(row, plane_count), :] = xrecv[
                side, pl.ds(e * plane_count, plane_count), :
            ]
    for side in range(4):
        for e, (q, dz, dx) in enumerate(CORNER_MOVES[side]):
            sz, sx = DIRECTIONS[4 + side]
            row = (outer_row(sx, dx, columns) + 1) * extent + outer_row(sz, dz, plane_count)
            post_three[q, pl.ds(row, 1), :] = crecv[side, pl.ds(e, 1), :]

    collide_columns(post_three, post_one)

    for p in range(plane_count):
        for q, value in enumerate(pulled_plane(post_one, p)):
            next_ref[q, p] = value

    @pl.loop(1, slabs)
    def _(d):
        coarse_copy(d).wait_send()

    for index in range(8):

        @pl.when(beside(DIRECTIONS[index], 1))
        def _():
            block_copy(raw, raw_sems, index, HALO).wait_send()
            face_copy(index).wait_send()
            halo_copy(index).wait_send()
            if index < 2:
                force_copy(index).wait_send()


def flow_kernel(fields_ref, next_ref, flow_ref, flow, sems):
    whole = pltpu.make_async_copy(fields_ref, next_ref, sems.at[0])
    whole.start()
    for p in range(fields_ref.shape[1]):
        fields = [fields_ref[q, p] for q in range(19)]
        density, momentum = moments_of(fields)
        inverse = ROOT_THREE / density
        for k in range(3):
            flow[k, p] = momentum[k] * inverse
    part = pltpu.make_async_copy(flow, flow_ref, sems.at[1])
    part.start()
    whole.wait()
    part.wait()


def coarse_rows(slabs, coarse_moments):
    count, width = coarse_moments.shape
    return math.gcd(slabs, 8) * count * (width // 128)


def on_device(
    slabs, crosses,
    populations, fluid_mask, relaxation, positions, triangles, tension, coarse_moments, interface,
):
    _, plane_count, columns, rows = populations.shape
    _, membranes, nodes = positions.shape
    padded = round_up(nodes, 128)
    corners = triangles.shape[1]
    half, planes = (columns + 6) // 2, plane_count + 2
    cells = round_up(planes * half, 16)
    flat = (columns + 2 * HALO + 2) * (plane_count + 2 * HALO)
    vmem = pl.BlockSpec(memory_space=pltpu.VMEM)
    block = (19, plane_count, columns, rows)
    operands = (
        triangles, populations, relaxation, fluid_mask, positions, tension, coarse_moments, interface,
    )
    fields = pl.pallas_call(
        functools.partial(lattice_kernel, slabs, crosses),
        name="lattice_steps",
        out_shape=pltpu.VMEM(block, F32),
        in_specs=[pl.BlockSpec(memory_space=pl.ANY)] * 8,
        out_specs=vmem,
        scratch_shapes=[pltpu.VMEM(operand.shape, operand.dtype) for operand in operands]
        + [
            pltpu.VMEM((3, membranes, padded), F32),
            pltpu.VMEM((padded, corners), BF16),
            pltpu.VMEM((3, membranes, padded), F32),
            pltpu.VMEM((membranes, padded), I32),
            pltpu.VMEM((membranes, padded), I32),
            pltpu.VMEM((6 * cells, 2 * rows), F32),
            pltpu.VMEM((3, half * planes + cells, rows), F32),
            pltpu.VMEM((3, (columns + 4) * planes + 16, rows), F32),
            pltpu.VMEM((20, flat, rows), F32),
            pltpu.VMEM((3, flat, rows), F32),
            pltpu.VMEM((3, flat, rows), F32),
            pltpu.VMEM((3, flat, rows), F32),
            pltpu.VMEM((5, flat, rows), F32),
            pltpu.VMEM((19, flat, rows), F32),
            pltpu.VMEM((19, flat, rows), F32),
            pltpu.VMEM((19, flat, rows), F32),
            pltpu.VMEM((19, flat, rows), F32),
            pltpu.VMEM((slabs,) + coarse_moments.shape, F32),
            pltpu.VMEM((coarse_rows(slabs, coarse_moments), 128), F32),
            pltpu.VMEM((8,) + interface.shape, I32),
            pltpu.VMEM((2, 19, columns, rows), F32),
            pltpu.VMEM((2, 19, columns, rows), F32),
            pltpu.VMEM((2, round_up(19 * plane_count, 8), rows), F32),
            pltpu.VMEM((2, round_up(19 * plane_count, 8), rows), F32),
            pltpu.VMEM((4, 24, rows), F32),
            pltpu.VMEM((4, 24, rows), F32),
            pltpu.SemaphoreType.DMA((8,)),
            pltpu.SemaphoreType.DMA((2, slabs)),
            pltpu.SemaphoreType.DMA((2, 8)),
            pltpu.SemaphoreType.DMA((2, 2)),
            pltpu.SemaphoreType.DMA((2, 8)),
            pltpu.SemaphoreType.DMA((2, 8)),
        ],
        compiler_params=pltpu.CompilerParams(collective_id=0, has_side_effects=True),
    )(*operands)
    return pl.pallas_call(
        flow_kernel,
        name="flow",
        out_shape=(
            jax.ShapeDtypeStruct(block, F32),
            jax.ShapeDtypeStruct((3,) + block[1:], F32),
        ),
        in_specs=[vmem],
        out_specs=(pl.BlockSpec(memory_space=pl.ANY),) * 2,
        scratch_shapes=[pltpu.VMEM((3,) + block[1:], F32), pltpu.SemaphoreType.DMA((2,))],
    )(pltpu.with_memory_space_constraint(fields, pltpu.VMEM))


def solution(mesh):
    in_specs = (
        P(None, "slab", "cross", None),
        P("slab", "cross", None),
        P("slab", "cross", None),
        P(None, "slab", None),
        P(),
        P("slab", None),
        P(None, "slab"),
        P(None, ("slab", "cross")),
    )
    out_specs = (P(None, "slab", "cross", None), P(None, "slab", "cross", None))
    return jax.shard_map(
        functools.partial(on_device, mesh.shape["slab"], mesh.shape["cross"]),
        mesh=mesh, in_specs=in_specs, out_specs=out_specs, check_vma=False,
    )
```

```python
import functools
import math

import jax
import jax.numpy as jnp
from jax import lax
from jax.experimental import pallas as pl
from jax.experimental.pallas import tpu as pltpu
from jax.sharding import PartitionSpec as P

STEPS = 4
MESH = pl.DeviceIdType.MESH
LATTICE_VECTORS = [
    (0, 0, 0),
    (1, 0, 0),
    (-1, 0, 0),
    (0, 1, 0),
    (0, -1, 0),
    (0, 0, 1),
    (0, 0, -1),
    (1, 1, 0),
    (-1, -1, 0),
    (1, -1, 0),
    (-1, 1, 0),
    (1, 0, 1),
    (-1, 0, -1),
    (1, 0, -1),
    (-1, 0, 1),
    (0, 1, 1),
    (0, -1, -1),
    (0, 1, -1),
    (0, -1, 1),
]
LATTICE_WEIGHTS = [1.0 / 3.0] + [1.0 / 18.0] * 6 + [1.0 / 36.0] * 12
OPPOSITE = [0] + [q + 1 if q % 2 == 1 else q - 1 for q in range(1, 19)]
ROOT_THREE = math.sqrt(3.0)
DIRECTIONS = [(1, 0), (-1, 0), (0, 1), (0, -1), (1, 1), (-1, -1), (1, -1), (-1, 1)]
NT = (((1,), (1,)), ((), ()))
F32, BF16, I32, I16 = jnp.float32, jnp.bfloat16, jnp.int32, jnp.int16
HALO = 2


def slab_moves(extra):
    return [
        [
            (q, depth)
            for depth in (1, 2)
            for q in [m for m in range(19) if LATTICE_VECTORS[m][0] * sign >= depth - 1] + extra
        ]
        for sign in (1, -1)
    ]


def cross_moves(extra):
    return [
        [
            (q, depth)
            for depth in (1, 2)
            for q in [m for m in range(19) if LATTICE_VECTORS[m][1] * sign >= depth - 1] + extra
        ]
        for sign in (1, -1)
    ]


def corner_moves(extra):
    return [
        [
            (q, dz, dx)
            for dz in (1, 2)
            for dx in (1, 2)
            for q in [
                m
                for m in range(19)
                if LATTICE_VECTORS[m][0] * sz >= dz - 1 and LATTICE_VECTORS[m][1] * sx >= dx - 1
            ]
            + extra
        ]
        for sz, sx in DIRECTIONS[4:]
    ]


RATE, DENSITY, MOMENTUM, CHANNELS = 19, 20, 21, 24
MOVES = (slab_moves([]), cross_moves([]), corner_moves([]))
EXTRA = list(range(19, CHANNELS))
RAW_MOVES = (slab_moves(EXTRA), cross_moves(EXTRA), corner_moves(EXTRA))


def buffer_shapes(moves, plane_count, columns, rows):
    return [
        (2, len(moves[0][0]), columns, rows),
        (2, round_up(len(moves[1][0]) * plane_count, 8), rows),
        (4, round_up(len(moves[2][0]), 8), rows),
    ]


def round_up(value, unit):
    return (value + unit - 1) // unit * unit


def split(value, parts):
    pieces = []
    for _ in range(parts):
        piece = value.astype(BF16).astype(F32)
        pieces.append(piece)
        value = value - piece
    return pieces


def incidence_stage(tri_ref, inc, nodes):
    triangles = tri_ref.shape[1]
    tiles = triangles // 128
    corners = [
        [
            jnp.broadcast_to(tri_ref[pl.ds(k, 1), t * 128 : (t + 1) * 128], (16, 128)).astype(I16)
            for t in range(tiles)
        ]
        for k in range(3)
    ]
    iota = lax.broadcasted_iota(I32, (16, 128), 0)

    def rows_at(start):
        ids = (iota + start).astype(I16)
        for t in range(tiles):
            hit = (ids == corners[0][t]) | (ids == corners[1][t]) | (ids == corners[2][t])
            inc[pl.ds(start, 16), t * 128 : (t + 1) * 128] = jnp.where(
                hit, jnp.ones((), BF16), jnp.zeros((), BF16)
            )

    chunk = 128

    @pl.loop(0, nodes // chunk)
    def _(i):
        for r in range(chunk // 16):
            rows_at(pl.multiple_of(i * chunk + r * 16, 16))

    done = nodes // chunk * chunk
    while done < nodes:
        rows_at(done)
        done += 16
    if done < inc.shape[0]:
        inc[done:, :] = jnp.zeros((inc.shape[0] - done, triangles), BF16)


def nodal_stage(plane_count, columns, rows, pos_ref, ten_ref, inc, xs, cell_ref, lane_ref, force):
    dims, membranes, nodes = pos_ref.shape
    padded = xs.shape[2]
    slab = lax.axis_index("slab")
    cross = lax.axis_index("cross")
    planes, half = plane_count + 2, (columns + 6) // 2

    cell_ref[...] = jnp.full(cell_ref.shape, -1, I32)
    lane_ref[...] = jnp.full(lane_ref.shape, -1, I32)
    plane = pos_ref[0] - (slab * plane_count - 1)
    column = pos_ref[1] - (cross * columns - 3)
    row = pos_ref[2]
    inside = (column >= 0) & (column < 2 * half)
    upper = column >= half
    cell = jnp.where(upper, column - half, column) * planes + plane
    cell_ref[:, :nodes] = jnp.where(inside, cell, -1)
    lane_ref[:, :nodes] = row + jnp.where(upper, rows, 0)

    xs[...] = jnp.zeros_like(xs)
    for k in range(3):
        xs[k, :, :nodes] = (pos_ref[k] - pos_ref[k, :, 0:1]).astype(F32)

    coords = xs[...].reshape(dims * membranes, padded)
    sums = jnp.dot(coords.astype(BF16), inc[...], preferred_element_type=F32)
    tension = ten_ref[...]
    terms = jnp.concatenate(
        [sums[k * membranes : (k + 1) * membranes] * tension for k in range(3)] + [tension], axis=0
    )
    stacked = jnp.concatenate(split(terms, 2), axis=0).astype(BF16)
    gathered = lax.dot_general(stacked, inc[...], NT, preferred_element_type=F32)
    count = terms.shape[0]
    total = gathered[:count] + gathered[count:]
    weight = total[3 * membranes :]
    for k in range(3):
        force[k] = total[k * membranes : (k + 1) * membranes] - 3.0 * xs[k] * weight


def spread_stage(plane_count, columns, cell_ref, lane_ref, force, acc, along, across, out_ref):
    _, membranes, padded = force.shape
    rows = out_ref.shape[2]
    planes, half = plane_count + 2, (columns + 6) // 2
    extent = plane_count + 2 * HALO
    cells = acc.shape[0] // 6
    acc[...] = jnp.zeros_like(acc)
    unroll = 4 if membranes % 4 == 0 else 1
    zero, one = jnp.zeros((), BF16), jnp.ones((), BF16)

    @pl.loop(0, membranes // unroll)
    def _(i):
        running = None
        for inner in range(unroll):
            m = pl.ds(i * unroll + inner, 1)
            cell = cell_ref[m, :].astype(I16)
            lane = lane_ref[m, :].astype(I16)
            mask = lax.broadcasted_iota(I16, (cells, padded), 0) == cell
            values = [split(force[k, m, :], 2) for k in range(3)]
            left = jnp.concatenate(
                [
                    jnp.where(mask, values[k][part].astype(BF16), zero)
                    for part in range(2)
                    for k in range(3)
                ],
                axis=0,
            )
            right = jnp.where(lax.broadcasted_iota(I16, (2 * rows, padded), 0) == lane, one, zero)
            product = lax.dot_general(left, right, NT, preferred_element_type=F32)
            running = product if running is None else running + product
        acc[...] += running

    used = half * planes
    inner = (columns + 4) * planes
    step = lax.broadcasted_iota(I32, (extent, rows), 0)
    weights = [
        jnp.where((step >= 2 - shift) & (step < planes + 2 - shift), w, 0.0)
        for shift, w in ((0, 0.25), (1, 0.5), (2, 0.25))
    ]
    for k in range(3):
        value = acc[k * cells : (k + 1) * cells] + acc[(3 + k) * cells : (4 + k) * cells]
        for part in range(2):
            b = value[:, part * rows : (part + 1) * rows]
            b = 0.5 * b + 0.25 * (pltpu.roll(b, 1, 1) + pltpu.roll(b, rows - 1, 1))
            along[k, part * used : part * used + cells] = b
        across[k, 0:8] = jnp.zeros((8, rows), F32)
        across[k, 8 + inner : 16 + inner] = jnp.zeros((8, rows), F32)
        across[k, 8 : 8 + inner] = 0.5 * along[k, planes : planes + inner] + 0.25 * (
            along[k, 0:inner] + along[k, 2 * planes : 2 * planes + inner]
        )
        for c in range(columns + 4):
            start = 8 + c * planes
            out_ref[k, (c + 1) * extent : (c + 2) * extent] = (
                weights[0] * across[k, start - 2 : start - 2 + extent]
                + weights[1] * across[k, start - 1 : start - 1 + extent]
                + weights[2] * across[k, start : start + extent]
            )


def equilibrium_pairs(density, velocity):
    squared = velocity[0] * velocity[0] + velocity[1] * velocity[1] + velocity[2] * velocity[2]
    base = 1.0 - 1.5 * squared
    result = [None] * 19
    result[0] = LATTICE_WEIGHTS[0] * density * base
    scaled = {w: w * density for w in (1.0 / 18.0, 1.0 / 36.0)}
    for q in range(1, 19, 2):
        projected = None
        for c, v in zip(LATTICE_VECTORS[q], velocity):
            if c == 0:
                continue
            if projected is None:
                projected = v if c == 1 else -v
            else:
                projected = projected + v if c == 1 else projected - v
        even = base + 4.5 * projected * projected
        odd = 3.0 * projected
        weight = scaled[LATTICE_WEIGHTS[q]]
        result[q] = weight * (even + odd)
        result[q + 1] = weight * (even - odd)
    return result


def moments_of(fields):
    density = functools.reduce(lambda a, b: a + b, fields)
    momentum = []
    for k in range(3):
        plus = [fields[q] for q in range(19) if LATTICE_VECTORS[q][k] == 1]
        minus = [fields[q] for q in range(19) if LATTICE_VECTORS[q][k] == -1]
        momentum.append(functools.reduce(lambda a, b: a + b, [a - b for a, b in zip(plus, minus)]))
    return density, momentum


def local_moments(fields):
    gaps = [fields[q] - fields[q + 1] for q in range(1, 19, 2)]
    sums = [fields[q] + fields[q + 1] for q in range(1, 19, 2)]
    density = functools.reduce(lambda a, b: a + b, sums) + fields[0]
    momentum = []
    for k in range(3):
        total = None
        for pair in range(9):
            c = LATTICE_VECTORS[2 * pair + 1][k]
            if c and total is None:
                total = gaps[pair]
            elif c:
                total = total + gaps[pair] if c == 1 else total - gaps[pair]
        momentum.append(total)
    return density, momentum


def pull_terms(density, momentum, rate, pushed, needed):
    scale = 3.0 / density
    tripled = [(m + p) * scale for m, p in zip(momentum, pushed)]
    squared = tripled[0] * tripled[0] + tripled[1] * tripled[1] + tripled[2] * tripled[2]
    base = 1.0 - (1.0 / 6.0) * squared
    strength = rate * density
    scaled = {w: w * strength for w in (1.0 / 18.0, 1.0 / 36.0)}
    result = [None] * 19
    result[0] = (LATTICE_WEIGHTS[0] * strength) * base
    for q in range(1, 19, 2):
        if q not in needed and q + 1 not in needed:
            continue
        projected = None
        for c, v in zip(LATTICE_VECTORS[q], tripled):
            if c == 0:
                continue
            if projected is None:
                projected = v if c == 1 else -v
            else:
                projected = projected + v if c == 1 else projected - v
        weight = scaled[LATTICE_WEIGHTS[q]]
        even = weight * (base + 0.5 * projected * projected)
        odd = weight * projected
        result[q] = even + odd
        result[q + 1] = even - odd
    return result


def collide(fields, rate, pushed, needed=range(19)):
    density, momentum = local_moments(fields)
    terms = pull_terms(density, momentum, rate, pushed, needed)
    fluid = rate > 0.0
    keep = 1.0 - rate
    return {q: jnp.where(fluid, keep * fields[q] + terms[q], fields[OPPOSITE[q]]) for q in needed}


def lattice_kernel(
    slabs, crosses,
    tri_hbm, pop_hbm, relax_hbm, fluid_hbm, pos_hbm, ten_hbm, coarse_hbm, face_hbm,
    next_ref,
    tri_ref, pop_ref, relax_ref, fluid_ref, pos_ref, ten_ref, coarse_ref, face_ref,
    xs, inc, nodal, cell_ref, lane_ref, acc, along, across,
    raw, own_force, far_force, pushed, placed_ref, rim, post_one, post_two, post_three,
    coarse_all, table, faces,
    zsend, xsend, csend, zrecv, xrecv, crecv,
    raw_zsend, raw_xsend, raw_csend, raw_zrecv, raw_xrecv, raw_crecv,
    load_sems, coarse_sems, raw_sems, force_sems, face_sems, halo_sems,
):
    _, plane_count, columns, rows = pop_ref.shape
    extent, wide = plane_count + 2 * HALO, columns + 2 * HALO
    slab = lax.axis_index("slab")
    cross = lax.axis_index("cross")

    def beside(direction, sign):
        dz, dx = direction[0] * sign, direction[1] * sign
        conditions = []
        if dz == 1:
            conditions.append(slab < slabs - 1)
        if dz == -1:
            conditions.append(slab > 0)
        if dx == 1:
            conditions.append(cross < crosses - 1)
        if dx == -1:
            conditions.append(cross > 0)
        return functools.reduce(jnp.logical_and, conditions)

    def target(direction):
        return {"slab": slab + direction[0], "cross": cross + direction[1]}

    def cubed(ref):
        return ref.reshape(ref.shape[0], wide + 2, extent, rows)

    def inner_row(step, depth, size):
        return HALO + (size - depth if step == 1 else depth - 1)

    def outer_row(step, depth, size):
        return HALO + (-depth if step == 1 else size - 1 + depth)

    def pack(source, moves, buffers):
        for side in range(4):
            sz, sx = DIRECTIONS[4 + side]
            for e, (q, dz, dx) in enumerate(moves[2][side]):
                row = (inner_row(sx, dx, columns) + 1) * extent + inner_row(sz, dz, plane_count)
                buffers[2][side, pl.ds(e, 1), :] = source[q, pl.ds(row, 1), :]
        for side in range(2):
            for e, (q, depth) in enumerate(moves[1][side]):
                row = (inner_row(DIRECTIONS[2 + side][1], depth, columns) + 1) * extent + HALO
                buffers[1][side, pl.ds(e * plane_count, plane_count), :] = source[
                    q, pl.ds(row, plane_count), :
                ]

    def unpack(sink, moves, buffers):
        for side in range(2):
            for e, (q, depth) in enumerate(moves[0][side]):
                row = outer_row(DIRECTIONS[side][0], depth, plane_count)
                sink[q, plane_rows(row - HALO), :] = buffers[0][side, e]
            for e, (q, depth) in enumerate(moves[1][side]):
                row = (outer_row(DIRECTIONS[2 + side][1], depth, columns) + 1) * extent + HALO
                sink[q, pl.ds(row, plane_count), :] = buffers[1][
                    side, pl.ds(e * plane_count, plane_count), :
                ]
        for side in range(4):
            sz, sx = DIRECTIONS[4 + side]
            for e, (q, dz, dx) in enumerate(moves[2][side]):
                row = (outer_row(sx, dx, columns) + 1) * extent + outer_row(sz, dz, plane_count)
                sink[q, pl.ds(row, 1), :] = buffers[2][side, pl.ds(e, 1), :]

    def keep_plane(q, p, value, moves, buffer):
        for side in range(2):
            entry = (q, plane_count - p if side == 0 else p + 1)
            if entry in moves[0][side]:
                buffer[side, moves[0][side].index(entry)] = value

    def buffers_copy(sources, sinks, sems, index):
        kind, place = (0, index) if index < 2 else (1, index - 2) if index < 4 else (2, index - 4)
        return pltpu.make_async_remote_copy(
            src_ref=sources[kind].at[place],
            dst_ref=sinks[kind].at[place],
            send_sem=sems.at[0, index],
            recv_sem=sems.at[1, index],
            device_id=target(DIRECTIONS[index]),
            device_id_type=MESH,
        )

    def halo_copy(index):
        return buffers_copy((zsend, xsend, csend), (zrecv, xrecv, crecv), halo_sems, index)

    def raw_copy(index):
        return buffers_copy(
            (raw_zsend, raw_xsend, raw_csend), (raw_zrecv, raw_xrecv, raw_crecv), raw_sems, index
        )

    def column_rows(c):
        return pl.ds((c + 1) * extent, extent)

    def plane_rows(p, dz=0, dx=0):
        return pl.ds((HALO + 1 - dx) * extent + HALO + p - dz, columns, stride=extent)

    loads = [
        pltpu.make_async_copy(source, sink, load_sems.at[i])
        for i, (source, sink) in enumerate(
            (
                (tri_hbm, tri_ref),
                (pop_hbm, pop_ref),
                (relax_hbm, relax_ref),
                (fluid_hbm, fluid_ref),
                (pos_hbm, pos_ref),
                (ten_hbm, ten_ref),
                (coarse_hbm, coarse_ref),
                (face_hbm, face_ref),
            )
        )
    ]
    for load in loads:
        load.start()

    barrier = pltpu.get_barrier_semaphore()

    @pl.loop(1, slabs)
    def _(d):
        peer = lax.rem(slab + d, slabs)
        pl.semaphore_signal(
            barrier, inc=1, device_id={"slab": peer, "cross": cross}, device_id_type=MESH
        )

    expected = slabs - 1
    for direction in DIRECTIONS:
        if direction[1] == 0:
            continue
        there = beside(direction, 1)
        expected = expected + jnp.where(there, 1, 0)

        @pl.when(there)
        def _():
            pl.semaphore_signal(
                barrier, inc=1, device_id=target(direction), device_id_type=MESH
            )

    def clear(side):
        kind, place = (0, side) if side < 2 else (1, side - 2) if side < 4 else (2, side - 4)
        for sinks in ((zrecv, xrecv, crecv), (raw_zrecv, raw_xrecv, raw_crecv)):
            sinks[kind][place] = jnp.zeros(sinks[kind].shape[1:], F32)
        faces[side] = jnp.full(faces.shape[1:], -1, I32)
        if side < 2:
            near = side * (extent // 2)
            for c in range(wide):
                for k in range(3):
                    far_force[k, pl.ds((c + 1) * extent + near, extent // 2), :] = jnp.zeros(
                        (extent // 2, rows), F32
                    )

    for side in range(8):

        @pl.when(jnp.logical_not(beside(DIRECTIONS[side], -1)))
        def _():
            clear(side)

    loads[0].wait()
    incidence_stage(tri_ref, inc, pos_ref.shape[2])
    for load in loads[1:4]:
        load.wait()
    for p in range(plane_count):
        at = plane_rows(p)
        fields = [pop_ref[q, p] for q in range(19)]
        density, momentum = local_moments(fields)
        fluid = fluid_ref[p] == 1
        keep = 1.0 - relax_ref[p]
        values = [jnp.where(fluid, keep * fields[q], fields[OPPOSITE[q]]) for q in range(19)]
        values += [jnp.where(fluid, relax_ref[p], 0.0), density] + momentum
        for q, value in enumerate(values):
            raw[q, at, :] = value
            keep_plane(q, p, value, RAW_MOVES, raw_zsend)
    pack(raw, RAW_MOVES, (None, raw_xsend, raw_csend))
    loads[6].wait()
    pl.semaphore_wait(barrier, expected)

    coarse_all[slab] = coarse_ref[...]

    def coarse_copy(d):
        return pltpu.make_async_remote_copy(
            src_ref=coarse_ref,
            dst_ref=coarse_all.at[slab],
            send_sem=coarse_sems.at[0, d],
            recv_sem=coarse_sems.at[1, d],
            device_id={"slab": lax.rem(slab + d, slabs), "cross": cross},
            device_id_type=MESH,
        )

    @pl.loop(1, slabs)
    def _(d):
        coarse_copy(d).start()

    loads[7].wait()

    def face_copy(index):
        return pltpu.make_async_remote_copy(
            src_ref=face_ref,
            dst_ref=faces.at[index],
            send_sem=face_sems.at[0, index],
            recv_sem=face_sems.at[1, index],
            device_id=target(DIRECTIONS[index]),
            device_id_type=MESH,
        )

    for index in (4, 5, 6, 7, 0, 1, 2, 3):

        @pl.when(beside(DIRECTIONS[index], 1))
        def _():
            face_copy(index).start()

    for index in (4, 5, 6, 7, 0, 1, 2, 3):

        @pl.when(beside(DIRECTIONS[index], 1))
        def _():
            raw_copy(index).start()

    for load in loads[4:6]:
        load.wait()
    nodal_stage(
        plane_count, columns, rows, pos_ref, ten_ref, inc, xs, cell_ref, lane_ref, nodal
    )
    spread_stage(plane_count, columns, cell_ref, lane_ref, nodal, acc, along, across, own_force)

    def force_copy(index):
        part = extent // 2
        start = part if index == 0 else 0
        return pltpu.make_async_remote_copy(
            src_ref=cubed(own_force).at[:, pl.ds(1, wide), pl.ds(start, part)],
            dst_ref=cubed(far_force).at[:, pl.ds(1, wide), pl.ds(part - start, part)],
            send_sem=force_sems.at[0, index],
            recv_sem=force_sems.at[1, index],
            device_id=target(DIRECTIONS[index]),
            device_id_type=MESH,
        )

    for index in range(2):

        @pl.when(beside(DIRECTIONS[index], 1))
        def _():
            force_copy(index).start()

    @pl.loop(1, slabs)
    def _(d):
        pltpu.make_async_remote_copy(
            src_ref=coarse_ref,
            dst_ref=coarse_all.at[lax.rem(slab + slabs - d, slabs)],
            send_sem=coarse_sems.at[0, d],
            recv_sem=coarse_sems.at[1, d],
            device_id={"slab": lax.rem(slab + d, slabs), "cross": cross},
            device_id_type=MESH,
        ).wait_recv()

    for index in range(8):

        @pl.when(beside(DIRECTIONS[index], -1))
        def _():
            face_copy(index).wait_recv()

    slots = face_ref.shape[1]
    lanes = table.shape[1]
    chunks = coarse_ref.shape[1] // lanes
    together = table.shape[0] // (4 * chunks)
    groups = [[face_ref[pl.ds(k, 1), :] for k in range(3)]] + [
        [faces[index, pl.ds(k, 1), :] for k in range(3)] for index in range(8)
    ]
    wanted = [jnp.concatenate(group[1:], axis=1) for group in groups]
    one, zero = jnp.ones((), BF16), jnp.zeros((), BF16)
    picks = [
        jnp.where(
            lax.broadcasted_iota(I16, (lanes, 2 * slots), 0) == (index & (lanes - 1)).astype(I16),
            one, zero,
        )
        for index in wanted
    ]
    quarter = lax.shift_right_logical(
        lax.broadcasted_iota(I32, (table.shape[0], 2 * slots), 0), 2
    )

    def gather(base, found):
        for j in range(together):
            for chunk in range(chunks):
                table[pl.ds((j * chunks + chunk) * 4, 4), :] = coarse_all[
                    base * together + j, :, chunk * lanes : (chunk + 1) * lanes
                ]
        stacked = jnp.concatenate(split(table[...], 2), axis=0).astype(BF16)
        result = []
        for index, pick, total in zip(wanted, picks, found):
            both = jnp.dot(stacked, pick, preferred_element_type=F32)
            both = both[: table.shape[0]] + both[table.shape[0] :]
            high = lax.shift_right_logical(index, lanes.bit_length() - 1)
            both = jnp.where(quarter == high - base * (together * chunks), both, 0.0)
            for start in range(0, table.shape[0], 8):
                total = total + both[start : start + 8]
            result.append(total)
        return tuple(result)

    found = tuple(jnp.zeros((8, 2 * slots), F32) for _ in groups)
    if coarse_all.shape[0] == together:
        found = gather(0, found)
    else:
        found = lax.fori_loop(0, coarse_all.shape[0] // together, gather, found)
    blended = []
    for total in found:
        total = total[0:4] + total[4:8]
        blended.append(0.75 * total[:, :slots] + 0.25 * total[:, slots:])

    def spots(group):
        cell = group[0]
        used = cell >= 0
        line = cell // rows
        return used, line // columns, line % columns, jnp.where(used, cell % rows, -1)

    def put(size, goals, lane_rows, moments):
        mask = [lax.broadcasted_iota(I32, (size, slots), 0) == goal for goal in goals]
        pieces = [split(value, 2) for value in moments]
        left = [
            jnp.concatenate(
                [jnp.where(m, piece[part][k : k + 1], 0.0) for m, piece in zip(mask, pieces)], axis=1
            )
            for k in range(4)
            for part in range(2)
        ]
        left.append(jnp.concatenate([jnp.where(m, 1.0, 0.0) for m in mask], axis=1))
        right = jnp.concatenate(
            [
                jnp.where(lax.broadcasted_iota(I32, (rows, slots), 0) == lane, 1.0, 0.0)
                for lane in lane_rows
            ],
            axis=1,
        )
        out = lax.dot_general(
            jnp.concatenate(left, axis=0).astype(BF16), right.astype(BF16), NT,
            preferred_element_type=F32,
        )
        return [
            out[2 * k * size : (2 * k + 1) * size] + out[(2 * k + 1) * size : (2 * k + 2) * size]
            for k in range(4)
        ] + [out[8 * size : 9 * size]]

    used, plane, column, lane = spots(groups[0])
    goal = jnp.where(used, column * plane_count + plane, -1)
    for k, value in enumerate(put(columns * plane_count, [goal], [lane], blended[:1])):
        for c in range(columns):
            placed_ref[k, pl.ds((HALO + 1 + c) * extent + HALO, plane_count), :] = value[
                c * plane_count : (c + 1) * plane_count
            ]

    goals, lane_rows, offsets, offset = [], [], [], 0
    for index, (dz, dx) in enumerate(DIRECTIONS):
        used, plane, column, lane = spots(groups[1 + index])
        if dz:
            used = used & (plane == (plane_count - 1 if dz == 1 else 0))
        if dx:
            used = used & (column == (columns - 1 if dx == 1 else 0))
        along_edge = column if dx == 0 else plane if dz == 0 else jnp.zeros_like(plane)
        goals.append(jnp.where(used, along_edge + offset, -1))
        lane_rows.append(lane)
        offsets.append(offset)
        offset += columns if dx == 0 else plane_count if dz == 0 else 1
    for k, value in enumerate(put(round_up(offset, 16), goals, lane_rows, blended[1:])):
        for index, (dz, dx) in enumerate(DIRECTIONS):
            size = columns if dx == 0 else plane_count if dz == 0 else 1
            part = value[offsets[index] : offsets[index] + size]
            if k == 4:
                part = jnp.where(beside(DIRECTIONS[index], -1), part, 1.0)
            p = -1 if dz == 1 else plane_count
            c = HALO + (-1 if dx == 1 else columns)
            if dx == 0:
                placed_ref[k, plane_rows(p), :] = part
            elif dz == 0:
                placed_ref[k, pl.ds((c + 1) * extent + HALO, plane_count), :] = part
            else:
                placed_ref[k, pl.ds((c + 1) * extent + HALO + p, 1), :] = part

    for c in range(1, wide - 1):
        at = column_rows(c)
        density = placed_ref[0, at, :]
        velocity = [placed_ref[k, at, :] for k in range(1, 4)]
        for q, value in enumerate(equilibrium_pairs(density, velocity)):
            rim[q, at, :] = value

    for index in range(2):

        @pl.when(beside(DIRECTIONS[index], -1))
        def _():
            force_copy(index).wait_recv()

    for index in range(8):

        @pl.when(beside(DIRECTIONS[index], -1))
        def _():
            raw_copy(index).wait_recv()

    unpack(raw, RAW_MOVES, (raw_zrecv, raw_xrecv, raw_crecv))

    def pulled(source, at, starts):
        fixed = placed_ref[4, at, :] > 0.5
        fields = []
        for q, (cz, cx, cy) in enumerate(LATTICE_VECTORS):
            value = source[q, starts(cz, cx), :]
            if cy != 0:
                value = pltpu.roll(value, cy % rows, 1)
            fields.append(jnp.where(fixed, rim[q, at, :], value))
        return fields

    def pulled_column(source, c):
        return pulled(
            source,
            column_rows(c),
            lambda cz, cx: pl.ds((c + 1 - cx) * extent - cz, extent),
        )

    def pulled_plane(source, p):
        return pulled(source, plane_rows(p), lambda cz, cx: plane_rows(p, cz, cx))

    def inward(c, depth):
        if c < HALO:
            return [q for q in range(19) if LATTICE_VECTORS[q][1] >= HALO - c - depth]
        if c >= HALO + columns:
            return [q for q in range(19) if -LATTICE_VECTORS[q][1] >= c - HALO - columns + 1 - depth]
        return range(19)

    for c in range(wide):
        at = column_rows(c)
        rate = raw[RATE, at, :]
        fluid = rate > 0.0
        inverse = 1.0 / rate
        push = []
        for k in range(3):
            value = jnp.where(fluid, (own_force[k, at, :] + far_force[k, at, :]) * inverse, 0.0)
            pushed[k, at, :] = value
            push.append(value)
        momentum = [raw[MOMENTUM + k, at, :] for k in range(3)]
        needed = inward(c, 1)
        terms = pull_terms(raw[DENSITY, at, :], momentum, rate, push, needed)
        for q in needed:
            kept = raw[q, at, :]
            post_one[q, at, :] = jnp.where(fluid, kept + terms[q], kept)

    def collide_columns(source, sink):
        for c in range(1, wide - 1):
            at = column_rows(c)
            fields = pulled_column(source, c)
            push = [pushed[k, at, :] for k in range(3)]
            for q, value in collide(fields, raw[RATE, at, :], push, inward(c, 0)).items():
                sink[q, at, :] = value

    collide_columns(post_one, post_two)

    for p in range(plane_count):
        at = plane_rows(p)
        fields = pulled_plane(post_two, p)
        push = [pushed[k, at, :] for k in range(3)]
        for q, value in collide(fields, raw[RATE, at, :], push).items():
            post_three[q, at, :] = value
            keep_plane(q, p, value, MOVES, zsend)
    pack(post_three, MOVES, (None, xsend, csend))

    for index in (4, 5, 6, 7, 0, 1, 2, 3):

        @pl.when(beside(DIRECTIONS[index], 1))
        def _():
            halo_copy(index).start()

    for index in range(8):

        @pl.when(beside(DIRECTIONS[index], -1))
        def _():
            halo_copy(index).wait_recv()

    unpack(post_three, MOVES, (zrecv, xrecv, crecv))
    collide_columns(post_three, post_one)

    for p in range(plane_count):
        for q, value in enumerate(pulled_plane(post_one, p)):
            next_ref[q, p] = value

    @pl.loop(1, slabs)
    def _(d):
        coarse_copy(d).wait_send()

    for index in range(8):

        @pl.when(beside(DIRECTIONS[index], 1))
        def _():
            raw_copy(index).wait_send()
            face_copy(index).wait_send()
            halo_copy(index).wait_send()
            if index < 2:
                force_copy(index).wait_send()


def flow_kernel(fields_ref, next_ref, flow_ref, flow, sems):
    whole = pltpu.make_async_copy(fields_ref, next_ref, sems.at[0])
    whole.start()
    for p in range(fields_ref.shape[1]):
        fields = [fields_ref[q, p] for q in range(19)]
        density, momentum = moments_of(fields)
        inverse = ROOT_THREE / density
        for k in range(3):
            flow[k, p] = momentum[k] * inverse
    part = pltpu.make_async_copy(flow, flow_ref, sems.at[1])
    part.start()
    whole.wait()
    part.wait()


def coarse_rows(slabs, coarse_moments):
    count, width = coarse_moments.shape
    return math.gcd(slabs, 8) * count * (width // 128)


def on_device(
    slabs, crosses,
    populations, fluid_mask, relaxation, positions, triangles, tension, coarse_moments, interface,
):
    _, plane_count, columns, rows = populations.shape
    _, membranes, nodes = positions.shape
    padded = round_up(nodes, 128)
    corners = triangles.shape[1]
    half, planes = (columns + 6) // 2, plane_count + 2
    cells = round_up(planes * half, 16)
    flat = (columns + 2 * HALO + 2) * (plane_count + 2 * HALO)
    vmem = pl.BlockSpec(memory_space=pltpu.VMEM)
    block = (19, plane_count, columns, rows)
    operands = (
        triangles, populations, relaxation, fluid_mask, positions, tension, coarse_moments, interface,
    )
    fields = pl.pallas_call(
        functools.partial(lattice_kernel, slabs, crosses),
        name="lattice_steps",
        out_shape=pltpu.VMEM(block, F32),
        in_specs=[pl.BlockSpec(memory_space=pl.ANY)] * 8,
        out_specs=vmem,
        scratch_shapes=[pltpu.VMEM(operand.shape, operand.dtype) for operand in operands]
        + [
            pltpu.VMEM((3, membranes, padded), F32),
            pltpu.VMEM((padded, corners), BF16),
            pltpu.VMEM((3, membranes, padded), F32),
            pltpu.VMEM((membranes, padded), I32),
            pltpu.VMEM((membranes, padded), I32),
            pltpu.VMEM((6 * cells, 2 * rows), F32),
            pltpu.VMEM((3, half * planes + cells, rows), F32),
            pltpu.VMEM((3, (columns + 4) * planes + 16, rows), F32),
            pltpu.VMEM((CHANNELS, flat, rows), F32),
            pltpu.VMEM((3, flat, rows), F32),
            pltpu.VMEM((3, flat, rows), F32),
            pltpu.VMEM((3, flat, rows), F32),
            pltpu.VMEM((5, flat, rows), F32),
            pltpu.VMEM((19, flat, rows), F32),
            pltpu.VMEM((19, flat, rows), F32),
            pltpu.VMEM((19, flat, rows), F32),
            pltpu.VMEM((19, flat, rows), F32),
            pltpu.VMEM((slabs,) + coarse_moments.shape, F32),
            pltpu.VMEM((coarse_rows(slabs, coarse_moments), 128), F32),
            pltpu.VMEM((8,) + interface.shape, I32),
        ]
        + [
            pltpu.VMEM(shape, F32)
            for moves in (MOVES, MOVES, RAW_MOVES, RAW_MOVES)
            for shape in buffer_shapes(moves, plane_count, columns, rows)
        ]
        + [
            pltpu.SemaphoreType.DMA((8,)),
            pltpu.SemaphoreType.DMA((2, slabs)),
            pltpu.SemaphoreType.DMA((2, 8)),
            pltpu.SemaphoreType.DMA((2, 2)),
            pltpu.SemaphoreType.DMA((2, 8)),
            pltpu.SemaphoreType.DMA((2, 8)),
        ],
        compiler_params=pltpu.CompilerParams(collective_id=0, has_side_effects=True),
    )(*operands)
    return pl.pallas_call(
        flow_kernel,
        name="flow",
        out_shape=(
            jax.ShapeDtypeStruct(block, F32),
            jax.ShapeDtypeStruct((3,) + block[1:], F32),
        ),
        in_specs=[vmem],
        out_specs=(pl.BlockSpec(memory_space=pl.ANY),) * 2,
        scratch_shapes=[pltpu.VMEM((3,) + block[1:], F32), pltpu.SemaphoreType.DMA((2,))],
    )(pltpu.with_memory_space_constraint(fields, pltpu.VMEM))


def solution(mesh):
    in_specs = (
        P(None, "slab", "cross", None),
        P("slab", "cross", None),
        P("slab", "cross", None),
        P(None, "slab", None),
        P(),
        P("slab", None),
        P(None, "slab"),
        P(None, ("slab", "cross")),
    )
    out_specs = (P(None, "slab", "cross", None), P(None, "slab", "cross", None))
    return jax.shard_map(
        functools.partial(on_device, mesh.shape["slab"], mesh.shape["cross"]),
        mesh=mesh, in_specs=in_specs, out_specs=out_specs, check_vma=False,
    )
```

```python
import functools
import math

import jax
import jax.numpy as jnp
from jax import lax
from jax.experimental import pallas as pl
from jax.experimental.pallas import tpu as pltpu
from jax.sharding import PartitionSpec as P

STEPS = 4
MESH = pl.DeviceIdType.MESH
LATTICE_VECTORS = [
    (0, 0, 0),
    (1, 0, 0),
    (-1, 0, 0),
    (0, 1, 0),
    (0, -1, 0),
    (0, 0, 1),
    (0, 0, -1),
    (1, 1, 0),
    (-1, -1, 0),
    (1, -1, 0),
    (-1, 1, 0),
    (1, 0, 1),
    (-1, 0, -1),
    (1, 0, -1),
    (-1, 0, 1),
    (0, 1, 1),
    (0, -1, -1),
    (0, 1, -1),
    (0, -1, 1),
]
LATTICE_WEIGHTS = [1.0 / 3.0] + [1.0 / 18.0] * 6 + [1.0 / 36.0] * 12
OPPOSITE = [0] + [q + 1 if q % 2 == 1 else q - 1 for q in range(1, 19)]
ROOT_THREE = math.sqrt(3.0)
DIRECTIONS = [(1, 0), (-1, 0), (0, 1), (0, -1), (1, 1), (-1, -1), (1, -1), (-1, 1)]
NT = (((1,), (1,)), ((), ()))
F32, BF16, I32, I16 = jnp.float32, jnp.bfloat16, jnp.int32, jnp.int16
HALO = 2


def slab_moves(extra):
    return [
        [
            (q, depth)
            for depth in (1, 2)
            for q in [m for m in range(19) if LATTICE_VECTORS[m][0] * sign >= depth - 1] + extra
        ]
        for sign in (1, -1)
    ]


def cross_moves(extra):
    return [
        [
            (q, depth)
            for depth in (1, 2)
            for q in [m for m in range(19) if LATTICE_VECTORS[m][1] * sign >= depth - 1] + extra
        ]
        for sign in (1, -1)
    ]


def corner_moves(extra):
    return [
        [
            (q, dz, dx)
            for dz in (1, 2)
            for dx in (1, 2)
            for q in [
                m
                for m in range(19)
                if LATTICE_VECTORS[m][0] * sz >= dz - 1 and LATTICE_VECTORS[m][1] * sx >= dx - 1
            ]
            + extra
        ]
        for sz, sx in DIRECTIONS[4:]
    ]


RATE, DENSITY, MOMENTUM, CHANNELS = 19, 20, 21, 24
MOVES = (slab_moves([]), cross_moves([]), corner_moves([]))
EXTRA = list(range(19, CHANNELS))
RAW_MOVES = (slab_moves(EXTRA), cross_moves(EXTRA), corner_moves(EXTRA))


def buffer_shapes(moves, plane_count, columns, rows):
    return [
        (2, len(moves[0][0]), columns, rows),
        (2, round_up(len(moves[1][0]) * plane_count, 8), rows),
        (4, round_up(len(moves[2][0]), 8), rows),
    ]


def round_up(value, unit):
    return (value + unit - 1) // unit * unit


def split(value, parts):
    pieces = []
    for _ in range(parts):
        piece = value.astype(BF16).astype(F32)
        pieces.append(piece)
        value = value - piece
    return pieces


def incidence_stage(tri_ref, inc, nodes):
    triangles = tri_ref.shape[1]
    tiles = triangles // 128
    corners = [
        [
            jnp.broadcast_to(tri_ref[pl.ds(k, 1), t * 128 : (t + 1) * 128], (16, 128)).astype(I16)
            for t in range(tiles)
        ]
        for k in range(3)
    ]
    iota = lax.broadcasted_iota(I32, (16, 128), 0)
    zero, one = jnp.zeros((16, 128), BF16), jnp.ones((16, 128), BF16)

    def rows_at(start):
        ids = (iota + start).astype(I16)
        for t in range(tiles):
            value = zero
            for k in range(3):
                value = jnp.where(ids == corners[k][t], one, value)
            inc[pl.ds(start, 16), t * 128 : (t + 1) * 128] = value

    chunk = 128

    @pl.loop(0, nodes // chunk)
    def _(i):
        for r in range(chunk // 16):
            rows_at(pl.multiple_of(i * chunk + r * 16, 16))

    done = nodes // chunk * chunk
    while done < nodes:
        rows_at(done)
        done += 16
    if done < inc.shape[0]:
        inc[done:, :] = jnp.zeros((inc.shape[0] - done, triangles), BF16)


def nodal_stage(plane_count, columns, rows, pos_ref, ten_ref, inc, xs, cell_ref, lane_ref, force):
    dims, membranes, nodes = pos_ref.shape
    padded = xs.shape[2]
    slab = lax.axis_index("slab")
    cross = lax.axis_index("cross")
    planes, half = plane_count + 2, (columns + 6) // 2

    cell_ref[...] = jnp.full(cell_ref.shape, -1, I32)
    lane_ref[...] = jnp.full(lane_ref.shape, -1, I32)
    plane = pos_ref[0] - (slab * plane_count - 1)
    column = pos_ref[1] - (cross * columns - 3)
    row = pos_ref[2]
    inside = (column >= 0) & (column < 2 * half)
    upper = column >= half
    cell = jnp.where(upper, column - half, column) * planes + plane
    cell_ref[:, :nodes] = jnp.where(inside, cell, -1)
    lane_ref[:, :nodes] = row + jnp.where(upper, rows, 0)

    xs[...] = jnp.zeros_like(xs)
    for k in range(3):
        xs[k, :, :nodes] = (pos_ref[k] - pos_ref[k, :, 0:1]).astype(F32)

    coords = xs[...].reshape(dims * membranes, padded)
    sums = jnp.dot(coords.astype(BF16), inc[...], preferred_element_type=F32)
    tension = ten_ref[...]
    terms = jnp.concatenate(
        [sums[k * membranes : (k + 1) * membranes] * tension for k in range(3)] + [tension], axis=0
    )
    stacked = jnp.concatenate(split(terms, 2), axis=0).astype(BF16)
    gathered = lax.dot_general(stacked, inc[...], NT, preferred_element_type=F32)
    count = terms.shape[0]
    total = gathered[:count] + gathered[count:]
    weight = total[3 * membranes :]
    for k in range(3):
        force[k] = total[k * membranes : (k + 1) * membranes] - 3.0 * xs[k] * weight


def spread_stage(plane_count, columns, nodes, cell_ref, lane_ref, force, acc, along, across, out_ref):
    _, membranes, padded = force.shape
    rows = out_ref.shape[2]
    planes, half = plane_count + 2, (columns + 6) // 2
    extent = plane_count + 2 * HALO
    cells = acc.shape[0] // 6
    unroll = 4 if membranes % 4 == 0 else 1
    zero, one = jnp.zeros((), BF16), jnp.ones((), BF16)

    main = nodes // 128 * 128
    tail = nodes - main
    packed = 0 < tail * membranes <= 128
    if not packed:
        main = padded

    def one_hots(cell, lane, force_rows):
        mask = lax.broadcasted_iota(I16, (cells, cell.shape[1]), 0) == cell.astype(I16)
        values = [split(value, 2) for value in force_rows]
        left = jnp.concatenate(
            [
                jnp.where(mask, values[k][part].astype(BF16), zero)
                for part in range(2)
                for k in range(3)
            ],
            axis=0,
        )
        ids = lax.broadcasted_iota(I16, (2 * rows, cell.shape[1]), 0)
        return left, jnp.where(ids == lane.astype(I16), one, zero)

    def gathered_tail(value):
        lanes = lax.broadcasted_iota(I32, (membranes, 128), 1)
        value = jnp.where(lanes < tail, value, jnp.zeros_like(value))
        value = pltpu.roll(value, 0, 1, stride=tail, stride_axis=0)
        return jnp.sum(value, axis=0, keepdims=True)

    if packed:
        ends = slice(main, main + 128)
        left, right = one_hots(
            gathered_tail(cell_ref[:, ends] + 1) - 1,
            gathered_tail(lane_ref[:, ends] + 1) - 1,
            [gathered_tail(force[k, :, ends]) for k in range(3)],
        )
        acc[...] = lax.dot_general(left, right, NT, preferred_element_type=F32)
    else:
        acc[...] = jnp.zeros_like(acc)

    @pl.loop(0, membranes // unroll)
    def _(i):
        parts = []
        for inner in range(unroll):
            m = pl.ds(i * unroll + inner, 1)
            parts.append(
                one_hots(
                    cell_ref[m, :main], lane_ref[m, :main], [force[k, m, :main] for k in range(3)]
                )
            )
        left, right = (jnp.concatenate(side, axis=1) for side in zip(*parts))
        acc[...] += lax.dot_general(left, right, NT, preferred_element_type=F32)

    used = half * planes
    inner = (columns + 4) * planes
    step = lax.broadcasted_iota(I32, (extent, rows), 0)
    weights = [
        jnp.where((step >= 2 - shift) & (step < planes + 2 - shift), w, 0.0)
        for shift, w in ((0, 0.25), (1, 0.5), (2, 0.25))
    ]
    for k in range(3):
        value = acc[k * cells : (k + 1) * cells] + acc[(3 + k) * cells : (4 + k) * cells]
        for part in range(2):
            b = value[:, part * rows : (part + 1) * rows]
            b = 0.5 * b + 0.25 * (pltpu.roll(b, 1, 1) + pltpu.roll(b, rows - 1, 1))
            along[k, part * used : part * used + cells] = b
        across[k, 0:8] = jnp.zeros((8, rows), F32)
        across[k, 8 + inner : 16 + inner] = jnp.zeros((8, rows), F32)
        across[k, 8 : 8 + inner] = 0.5 * along[k, planes : planes + inner] + 0.25 * (
            along[k, 0:inner] + along[k, 2 * planes : 2 * planes + inner]
        )
        for c in range(columns + 4):
            start = 8 + c * planes
            out_ref[k, (c + 1) * extent : (c + 2) * extent] = (
                weights[0] * across[k, start - 2 : start - 2 + extent]
                + weights[1] * across[k, start - 1 : start - 1 + extent]
                + weights[2] * across[k, start : start + extent]
            )


def equilibrium_pairs(density, velocity):
    squared = velocity[0] * velocity[0] + velocity[1] * velocity[1] + velocity[2] * velocity[2]
    base = 1.0 - 1.5 * squared
    result = [None] * 19
    result[0] = LATTICE_WEIGHTS[0] * density * base
    scaled = {w: w * density for w in (1.0 / 18.0, 1.0 / 36.0)}
    for q in range(1, 19, 2):
        projected = None
        for c, v in zip(LATTICE_VECTORS[q], velocity):
            if c == 0:
                continue
            if projected is None:
                projected = v if c == 1 else -v
            else:
                projected = projected + v if c == 1 else projected - v
        even = base + 4.5 * projected * projected
        odd = 3.0 * projected
        weight = scaled[LATTICE_WEIGHTS[q]]
        result[q] = weight * (even + odd)
        result[q + 1] = weight * (even - odd)
    return result


def moments_of(fields):
    density = functools.reduce(lambda a, b: a + b, fields)
    momentum = []
    for k in range(3):
        plus = [fields[q] for q in range(19) if LATTICE_VECTORS[q][k] == 1]
        minus = [fields[q] for q in range(19) if LATTICE_VECTORS[q][k] == -1]
        momentum.append(functools.reduce(lambda a, b: a + b, [a - b for a, b in zip(plus, minus)]))
    return density, momentum


def local_moments(fields):
    gaps = [fields[q] - fields[q + 1] for q in range(1, 19, 2)]
    sums = [fields[q] + fields[q + 1] for q in range(1, 19, 2)]
    density = functools.reduce(lambda a, b: a + b, sums) + fields[0]
    momentum = []
    for k in range(3):
        total = None
        for pair in range(9):
            c = LATTICE_VECTORS[2 * pair + 1][k]
            if c and total is None:
                total = gaps[pair]
            elif c:
                total = total + gaps[pair] if c == 1 else total - gaps[pair]
        momentum.append(total)
    return density, momentum


def pull_terms(density, momentum, rate, pushed, needed):
    scale = 3.0 / density
    tripled = [(m + p) * scale for m, p in zip(momentum, pushed)]
    squared = tripled[0] * tripled[0] + tripled[1] * tripled[1] + tripled[2] * tripled[2]
    base = 1.0 - (1.0 / 6.0) * squared
    strength = rate * density
    scaled = {w: w * strength for w in (1.0 / 18.0, 1.0 / 36.0)}
    result = [None] * 19
    result[0] = (LATTICE_WEIGHTS[0] * strength) * base
    for q in range(1, 19, 2):
        if q not in needed and q + 1 not in needed:
            continue
        projected = None
        for c, v in zip(LATTICE_VECTORS[q], tripled):
            if c == 0:
                continue
            if projected is None:
                projected = v if c == 1 else -v
            else:
                projected = projected + v if c == 1 else projected - v
        weight = scaled[LATTICE_WEIGHTS[q]]
        even = weight * (base + 0.5 * projected * projected)
        odd = weight * projected
        result[q] = even + odd
        result[q + 1] = even - odd
    return result


def collide(fields, rate, pushed, needed=range(19)):
    density, momentum = local_moments(fields)
    terms = pull_terms(density, momentum, rate, pushed, needed)
    fluid = rate > 0.0
    keep = 1.0 - rate
    return {q: jnp.where(fluid, keep * fields[q] + terms[q], fields[OPPOSITE[q]]) for q in needed}


def lattice_kernel(
    slabs, crosses,
    tri_hbm, pop_hbm, relax_hbm, fluid_hbm, pos_hbm, ten_hbm, coarse_hbm, face_hbm,
    next_ref,
    tri_ref, pop_ref, relax_ref, fluid_ref, pos_ref, ten_ref, coarse_ref, face_ref,
    xs, inc, nodal, cell_ref, lane_ref, acc, along, across,
    raw, own_force, far_force, pushed, placed_ref, rim, post_one, post_two, post_three,
    coarse_all, table, faces,
    zsend, xsend, csend, zrecv, xrecv, crecv,
    raw_zsend, raw_xsend, raw_csend, raw_zrecv, raw_xrecv, raw_crecv,
    load_sems, coarse_sems, raw_sems, force_sems, face_sems, halo_sems,
):
    _, plane_count, columns, rows = pop_ref.shape
    extent, wide = plane_count + 2 * HALO, columns + 2 * HALO
    slab = lax.axis_index("slab")
    cross = lax.axis_index("cross")

    def beside(direction, sign):
        dz, dx = direction[0] * sign, direction[1] * sign
        conditions = []
        if dz == 1:
            conditions.append(slab < slabs - 1)
        if dz == -1:
            conditions.append(slab > 0)
        if dx == 1:
            conditions.append(cross < crosses - 1)
        if dx == -1:
            conditions.append(cross > 0)
        return functools.reduce(jnp.logical_and, conditions)

    def target(direction):
        return {"slab": slab + direction[0], "cross": cross + direction[1]}

    def cubed(ref):
        return ref.reshape(ref.shape[0], wide + 2, extent, rows)

    def inner_row(step, depth, size):
        return HALO + (size - depth if step == 1 else depth - 1)

    def outer_row(step, depth, size):
        return HALO + (-depth if step == 1 else size - 1 + depth)

    def pack_corners(source, moves, buffer):
        for side in range(4):
            sz, sx = DIRECTIONS[4 + side]
            for e, (q, dz, dx) in enumerate(moves[2][side]):
                row = (inner_row(sx, dx, columns) + 1) * extent + inner_row(sz, dz, plane_count)
                buffer[side, pl.ds(e, 1), :] = source[q, pl.ds(row, 1), :]

    def pack_cross(source, moves, buffer):
        for side in range(2):
            for e, (q, depth) in enumerate(moves[1][side]):
                row = (inner_row(DIRECTIONS[2 + side][1], depth, columns) + 1) * extent + HALO
                buffer[side, pl.ds(e * plane_count, plane_count), :] = source[
                    q, pl.ds(row, plane_count), :
                ]

    def unpack(sink, moves, buffers):
        for side in range(2):
            for e, (q, depth) in enumerate(moves[0][side]):
                row = outer_row(DIRECTIONS[side][0], depth, plane_count)
                sink[q, plane_rows(row - HALO), :] = buffers[0][side, e]
            for e, (q, depth) in enumerate(moves[1][side]):
                row = (outer_row(DIRECTIONS[2 + side][1], depth, columns) + 1) * extent + HALO
                sink[q, pl.ds(row, plane_count), :] = buffers[1][
                    side, pl.ds(e * plane_count, plane_count), :
                ]
        for side in range(4):
            sz, sx = DIRECTIONS[4 + side]
            for e, (q, dz, dx) in enumerate(moves[2][side]):
                row = (outer_row(sx, dx, columns) + 1) * extent + outer_row(sz, dz, plane_count)
                sink[q, pl.ds(row, 1), :] = buffers[2][side, pl.ds(e, 1), :]

    def keep_plane(q, p, value, moves, buffer):
        for side in range(2):
            entry = (q, plane_count - p if side == 0 else p + 1)
            if entry in moves[0][side]:
                buffer[side, moves[0][side].index(entry)] = value

    def buffers_copy(sources, sinks, sems, index):
        kind, place = (0, index) if index < 2 else (1, index - 2) if index < 4 else (2, index - 4)
        return pltpu.make_async_remote_copy(
            src_ref=sources[kind].at[place],
            dst_ref=sinks[kind].at[place],
            send_sem=sems.at[0, index],
            recv_sem=sems.at[1, index],
            device_id=target(DIRECTIONS[index]),
            device_id_type=MESH,
        )

    def halo_copy(index):
        return buffers_copy((zsend, xsend, csend), (zrecv, xrecv, crecv), halo_sems, index)

    def raw_copy(index):
        return buffers_copy(
            (raw_zsend, raw_xsend, raw_csend), (raw_zrecv, raw_xrecv, raw_crecv), raw_sems, index
        )

    def column_rows(c):
        return pl.ds((c + 1) * extent, extent)

    def plane_rows(p, dz=0, dx=0):
        return pl.ds((HALO + 1 - dx) * extent + HALO + p - dz, columns, stride=extent)

    loads = [
        pltpu.make_async_copy(source, sink, load_sems.at[i])
        for i, (source, sink) in enumerate(
            (
                (tri_hbm, tri_ref),
                (pop_hbm, pop_ref),
                (relax_hbm, relax_ref),
                (fluid_hbm, fluid_ref),
                (pos_hbm, pos_ref),
                (ten_hbm, ten_ref),
                (coarse_hbm, coarse_ref),
                (face_hbm, face_ref),
            )
        )
    ]
    for load in loads:
        load.start()

    barrier = pltpu.get_barrier_semaphore()

    @pl.loop(1, slabs)
    def _(d):
        peer = lax.rem(slab + d, slabs)
        pl.semaphore_signal(
            barrier, inc=1, device_id={"slab": peer, "cross": cross}, device_id_type=MESH
        )

    expected = slabs - 1
    for direction in DIRECTIONS:
        if direction[1] == 0:
            continue
        there = beside(direction, 1)
        expected = expected + jnp.where(there, 1, 0)

        @pl.when(there)
        def _():
            pl.semaphore_signal(
                barrier, inc=1, device_id=target(direction), device_id_type=MESH
            )

    def clear(side):
        kind, place = (0, side) if side < 2 else (1, side - 2) if side < 4 else (2, side - 4)
        for sinks in ((zrecv, xrecv, crecv), (raw_zrecv, raw_xrecv, raw_crecv)):
            sinks[kind][place] = jnp.zeros(sinks[kind].shape[1:], F32)
        faces[side] = jnp.full(faces.shape[1:], -1, I32)
        if side < 2:
            near = side * (extent // 2)
            for c in range(wide):
                for k in range(3):
                    far_force[k, pl.ds((c + 1) * extent + near, extent // 2), :] = jnp.zeros(
                        (extent // 2, rows), F32
                    )

    for side in range(8):

        @pl.when(jnp.logical_not(beside(DIRECTIONS[side], -1)))
        def _():
            clear(side)

    loads[0].wait()
    incidence_stage(tri_ref, inc, pos_ref.shape[2])
    for load in loads[1:4]:
        load.wait()
    for p in range(plane_count):
        at = plane_rows(p)
        fields = [pop_ref[q, p] for q in range(19)]
        density, momentum = local_moments(fields)
        fluid = fluid_ref[p] == 1
        keep = 1.0 - relax_ref[p]
        values = [jnp.where(fluid, keep * fields[q], fields[OPPOSITE[q]]) for q in range(19)]
        values += [jnp.where(fluid, relax_ref[p], 0.0), density] + momentum
        for q, value in enumerate(values):
            raw[q, at, :] = value
            keep_plane(q, p, value, RAW_MOVES, raw_zsend)
    pack_corners(raw, RAW_MOVES, raw_csend)
    pack_cross(raw, RAW_MOVES, raw_xsend)
    loads[6].wait()
    pl.semaphore_wait(barrier, expected)

    ways = 2 if slabs % 2 == 0 else 1
    share = slabs // ways
    way = slab % ways

    def place_of(index):
        return index % ways * share + index // ways

    coarse_all[place_of(slab)] = coarse_ref[...]

    def coarse_copy(d, sink):
        return pltpu.make_async_remote_copy(
            src_ref=coarse_ref,
            dst_ref=coarse_all.at[place_of(sink)],
            send_sem=coarse_sems.at[0, d],
            recv_sem=coarse_sems.at[1, d],
            device_id={"slab": lax.rem(slab + ways * d, slabs), "cross": cross},
            device_id_type=MESH,
        )

    def relay():
        half = coarse_all.at[pl.ds(way * share, share)]
        return pltpu.make_async_remote_copy(
            src_ref=half,
            dst_ref=half,
            send_sem=coarse_sems.at[0, 0],
            recv_sem=coarse_sems.at[1, 0],
            device_id={"slab": slab + 1 - 2 * way, "cross": cross},
            device_id_type=MESH,
        )

    @pl.loop(1, share)
    def _(d):
        coarse_copy(d, slab).start()

    loads[7].wait()

    def face_copy(index):
        return pltpu.make_async_remote_copy(
            src_ref=face_ref,
            dst_ref=faces.at[index],
            send_sem=face_sems.at[0, index],
            recv_sem=face_sems.at[1, index],
            device_id=target(DIRECTIONS[index]),
            device_id_type=MESH,
        )

    for index in (4, 5, 6, 7, 0, 1, 2, 3):

        @pl.when(beside(DIRECTIONS[index], 1))
        def _():
            face_copy(index).start()

    for index in (4, 5, 6, 7, 0, 1, 2, 3):

        @pl.when(beside(DIRECTIONS[index], 1))
        def _():
            raw_copy(index).start()

    for load in loads[4:6]:
        load.wait()
    nodal_stage(
        plane_count, columns, rows, pos_ref, ten_ref, inc, xs, cell_ref, lane_ref, nodal
    )
    spread_stage(plane_count, columns, pos_ref.shape[2], cell_ref, lane_ref, nodal, acc, along, across, own_force)

    def force_copy(index):
        part = extent // 2
        start = part if index == 0 else 0
        return pltpu.make_async_remote_copy(
            src_ref=cubed(own_force).at[:, pl.ds(1, wide), pl.ds(start, part)],
            dst_ref=cubed(far_force).at[:, pl.ds(1, wide), pl.ds(part - start, part)],
            send_sem=force_sems.at[0, index],
            recv_sem=force_sems.at[1, index],
            device_id=target(DIRECTIONS[index]),
            device_id_type=MESH,
        )

    for index in range(2):

        @pl.when(beside(DIRECTIONS[index], 1))
        def _():
            force_copy(index).start()

    @pl.loop(1, share)
    def _(d):
        coarse_copy(d, lax.rem(slab + slabs - ways * d, slabs)).wait_recv()

    if ways == 2:
        relay().start()
        pltpu.make_async_remote_copy(
            src_ref=coarse_all.at[pl.ds(way * share, share)],
            dst_ref=coarse_all.at[pl.ds((1 - way) * share, share)],
            send_sem=coarse_sems.at[0, 0],
            recv_sem=coarse_sems.at[1, 0],
            device_id={"slab": slab + 1 - 2 * way, "cross": cross},
            device_id_type=MESH,
        ).wait_recv()

    for index in range(8):

        @pl.when(beside(DIRECTIONS[index], -1))
        def _():
            face_copy(index).wait_recv()

    slots = face_ref.shape[1]
    lanes = table.shape[1]
    chunks = coarse_ref.shape[1] // lanes
    together = table.shape[0] // (4 * chunks)
    groups = [[face_ref[pl.ds(k, 1), :] for k in range(3)]] + [
        [faces[index, pl.ds(k, 1), :] for k in range(3)] for index in range(8)
    ]
    wanted = [jnp.concatenate(group[1:], axis=1) for group in groups]
    one, zero = jnp.ones((), BF16), jnp.zeros((), BF16)
    picks = [
        jnp.where(
            lax.broadcasted_iota(I16, (lanes, 2 * slots), 0) == (index & (lanes - 1)).astype(I16),
            one, zero,
        )
        for index in wanted
    ]
    quarter = lax.shift_right_logical(
        lax.broadcasted_iota(I32, (table.shape[0], 2 * slots), 0), 2
    )

    def gather(base, found):
        for j in range(together):
            for chunk in range(chunks):
                table[pl.ds((j * chunks + chunk) * 4, 4), :] = coarse_all[
                    place_of(base * together + j), :, chunk * lanes : (chunk + 1) * lanes
                ]
        stacked = jnp.concatenate(split(table[...], 2), axis=0).astype(BF16)
        result = []
        for index, pick, total in zip(wanted, picks, found):
            both = jnp.dot(stacked, pick, preferred_element_type=F32)
            both = both[: table.shape[0]] + both[table.shape[0] :]
            high = lax.shift_right_logical(index, lanes.bit_length() - 1)
            both = jnp.where(quarter == high - base * (together * chunks), both, 0.0)
            for start in range(0, table.shape[0], 8):
                total = total + both[start : start + 8]
            result.append(total)
        return tuple(result)

    found = tuple(jnp.zeros((8, 2 * slots), F32) for _ in groups)
    if coarse_all.shape[0] == together:
        found = gather(0, found)
    else:
        found = lax.fori_loop(0, coarse_all.shape[0] // together, gather, found)
    blended = []
    for total in found:
        total = total[0:4] + total[4:8]
        blended.append(0.75 * total[:, :slots] + 0.25 * total[:, slots:])

    def spots(group):
        cell = group[0]
        used = cell >= 0
        line = cell // rows
        return used, line // columns, line % columns, jnp.where(used, cell % rows, -1)

    def put(size, goals, lane_rows, moments):
        mask = [lax.broadcasted_iota(I32, (size, slots), 0) == goal for goal in goals]
        pieces = [split(value, 2) for value in moments]
        left = [
            jnp.concatenate(
                [jnp.where(m, piece[part][k : k + 1], 0.0) for m, piece in zip(mask, pieces)], axis=1
            )
            for k in range(4)
            for part in range(2)
        ]
        left.append(jnp.concatenate([jnp.where(m, 1.0, 0.0) for m in mask], axis=1))
        right = jnp.concatenate(
            [
                jnp.where(lax.broadcasted_iota(I32, (rows, slots), 0) == lane, 1.0, 0.0)
                for lane in lane_rows
            ],
            axis=1,
        )
        out = lax.dot_general(
            jnp.concatenate(left, axis=0).astype(BF16), right.astype(BF16), NT,
            preferred_element_type=F32,
        )
        return [
            out[2 * k * size : (2 * k + 1) * size] + out[(2 * k + 1) * size : (2 * k + 2) * size]
            for k in range(4)
        ] + [out[8 * size : 9 * size]]

    used, plane, column, lane = spots(groups[0])
    goal = jnp.where(used, column * plane_count + plane, -1)
    for k, value in enumerate(put(columns * plane_count, [goal], [lane], blended[:1])):
        for c in range(columns):
            placed_ref[k, pl.ds((HALO + 1 + c) * extent + HALO, plane_count), :] = value[
                c * plane_count : (c + 1) * plane_count
            ]

    goals, lane_rows, offsets, offset = [], [], [], 0
    for index, (dz, dx) in enumerate(DIRECTIONS):
        used, plane, column, lane = spots(groups[1 + index])
        if dz:
            used = used & (plane == (plane_count - 1 if dz == 1 else 0))
        if dx:
            used = used & (column == (columns - 1 if dx == 1 else 0))
        along_edge = column if dx == 0 else plane if dz == 0 else jnp.zeros_like(plane)
        goals.append(jnp.where(used, along_edge + offset, -1))
        lane_rows.append(lane)
        offsets.append(offset)
        offset += columns if dx == 0 else plane_count if dz == 0 else 1
    for k, value in enumerate(put(round_up(offset, 16), goals, lane_rows, blended[1:])):
        for index, (dz, dx) in enumerate(DIRECTIONS):
            size = columns if dx == 0 else plane_count if dz == 0 else 1
            part = value[offsets[index] : offsets[index] + size]
            if k == 4:
                part = jnp.where(beside(DIRECTIONS[index], -1), part, 1.0)
            p = -1 if dz == 1 else plane_count
            c = HALO + (-1 if dx == 1 else columns)
            if dx == 0:
                placed_ref[k, plane_rows(p), :] = part
            elif dz == 0:
                placed_ref[k, pl.ds((c + 1) * extent + HALO, plane_count), :] = part
            else:
                placed_ref[k, pl.ds((c + 1) * extent + HALO + p, 1), :] = part

    for c in range(1, wide - 1):
        at = column_rows(c)
        density = placed_ref[0, at, :]
        velocity = [placed_ref[k, at, :] for k in range(1, 4)]
        for q, value in enumerate(equilibrium_pairs(density, velocity)):
            rim[q, at, :] = value

    for index in range(8):

        @pl.when(beside(DIRECTIONS[index], -1))
        def _():
            raw_copy(index).wait_recv()

    unpack(raw, RAW_MOVES, (raw_zrecv, raw_xrecv, raw_crecv))

    for index in range(2):

        @pl.when(beside(DIRECTIONS[index], -1))
        def _():
            force_copy(index).wait_recv()

    def pulled(source, at, starts):
        fixed = placed_ref[4, at, :] > 0.5
        fields = []
        for q, (cz, cx, cy) in enumerate(LATTICE_VECTORS):
            value = source[q, starts(cz, cx), :]
            if cy != 0:
                value = pltpu.roll(value, cy % rows, 1)
            fields.append(jnp.where(fixed, rim[q, at, :], value))
        return fields

    def pulled_column(source, c):
        return pulled(
            source,
            column_rows(c),
            lambda cz, cx: pl.ds((c + 1 - cx) * extent - cz, extent),
        )

    def pulled_plane(source, p):
        return pulled(source, plane_rows(p), lambda cz, cx: plane_rows(p, cz, cx))

    def inward(c, depth):
        if c < HALO:
            return [q for q in range(19) if LATTICE_VECTORS[q][1] >= HALO - c - depth]
        if c >= HALO + columns:
            return [q for q in range(19) if -LATTICE_VECTORS[q][1] >= c - HALO - columns + 1 - depth]
        return range(19)

    for c in range(wide):
        at = column_rows(c)
        rate = raw[RATE, at, :]
        fluid = rate > 0.0
        inverse = 1.0 / rate
        push = []
        for k in range(3):
            value = jnp.where(fluid, (own_force[k, at, :] + far_force[k, at, :]) * inverse, 0.0)
            pushed[k, at, :] = value
            push.append(value)
        momentum = [raw[MOMENTUM + k, at, :] for k in range(3)]
        needed = inward(c, 1)
        terms = pull_terms(raw[DENSITY, at, :], momentum, rate, push, needed)
        for q in needed:
            kept = raw[q, at, :]
            post_one[q, at, :] = jnp.where(fluid, kept + terms[q], kept)

    def collide_columns(source, sink):
        for c in range(1, wide - 1):
            at = column_rows(c)
            fields = pulled_column(source, c)
            push = [pushed[k, at, :] for k in range(3)]
            for q, value in collide(fields, raw[RATE, at, :], push, inward(c, 0)).items():
                sink[q, at, :] = value

    collide_columns(post_one, post_two)

    def send_halo(indices):
        for index in indices:

            @pl.when(beside(DIRECTIONS[index], 1))
            def _():
                halo_copy(index).start()

    for p in range(plane_count):
        at = plane_rows(p)
        fields = pulled_plane(post_two, p)
        push = [pushed[k, at, :] for k in range(3)]
        for q, value in collide(fields, raw[RATE, at, :], push).items():
            post_three[q, at, :] = value
            keep_plane(q, p, value, MOVES, zsend)
        if p == HALO - 1:
            send_halo([1])
    send_halo([0])
    pack_corners(post_three, MOVES, csend)
    send_halo([4, 5, 6, 7])
    pack_cross(post_three, MOVES, xsend)
    send_halo([2, 3])

    @pl.loop(1, share)
    def _(d):
        coarse_copy(d, slab).wait_send()

    if ways == 2:
        relay().wait_send()

    for index in range(8):

        @pl.when(beside(DIRECTIONS[index], 1))
        def _():
            raw_copy(index).wait_send()
            face_copy(index).wait_send()
            if index < 2:
                force_copy(index).wait_send()

    for index in range(8):

        @pl.when(beside(DIRECTIONS[index], -1))
        def _():
            halo_copy(index).wait_recv()

    for index in range(8):

        @pl.when(beside(DIRECTIONS[index], 1))
        def _():
            halo_copy(index).wait_send()

    unpack(post_three, MOVES, (zrecv, xrecv, crecv))
    collide_columns(post_three, post_one)

    for p in range(plane_count):
        for q, value in enumerate(pulled_plane(post_one, p)):
            next_ref[q, p] = value


def flow_kernel(fields_ref, next_ref, flow_ref, flow, sems):
    whole = pltpu.make_async_copy(fields_ref, next_ref, sems.at[0])
    whole.start()
    for p in range(fields_ref.shape[1]):
        fields = [fields_ref[q, p] for q in range(19)]
        density, momentum = moments_of(fields)
        inverse = ROOT_THREE / density
        for k in range(3):
            flow[k, p] = momentum[k] * inverse
    part = pltpu.make_async_copy(flow, flow_ref, sems.at[1])
    part.start()
    whole.wait()
    part.wait()


def coarse_rows(slabs, coarse_moments):
    count, width = coarse_moments.shape
    return math.gcd(slabs, 8) * count * (width // 128)


def on_device(
    slabs, crosses,
    populations, fluid_mask, relaxation, positions, triangles, tension, coarse_moments, interface,
):
    _, plane_count, columns, rows = populations.shape
    _, membranes, nodes = positions.shape
    padded = round_up(nodes, 128)
    corners = triangles.shape[1]
    half, planes = (columns + 6) // 2, plane_count + 2
    cells = round_up(planes * half, 16)
    flat = (columns + 2 * HALO + 2) * (plane_count + 2 * HALO)
    vmem = pl.BlockSpec(memory_space=pltpu.VMEM)
    block = (19, plane_count, columns, rows)
    operands = (
        triangles, populations, relaxation, fluid_mask, positions, tension, coarse_moments, interface,
    )
    fields = pl.pallas_call(
        functools.partial(lattice_kernel, slabs, crosses),
        name="lattice_steps",
        out_shape=pltpu.VMEM(block, F32),
        in_specs=[pl.BlockSpec(memory_space=pl.ANY)] * 8,
        out_specs=vmem,
        scratch_shapes=[pltpu.VMEM(operand.shape, operand.dtype) for operand in operands]
        + [
            pltpu.VMEM((3, membranes, padded), F32),
            pltpu.VMEM((padded, corners), BF16),
            pltpu.VMEM((3, membranes, padded), F32),
            pltpu.VMEM((membranes, padded), I32),
            pltpu.VMEM((membranes, padded), I32),
            pltpu.VMEM((6 * cells, 2 * rows), F32),
            pltpu.VMEM((3, half * planes + cells, rows), F32),
            pltpu.VMEM((3, (columns + 4) * planes + 16, rows), F32),
            pltpu.VMEM((CHANNELS, flat, rows), F32),
            pltpu.VMEM((3, flat, rows), F32),
            pltpu.VMEM((3, flat, rows), F32),
            pltpu.VMEM((3, flat, rows), F32),
            pltpu.VMEM((5, flat, rows), F32),
            pltpu.VMEM((19, flat, rows), F32),
            pltpu.VMEM((19, flat, rows), F32),
            pltpu.VMEM((19, flat, rows), F32),
            pltpu.VMEM((19, flat, rows), F32),
            pltpu.VMEM((slabs,) + coarse_moments.shape, F32),
            pltpu.VMEM((coarse_rows(slabs, coarse_moments), 128), F32),
            pltpu.VMEM((8,) + interface.shape, I32),
        ]
        + [
            pltpu.VMEM(shape, F32)
            for moves in (MOVES, MOVES, RAW_MOVES, RAW_MOVES)
            for shape in buffer_shapes(moves, plane_count, columns, rows)
        ]
        + [
            pltpu.SemaphoreType.DMA((8,)),
            pltpu.SemaphoreType.DMA((2, slabs)),
            pltpu.SemaphoreType.DMA((2, 8)),
            pltpu.SemaphoreType.DMA((2, 2)),
            pltpu.SemaphoreType.DMA((2, 8)),
            pltpu.SemaphoreType.DMA((2, 8)),
        ],
        compiler_params=pltpu.CompilerParams(collective_id=0, has_side_effects=True),
    )(*operands)
    return pl.pallas_call(
        flow_kernel,
        name="flow",
        out_shape=(
            jax.ShapeDtypeStruct(block, F32),
            jax.ShapeDtypeStruct((3,) + block[1:], F32),
        ),
        in_specs=[vmem],
        out_specs=(pl.BlockSpec(memory_space=pl.ANY),) * 2,
        scratch_shapes=[pltpu.VMEM((3,) + block[1:], F32), pltpu.SemaphoreType.DMA((2,))],
    )(pltpu.with_memory_space_constraint(fields, pltpu.VMEM))


def solution(mesh):
    in_specs = (
        P(None, "slab", "cross", None),
        P("slab", "cross", None),
        P("slab", "cross", None),
        P(None, "slab", None),
        P(),
        P("slab", None),
        P(None, "slab"),
        P(None, ("slab", "cross")),
    )
    out_specs = (P(None, "slab", "cross", None), P(None, "slab", "cross", None))
    return jax.shard_map(
        functools.partial(on_device, mesh.shape["slab"], mesh.shape["cross"]),
        mesh=mesh, in_specs=in_specs, out_specs=out_specs, check_vma=False,
    )
```

```python
import functools
import math

import jax
import jax.numpy as jnp
from jax import lax
from jax.experimental import pallas as pl
from jax.experimental.pallas import tpu as pltpu
from jax.sharding import PartitionSpec as P

STEPS = 4
MESH = pl.DeviceIdType.MESH
LATTICE_VECTORS = [
    (0, 0, 0),
    (1, 0, 0),
    (-1, 0, 0),
    (0, 1, 0),
    (0, -1, 0),
    (0, 0, 1),
    (0, 0, -1),
    (1, 1, 0),
    (-1, -1, 0),
    (1, -1, 0),
    (-1, 1, 0),
    (1, 0, 1),
    (-1, 0, -1),
    (1, 0, -1),
    (-1, 0, 1),
    (0, 1, 1),
    (0, -1, -1),
    (0, 1, -1),
    (0, -1, 1),
]
LATTICE_WEIGHTS = [1.0 / 3.0] + [1.0 / 18.0] * 6 + [1.0 / 36.0] * 12
OPPOSITE = [0] + [q + 1 if q % 2 == 1 else q - 1 for q in range(1, 19)]
ROOT_THREE = math.sqrt(3.0)
DIRECTIONS = [(1, 0), (-1, 0), (0, 1), (0, -1), (1, 1), (-1, -1), (1, -1), (-1, 1)]
NT = (((1,), (1,)), ((), ()))
F32, BF16, I32, I16 = jnp.float32, jnp.bfloat16, jnp.int32, jnp.int16
HALO = 2


def slab_moves(extra):
    return [
        [
            (q, depth)
            for depth in (1, 2)
            for q in [m for m in range(19) if LATTICE_VECTORS[m][0] * sign >= depth - 1] + extra
        ]
        for sign in (1, -1)
    ]


def cross_moves(extra):
    return [
        [
            (q, depth)
            for depth in (1, 2)
            for q in [m for m in range(19) if LATTICE_VECTORS[m][1] * sign >= depth - 1] + extra
        ]
        for sign in (1, -1)
    ]


def corner_moves(extra):
    return [
        [
            (q, dz, dx)
            for dz in (1, 2)
            for dx in (1, 2)
            for q in [
                m
                for m in range(19)
                if LATTICE_VECTORS[m][0] * sz >= dz - 1 and LATTICE_VECTORS[m][1] * sx >= dx - 1
            ]
            + extra
        ]
        for sz, sx in DIRECTIONS[4:]
    ]


RATE, DENSITY, MOMENTUM, CHANNELS = 19, 20, 21, 24
MOVES = (slab_moves([]), cross_moves([]), corner_moves([]))
EXTRA = list(range(19, CHANNELS))
RAW_MOVES = (slab_moves(EXTRA), cross_moves(EXTRA), corner_moves(EXTRA))


def buffer_shapes(moves, plane_count, columns, rows):
    return [
        (2, len(moves[0][0]), columns, rows),
        (2, round_up(len(moves[1][0]) * plane_count, 8), rows),
        (4, round_up(len(moves[2][0]), 8), rows),
    ]


def round_up(value, unit):
    return (value + unit - 1) // unit * unit


def split(value, parts):
    pieces = []
    for _ in range(parts):
        piece = value.astype(BF16).astype(F32)
        pieces.append(piece)
        value = value - piece
    return pieces


def incidence_stage(tri_ref, inc, nodes):
    triangles = tri_ref.shape[1]
    tiles = triangles // 128
    corners = [
        [
            jnp.broadcast_to(tri_ref[pl.ds(k, 1), t * 128 : (t + 1) * 128], (16, 128)).astype(I16)
            for t in range(tiles)
        ]
        for k in range(3)
    ]
    iota = lax.broadcasted_iota(I32, (16, 128), 0)
    zero, one = jnp.zeros((16, 128), BF16), jnp.ones((16, 128), BF16)

    def rows_at(start):
        ids = (iota + start).astype(I16)
        for t in range(tiles):
            value = zero
            for k in range(3):
                value = jnp.where(ids == corners[k][t], one, value)
            inc[pl.ds(start, 16), t * 128 : (t + 1) * 128] = value

    chunk = 128

    @pl.loop(0, nodes // chunk)
    def _(i):
        for r in range(chunk // 16):
            rows_at(pl.multiple_of(i * chunk + r * 16, 16))

    done = nodes // chunk * chunk
    while done < nodes:
        rows_at(done)
        done += 16
    if done < inc.shape[0]:
        inc[done:, :] = jnp.zeros((inc.shape[0] - done, triangles), BF16)


def nodal_stage(plane_count, columns, rows, pos_ref, ten_ref, inc, xs, cell_ref, lane_ref, force):
    dims, membranes, nodes = pos_ref.shape
    padded = xs.shape[2]
    slab = lax.axis_index("slab")
    cross = lax.axis_index("cross")
    planes, half = plane_count + 2, (columns + 6) // 2

    cell_ref[...] = jnp.full(cell_ref.shape, -1, I32)
    lane_ref[...] = jnp.full(lane_ref.shape, -1, I32)
    plane = pos_ref[0] - (slab * plane_count - 1)
    column = pos_ref[1] - (cross * columns - 3)
    row = pos_ref[2]
    inside = (column >= 0) & (column < 2 * half)
    upper = column >= half
    cell = jnp.where(upper, column - half, column) * planes + plane
    cell_ref[:, :nodes] = jnp.where(inside, cell, -1)
    lane_ref[:, :nodes] = row + jnp.where(upper, rows, 0)

    xs[...] = jnp.zeros_like(xs)
    for k in range(3):
        xs[k, :, :nodes] = (pos_ref[k] - pos_ref[k, :, 0:1]).astype(F32)

    coords = xs[...].reshape(dims * membranes, padded)
    sums = jnp.dot(coords.astype(BF16), inc[...], preferred_element_type=F32)
    tension = ten_ref[...]
    terms = jnp.concatenate(
        [sums[k * membranes : (k + 1) * membranes] * tension for k in range(3)] + [tension], axis=0
    )
    stacked = jnp.concatenate(split(terms, 2), axis=0).astype(BF16)
    gathered = lax.dot_general(stacked, inc[...], NT, preferred_element_type=F32)
    count = terms.shape[0]
    total = gathered[:count] + gathered[count:]
    weight = total[3 * membranes :]
    for k in range(3):
        force[k] = total[k * membranes : (k + 1) * membranes] - 3.0 * xs[k] * weight


def spread_stage(plane_count, columns, nodes, cell_ref, lane_ref, force, acc, along, across, out_ref, ready):
    _, membranes, padded = force.shape
    rows = out_ref.shape[2]
    planes, half = plane_count + 2, (columns + 6) // 2
    extent = plane_count + 2 * HALO
    cells = acc.shape[0] // 6
    unroll = 4 if membranes % 4 == 0 else 1
    zero, one = jnp.zeros((), BF16), jnp.ones((), BF16)

    main = nodes // 128 * 128
    tail = nodes - main
    packed = 0 < tail * membranes <= 128
    if not packed:
        main = padded

    def one_hots(cell, lane, force_rows):
        mask = lax.broadcasted_iota(I16, (cells, cell.shape[1]), 0) == cell.astype(I16)
        values = [split(value, 2) for value in force_rows]
        left = jnp.concatenate(
            [
                jnp.where(mask, values[k][part].astype(BF16), zero)
                for part in range(2)
                for k in range(3)
            ],
            axis=0,
        )
        ids = lax.broadcasted_iota(I16, (2 * rows, cell.shape[1]), 0)
        return left, jnp.where(ids == lane.astype(I16), one, zero)

    def gathered_tail(value):
        lanes = lax.broadcasted_iota(I32, (membranes, 128), 1)
        value = jnp.where(lanes < tail, value, jnp.zeros_like(value))
        value = pltpu.roll(value, 0, 1, stride=tail, stride_axis=0)
        return jnp.sum(value, axis=0, keepdims=True)

    if packed:
        ends = slice(main, main + 128)
        left, right = one_hots(
            gathered_tail(cell_ref[:, ends] + 1) - 1,
            gathered_tail(lane_ref[:, ends] + 1) - 1,
            [gathered_tail(force[k, :, ends]) for k in range(3)],
        )
        acc[...] = lax.dot_general(left, right, NT, preferred_element_type=F32)
    else:
        acc[...] = jnp.zeros_like(acc)

    @pl.loop(0, membranes // unroll)
    def _(i):
        parts = []
        for inner in range(unroll):
            m = pl.ds(i * unroll + inner, 1)
            parts.append(
                one_hots(
                    cell_ref[m, :main], lane_ref[m, :main], [force[k, m, :main] for k in range(3)]
                )
            )
        left, right = (jnp.concatenate(side, axis=1) for side in zip(*parts))
        acc[...] += lax.dot_general(left, right, NT, preferred_element_type=F32)

    used = half * planes
    inner = (columns + 4) * planes
    step = lax.broadcasted_iota(I32, (extent, rows), 0)
    weights = [
        jnp.where((step >= 2 - shift) & (step < planes + 2 - shift), w, 0.0)
        for shift, w in ((0, 0.25), (1, 0.5), (2, 0.25))
    ]
    for k in range(3):
        value = acc[k * cells : (k + 1) * cells] + acc[(3 + k) * cells : (4 + k) * cells]
        for part in range(2):
            b = value[:, part * rows : (part + 1) * rows]
            b = 0.5 * b + 0.25 * (pltpu.roll(b, 1, 1) + pltpu.roll(b, rows - 1, 1))
            along[k, part * used : part * used + cells] = b
        across[k, 0:8] = jnp.zeros((8, rows), F32)
        across[k, 8 + inner : 16 + inner] = jnp.zeros((8, rows), F32)
        across[k, 8 : 8 + inner] = 0.5 * along[k, planes : planes + inner] + 0.25 * (
            along[k, 0:inner] + along[k, 2 * planes : 2 * planes + inner]
        )
        for c in range(columns + 4):
            start = 8 + c * planes
            out_ref[k, (c + 1) * extent : (c + 2) * extent] = (
                weights[0] * across[k, start - 2 : start - 2 + extent]
                + weights[1] * across[k, start - 1 : start - 1 + extent]
                + weights[2] * across[k, start : start + extent]
            )
        ready(k)


def equilibrium_pairs(density, velocity):
    squared = velocity[0] * velocity[0] + velocity[1] * velocity[1] + velocity[2] * velocity[2]
    base = 1.0 - 1.5 * squared
    result = [None] * 19
    result[0] = LATTICE_WEIGHTS[0] * density * base
    scaled = {w: w * density for w in (1.0 / 18.0, 1.0 / 36.0)}
    for q in range(1, 19, 2):
        projected = None
        for c, v in zip(LATTICE_VECTORS[q], velocity):
            if c == 0:
                continue
            if projected is None:
                projected = v if c == 1 else -v
            else:
                projected = projected + v if c == 1 else projected - v
        even = base + 4.5 * projected * projected
        odd = 3.0 * projected
        weight = scaled[LATTICE_WEIGHTS[q]]
        result[q] = weight * (even + odd)
        result[q + 1] = weight * (even - odd)
    return result


def moments_of(fields):
    density = functools.reduce(lambda a, b: a + b, fields)
    momentum = []
    for k in range(3):
        plus = [fields[q] for q in range(19) if LATTICE_VECTORS[q][k] == 1]
        minus = [fields[q] for q in range(19) if LATTICE_VECTORS[q][k] == -1]
        momentum.append(functools.reduce(lambda a, b: a + b, [a - b for a, b in zip(plus, minus)]))
    return density, momentum


def local_moments(fields):
    gaps = [fields[q] - fields[q + 1] for q in range(1, 19, 2)]
    sums = [fields[q] + fields[q + 1] for q in range(1, 19, 2)]
    density = functools.reduce(lambda a, b: a + b, sums) + fields[0]
    momentum = []
    for k in range(3):
        total = None
        for pair in range(9):
            c = LATTICE_VECTORS[2 * pair + 1][k]
            if c and total is None:
                total = gaps[pair]
            elif c:
                total = total + gaps[pair] if c == 1 else total - gaps[pair]
        momentum.append(total)
    return density, momentum


def pull_terms(density, momentum, rate, pushed, needed):
    scale = 3.0 / density
    tripled = [(m + p) * scale for m, p in zip(momentum, pushed)]
    squared = tripled[0] * tripled[0] + tripled[1] * tripled[1] + tripled[2] * tripled[2]
    base = 1.0 - (1.0 / 6.0) * squared
    strength = rate * density
    scaled = {w: w * strength for w in (1.0 / 18.0, 1.0 / 36.0)}
    result = [None] * 19
    result[0] = (LATTICE_WEIGHTS[0] * strength) * base
    for q in range(1, 19, 2):
        if q not in needed and q + 1 not in needed:
            continue
        projected = None
        for c, v in zip(LATTICE_VECTORS[q], tripled):
            if c == 0:
                continue
            if projected is None:
                projected = v if c == 1 else -v
            else:
                projected = projected + v if c == 1 else projected - v
        weight = scaled[LATTICE_WEIGHTS[q]]
        even = weight * (base + 0.5 * projected * projected)
        odd = weight * projected
        result[q] = even + odd
        result[q + 1] = even - odd
    return result


def collide(fields, rate, pushed, needed=range(19)):
    density, momentum = local_moments(fields)
    terms = pull_terms(density, momentum, rate, pushed, needed)
    fluid = rate > 0.0
    keep = 1.0 - rate
    return {q: jnp.where(fluid, keep * fields[q] + terms[q], fields[OPPOSITE[q]]) for q in needed}


def lattice_kernel(
    slabs, crosses,
    tri_hbm, pop_hbm, relax_hbm, fluid_hbm, pos_hbm, ten_hbm, coarse_hbm, face_hbm,
    next_ref,
    tri_ref, pop_ref, relax_ref, fluid_ref, pos_ref, ten_ref, coarse_ref, face_ref,
    xs, inc, nodal, cell_ref, lane_ref, acc, along, across,
    raw, own_force, far_force, pushed, placed_ref, rim, post_one, post_two, post_three,
    coarse_all, table, faces,
    zsend, xsend, csend, zrecv, xrecv, crecv,
    raw_zsend, raw_xsend, raw_csend, raw_zrecv, raw_xrecv, raw_crecv,
    load_sems, coarse_sems, raw_sems, force_sems, face_sems, halo_sems,
):
    _, plane_count, columns, rows = pop_ref.shape
    extent, wide = plane_count + 2 * HALO, columns + 2 * HALO
    slab = lax.axis_index("slab")
    cross = lax.axis_index("cross")

    def beside(direction, sign):
        dz, dx = direction[0] * sign, direction[1] * sign
        conditions = []
        if dz == 1:
            conditions.append(slab < slabs - 1)
        if dz == -1:
            conditions.append(slab > 0)
        if dx == 1:
            conditions.append(cross < crosses - 1)
        if dx == -1:
            conditions.append(cross > 0)
        return functools.reduce(jnp.logical_and, conditions)

    def target(direction):
        return {"slab": slab + direction[0], "cross": cross + direction[1]}

    def cubed(ref):
        return ref.reshape(ref.shape[0], wide + 2, extent, rows)

    def inner_row(step, depth, size):
        return HALO + (size - depth if step == 1 else depth - 1)

    def outer_row(step, depth, size):
        return HALO + (-depth if step == 1 else size - 1 + depth)

    def pack_corners(source, moves, buffer):
        for side in range(4):
            sz, sx = DIRECTIONS[4 + side]
            for e, (q, dz, dx) in enumerate(moves[2][side]):
                row = (inner_row(sx, dx, columns) + 1) * extent + inner_row(sz, dz, plane_count)
                buffer[side, pl.ds(e, 1), :] = source[q, pl.ds(row, 1), :]

    def pack_cross(source, moves, buffer):
        for side in range(2):
            for e, (q, depth) in enumerate(moves[1][side]):
                row = (inner_row(DIRECTIONS[2 + side][1], depth, columns) + 1) * extent + HALO
                buffer[side, pl.ds(e * plane_count, plane_count), :] = source[
                    q, pl.ds(row, plane_count), :
                ]

    def unpack(sink, moves, buffers):
        for side in range(2):
            for e, (q, depth) in enumerate(moves[0][side]):
                row = outer_row(DIRECTIONS[side][0], depth, plane_count)
                sink[q, plane_rows(row - HALO), :] = buffers[0][side, e]
            for e, (q, depth) in enumerate(moves[1][side]):
                row = (outer_row(DIRECTIONS[2 + side][1], depth, columns) + 1) * extent + HALO
                sink[q, pl.ds(row, plane_count), :] = buffers[1][
                    side, pl.ds(e * plane_count, plane_count), :
                ]
        for side in range(4):
            sz, sx = DIRECTIONS[4 + side]
            for e, (q, dz, dx) in enumerate(moves[2][side]):
                row = (outer_row(sx, dx, columns) + 1) * extent + outer_row(sz, dz, plane_count)
                sink[q, pl.ds(row, 1), :] = buffers[2][side, pl.ds(e, 1), :]

    def keep_plane(q, p, value, moves, buffer):
        for side in range(2):
            entry = (q, plane_count - p if side == 0 else p + 1)
            if entry in moves[0][side]:
                buffer[side, moves[0][side].index(entry)] = value

    def buffers_copy(sources, sinks, sems, index):
        kind, place = (0, index) if index < 2 else (1, index - 2) if index < 4 else (2, index - 4)
        return pltpu.make_async_remote_copy(
            src_ref=sources[kind].at[place],
            dst_ref=sinks[kind].at[place],
            send_sem=sems.at[0, index],
            recv_sem=sems.at[1, index],
            device_id=target(DIRECTIONS[index]),
            device_id_type=MESH,
        )

    def halo_copy(index):
        return buffers_copy((zsend, xsend, csend), (zrecv, xrecv, crecv), halo_sems, index)

    def raw_copy(index):
        return buffers_copy(
            (raw_zsend, raw_xsend, raw_csend), (raw_zrecv, raw_xrecv, raw_crecv), raw_sems, index
        )

    def column_rows(c):
        return pl.ds((c + 1) * extent, extent)

    def plane_rows(p, dz=0, dx=0):
        return pl.ds((HALO + 1 - dx) * extent + HALO + p - dz, columns, stride=extent)

    loads = [
        pltpu.make_async_copy(source, sink, load_sems.at[i])
        for i, (source, sink) in enumerate(
            (
                (tri_hbm, tri_ref),
                (pop_hbm, pop_ref),
                (relax_hbm, relax_ref),
                (fluid_hbm, fluid_ref),
                (pos_hbm, pos_ref),
                (ten_hbm, ten_ref),
                (coarse_hbm, coarse_ref),
                (face_hbm, face_ref),
            )
        )
    ]
    for load in loads:
        load.start()

    barrier = pltpu.get_barrier_semaphore()

    @pl.loop(1, slabs)
    def _(d):
        peer = lax.rem(slab + d, slabs)
        pl.semaphore_signal(
            barrier, inc=1, device_id={"slab": peer, "cross": cross}, device_id_type=MESH
        )

    expected = slabs - 1
    for direction in DIRECTIONS:
        if direction[1] == 0:
            continue
        there = beside(direction, 1)
        expected = expected + jnp.where(there, 1, 0)

        @pl.when(there)
        def _():
            pl.semaphore_signal(
                barrier, inc=1, device_id=target(direction), device_id_type=MESH
            )

    def clear(side):
        kind, place = (0, side) if side < 2 else (1, side - 2) if side < 4 else (2, side - 4)
        for sinks in ((zrecv, xrecv, crecv), (raw_zrecv, raw_xrecv, raw_crecv)):
            sinks[kind][place] = jnp.zeros(sinks[kind].shape[1:], F32)
        faces[side] = jnp.full(faces.shape[1:], -1, I32)
        if side < 2:
            near = side * (extent // 2)
            for c in range(wide):
                for k in range(3):
                    far_force[k, pl.ds((c + 1) * extent + near, extent // 2), :] = jnp.zeros(
                        (extent // 2, rows), F32
                    )

    for side in range(8):

        @pl.when(jnp.logical_not(beside(DIRECTIONS[side], -1)))
        def _():
            clear(side)

    loads[0].wait()
    incidence_stage(tri_ref, inc, pos_ref.shape[2])
    for load in loads[1:4]:
        load.wait()
    for p in range(plane_count):
        at = plane_rows(p)
        fields = [pop_ref[q, p] for q in range(19)]
        density, momentum = local_moments(fields)
        fluid = fluid_ref[p] == 1
        keep = 1.0 - relax_ref[p]
        values = [jnp.where(fluid, keep * fields[q], fields[OPPOSITE[q]]) for q in range(19)]
        values += [jnp.where(fluid, relax_ref[p], 0.0), density] + momentum
        for q, value in enumerate(values):
            raw[q, at, :] = value
            keep_plane(q, p, value, RAW_MOVES, raw_zsend)
    pack_corners(raw, RAW_MOVES, raw_csend)
    pack_cross(raw, RAW_MOVES, raw_xsend)
    loads[6].wait()
    pl.semaphore_wait(barrier, expected)

    ways = 2 if slabs % 2 == 0 else 1
    share = slabs // ways
    way = slab % ways

    def place_of(index):
        return index % ways * share + index // ways

    coarse_all[place_of(slab)] = coarse_ref[...]

    def coarse_copy(d, sink):
        return pltpu.make_async_remote_copy(
            src_ref=coarse_ref,
            dst_ref=coarse_all.at[place_of(sink)],
            send_sem=coarse_sems.at[0, d],
            recv_sem=coarse_sems.at[1, d],
            device_id={"slab": lax.rem(slab + ways * d, slabs), "cross": cross},
            device_id_type=MESH,
        )

    def relay():
        half = coarse_all.at[pl.ds(way * share, share)]
        return pltpu.make_async_remote_copy(
            src_ref=half,
            dst_ref=half,
            send_sem=coarse_sems.at[0, 0],
            recv_sem=coarse_sems.at[1, 0],
            device_id={"slab": slab + 1 - 2 * way, "cross": cross},
            device_id_type=MESH,
        )

    @pl.loop(1, share)
    def _(d):
        coarse_copy(d, slab).start()

    loads[7].wait()

    def face_copy(index):
        return pltpu.make_async_remote_copy(
            src_ref=face_ref,
            dst_ref=faces.at[index],
            send_sem=face_sems.at[0, index],
            recv_sem=face_sems.at[1, index],
            device_id=target(DIRECTIONS[index]),
            device_id_type=MESH,
        )

    for index in (4, 5, 6, 7, 0, 1, 2, 3):

        @pl.when(beside(DIRECTIONS[index], 1))
        def _():
            face_copy(index).start()

    for index in (4, 5, 6, 7, 0, 1, 2, 3):

        @pl.when(beside(DIRECTIONS[index], 1))
        def _():
            raw_copy(index).start()

    for load in loads[4:6]:
        load.wait()
    nodal_stage(
        plane_count, columns, rows, pos_ref, ten_ref, inc, xs, cell_ref, lane_ref, nodal
    )
    def force_copy(index, k):
        part = extent // 2
        start = part if index == 0 else 0
        return pltpu.make_async_remote_copy(
            src_ref=cubed(own_force).at[pl.ds(k, 1), pl.ds(1, wide), pl.ds(start, part)],
            dst_ref=cubed(far_force).at[pl.ds(k, 1), pl.ds(1, wide), pl.ds(part - start, part)],
            send_sem=force_sems.at[0, 3 * index + k],
            recv_sem=force_sems.at[1, 3 * index + k],
            device_id=target(DIRECTIONS[index]),
            device_id_type=MESH,
        )

    def send_force(k):
        for index in range(2):

            @pl.when(beside(DIRECTIONS[index], 1))
            def _():
                force_copy(index, k).start()

    spread_stage(
        plane_count, columns, pos_ref.shape[2], cell_ref, lane_ref, nodal, acc, along, across, own_force,
        send_force,
    )

    @pl.loop(1, share)
    def _(d):
        coarse_copy(d, lax.rem(slab + slabs - ways * d, slabs)).wait_recv()

    if ways == 2:
        relay().start()
        pltpu.make_async_remote_copy(
            src_ref=coarse_all.at[pl.ds(way * share, share)],
            dst_ref=coarse_all.at[pl.ds((1 - way) * share, share)],
            send_sem=coarse_sems.at[0, 0],
            recv_sem=coarse_sems.at[1, 0],
            device_id={"slab": slab + 1 - 2 * way, "cross": cross},
            device_id_type=MESH,
        ).wait_recv()

    for index in range(8):

        @pl.when(beside(DIRECTIONS[index], -1))
        def _():
            face_copy(index).wait_recv()

    slots = face_ref.shape[1]
    lanes = table.shape[1]
    chunks = coarse_ref.shape[1] // lanes
    together = table.shape[0] // (4 * chunks)
    groups = [[face_ref[pl.ds(k, 1), :] for k in range(3)]] + [
        [faces[index, pl.ds(k, 1), :] for k in range(3)] for index in range(8)
    ]
    wanted = [jnp.concatenate(group[1:], axis=1) for group in groups]
    one, zero = jnp.ones((), BF16), jnp.zeros((), BF16)
    picks = [
        jnp.where(
            lax.broadcasted_iota(I16, (lanes, 2 * slots), 0) == (index & (lanes - 1)).astype(I16),
            one, zero,
        )
        for index in wanted
    ]
    quarter = lax.shift_right_logical(
        lax.broadcasted_iota(I32, (table.shape[0], 2 * slots), 0), 2
    )

    def gather(base, found):
        for j in range(together):
            for chunk in range(chunks):
                table[pl.ds((j * chunks + chunk) * 4, 4), :] = coarse_all[
                    place_of(base * together + j), :, chunk * lanes : (chunk + 1) * lanes
                ]
        stacked = jnp.concatenate(split(table[...], 2), axis=0).astype(BF16)
        result = []
        for index, pick, total in zip(wanted, picks, found):
            both = jnp.dot(stacked, pick, preferred_element_type=F32)
            both = both[: table.shape[0]] + both[table.shape[0] :]
            high = lax.shift_right_logical(index, lanes.bit_length() - 1)
            both = jnp.where(quarter == high - base * (together * chunks), both, 0.0)
            for start in range(0, table.shape[0], 8):
                total = total + both[start : start + 8]
            result.append(total)
        return tuple(result)

    found = tuple(jnp.zeros((8, 2 * slots), F32) for _ in groups)
    if coarse_all.shape[0] == together:
        found = gather(0, found)
    else:
        found = lax.fori_loop(0, coarse_all.shape[0] // together, gather, found)
    blended = []
    for total in found:
        total = total[0:4] + total[4:8]
        blended.append(0.75 * total[:, :slots] + 0.25 * total[:, slots:])

    def spots(group):
        cell = group[0]
        used = cell >= 0
        line = cell // rows
        return used, line // columns, line % columns, jnp.where(used, cell % rows, -1)

    def put(size, goals, lane_rows, moments):
        mask = [lax.broadcasted_iota(I32, (size, slots), 0) == goal for goal in goals]
        pieces = [split(value, 2) for value in moments]
        left = [
            jnp.concatenate(
                [jnp.where(m, piece[part][k : k + 1], 0.0) for m, piece in zip(mask, pieces)], axis=1
            )
            for k in range(4)
            for part in range(2)
        ]
        left.append(jnp.concatenate([jnp.where(m, 1.0, 0.0) for m in mask], axis=1))
        right = jnp.concatenate(
            [
                jnp.where(lax.broadcasted_iota(I32, (rows, slots), 0) == lane, 1.0, 0.0)
                for lane in lane_rows
            ],
            axis=1,
        )
        out = lax.dot_general(
            jnp.concatenate(left, axis=0).astype(BF16), right.astype(BF16), NT,
            preferred_element_type=F32,
        )
        return [
            out[2 * k * size : (2 * k + 1) * size] + out[(2 * k + 1) * size : (2 * k + 2) * size]
            for k in range(4)
        ] + [out[8 * size : 9 * size]]

    used, plane, column, lane = spots(groups[0])
    goal = jnp.where(used, column * plane_count + plane, -1)
    for k, value in enumerate(put(columns * plane_count, [goal], [lane], blended[:1])):
        for c in range(columns):
            placed_ref[k, pl.ds((HALO + 1 + c) * extent + HALO, plane_count), :] = value[
                c * plane_count : (c + 1) * plane_count
            ]

    goals, lane_rows, offsets, offset = [], [], [], 0
    for index, (dz, dx) in enumerate(DIRECTIONS):
        used, plane, column, lane = spots(groups[1 + index])
        if dz:
            used = used & (plane == (plane_count - 1 if dz == 1 else 0))
        if dx:
            used = used & (column == (columns - 1 if dx == 1 else 0))
        along_edge = column if dx == 0 else plane if dz == 0 else jnp.zeros_like(plane)
        goals.append(jnp.where(used, along_edge + offset, -1))
        lane_rows.append(lane)
        offsets.append(offset)
        offset += columns if dx == 0 else plane_count if dz == 0 else 1
    for k, value in enumerate(put(round_up(offset, 16), goals, lane_rows, blended[1:])):
        for index, (dz, dx) in enumerate(DIRECTIONS):
            size = columns if dx == 0 else plane_count if dz == 0 else 1
            part = value[offsets[index] : offsets[index] + size]
            if k == 4:
                part = jnp.where(beside(DIRECTIONS[index], -1), part, 1.0)
            p = -1 if dz == 1 else plane_count
            c = HALO + (-1 if dx == 1 else columns)
            if dx == 0:
                placed_ref[k, plane_rows(p), :] = part
            elif dz == 0:
                placed_ref[k, pl.ds((c + 1) * extent + HALO, plane_count), :] = part
            else:
                placed_ref[k, pl.ds((c + 1) * extent + HALO + p, 1), :] = part

    for c in range(1, wide - 1):
        at = column_rows(c)
        density = placed_ref[0, at, :]
        velocity = [placed_ref[k, at, :] for k in range(1, 4)]
        for q, value in enumerate(equilibrium_pairs(density, velocity)):
            rim[q, at, :] = value

    for index in range(8):

        @pl.when(beside(DIRECTIONS[index], -1))
        def _():
            raw_copy(index).wait_recv()

    unpack(raw, RAW_MOVES, (raw_zrecv, raw_xrecv, raw_crecv))

    for index in range(2):

        @pl.when(beside(DIRECTIONS[index], -1))
        def _():
            for k in range(3):
                force_copy(index, k).wait_recv()

    def pulled(source, at, starts):
        fixed = placed_ref[4, at, :] > 0.5
        fields = []
        for q, (cz, cx, cy) in enumerate(LATTICE_VECTORS):
            value = source[q, starts(cz, cx), :]
            if cy != 0:
                value = pltpu.roll(value, cy % rows, 1)
            fields.append(jnp.where(fixed, rim[q, at, :], value))
        return fields

    def pulled_column(source, c):
        return pulled(
            source,
            column_rows(c),
            lambda cz, cx: pl.ds((c + 1 - cx) * extent - cz, extent),
        )

    def pulled_plane(source, p):
        return pulled(source, plane_rows(p), lambda cz, cx: plane_rows(p, cz, cx))

    def inward(c, depth):
        if c < HALO:
            return [q for q in range(19) if LATTICE_VECTORS[q][1] >= HALO - c - depth]
        if c >= HALO + columns:
            return [q for q in range(19) if -LATTICE_VECTORS[q][1] >= c - HALO - columns + 1 - depth]
        return range(19)

    for c in range(wide):
        at = column_rows(c)
        rate = raw[RATE, at, :]
        fluid = rate > 0.0
        inverse = 1.0 / rate
        push = []
        for k in range(3):
            value = jnp.where(fluid, (own_force[k, at, :] + far_force[k, at, :]) * inverse, 0.0)
            pushed[k, at, :] = value
            push.append(value)
        momentum = [raw[MOMENTUM + k, at, :] for k in range(3)]
        needed = inward(c, 1)
        terms = pull_terms(raw[DENSITY, at, :], momentum, rate, push, needed)
        for q in needed:
            kept = raw[q, at, :]
            post_one[q, at, :] = jnp.where(fluid, kept + terms[q], kept)

    def collide_columns(source, sink):
        for c in range(1, wide - 1):
            at = column_rows(c)
            fields = pulled_column(source, c)
            push = [pushed[k, at, :] for k in range(3)]
            for q, value in collide(fields, raw[RATE, at, :], push, inward(c, 0)).items():
                sink[q, at, :] = value

    collide_columns(post_one, post_two)

    def send_halo(indices):
        for index in indices:

            @pl.when(beside(DIRECTIONS[index], 1))
            def _():
                halo_copy(index).start()

    for p in range(plane_count):
        at = plane_rows(p)
        fields = pulled_plane(post_two, p)
        push = [pushed[k, at, :] for k in range(3)]
        for q, value in collide(fields, raw[RATE, at, :], push).items():
            post_three[q, at, :] = value
            keep_plane(q, p, value, MOVES, zsend)
        if p == HALO - 1:
            send_halo([1])
    send_halo([0])
    pack_corners(post_three, MOVES, csend)
    send_halo([4, 5, 6, 7])
    pack_cross(post_three, MOVES, xsend)
    send_halo([2, 3])

    @pl.loop(1, share)
    def _(d):
        coarse_copy(d, slab).wait_send()

    if ways == 2:
        relay().wait_send()

    for index in range(8):

        @pl.when(beside(DIRECTIONS[index], 1))
        def _():
            raw_copy(index).wait_send()
            face_copy(index).wait_send()
            if index < 2:
                for k in range(3):
                    force_copy(index, k).wait_send()

    for index in range(8):

        @pl.when(beside(DIRECTIONS[index], -1))
        def _():
            halo_copy(index).wait_recv()

    for index in range(8):

        @pl.when(beside(DIRECTIONS[index], 1))
        def _():
            halo_copy(index).wait_send()

    unpack(post_three, MOVES, (zrecv, xrecv, crecv))
    collide_columns(post_three, post_one)

    for p in range(plane_count):
        for q, value in enumerate(pulled_plane(post_one, p)):
            next_ref[q, p] = value


def flow_kernel(fields_ref, next_ref, flow_ref, flow, sems):
    whole = pltpu.make_async_copy(fields_ref, next_ref, sems.at[0])
    whole.start()
    for p in range(fields_ref.shape[1]):
        fields = [fields_ref[q, p] for q in range(19)]
        density, momentum = moments_of(fields)
        inverse = ROOT_THREE / density
        for k in range(3):
            flow[k, p] = momentum[k] * inverse
    part = pltpu.make_async_copy(flow, flow_ref, sems.at[1])
    part.start()
    whole.wait()
    part.wait()


def coarse_rows(slabs, coarse_moments):
    count, width = coarse_moments.shape
    return math.gcd(slabs, 8) * count * (width // 128)


def on_device(
    slabs, crosses,
    populations, fluid_mask, relaxation, positions, triangles, tension, coarse_moments, interface,
):
    _, plane_count, columns, rows = populations.shape
    _, membranes, nodes = positions.shape
    padded = round_up(nodes, 128)
    corners = triangles.shape[1]
    half, planes = (columns + 6) // 2, plane_count + 2
    cells = round_up(planes * half, 16)
    flat = (columns + 2 * HALO + 2) * (plane_count + 2 * HALO)
    vmem = pl.BlockSpec(memory_space=pltpu.VMEM)
    block = (19, plane_count, columns, rows)
    operands = (
        triangles, populations, relaxation, fluid_mask, positions, tension, coarse_moments, interface,
    )
    fields = pl.pallas_call(
        functools.partial(lattice_kernel, slabs, crosses),
        name="lattice_steps",
        out_shape=pltpu.VMEM(block, F32),
        in_specs=[pl.BlockSpec(memory_space=pl.ANY)] * 8,
        out_specs=vmem,
        scratch_shapes=[pltpu.VMEM(operand.shape, operand.dtype) for operand in operands]
        + [
            pltpu.VMEM((3, membranes, padded), F32),
            pltpu.VMEM((padded, corners), BF16),
            pltpu.VMEM((3, membranes, padded), F32),
            pltpu.VMEM((membranes, padded), I32),
            pltpu.VMEM((membranes, padded), I32),
            pltpu.VMEM((6 * cells, 2 * rows), F32),
            pltpu.VMEM((3, half * planes + cells, rows), F32),
            pltpu.VMEM((3, (columns + 4) * planes + 16, rows), F32),
            pltpu.VMEM((CHANNELS, flat, rows), F32),
            pltpu.VMEM((3, flat, rows), F32),
            pltpu.VMEM((3, flat, rows), F32),
            pltpu.VMEM((3, flat, rows), F32),
            pltpu.VMEM((5, flat, rows), F32),
            pltpu.VMEM((19, flat, rows), F32),
            pltpu.VMEM((19, flat, rows), F32),
            pltpu.VMEM((19, flat, rows), F32),
            pltpu.VMEM((19, flat, rows), F32),
            pltpu.VMEM((slabs,) + coarse_moments.shape, F32),
            pltpu.VMEM((coarse_rows(slabs, coarse_moments), 128), F32),
            pltpu.VMEM((8,) + interface.shape, I32),
        ]
        + [
            pltpu.VMEM(shape, F32)
            for moves in (MOVES, MOVES, RAW_MOVES, RAW_MOVES)
            for shape in buffer_shapes(moves, plane_count, columns, rows)
        ]
        + [
            pltpu.SemaphoreType.DMA((8,)),
            pltpu.SemaphoreType.DMA((2, slabs)),
            pltpu.SemaphoreType.DMA((2, 8)),
            pltpu.SemaphoreType.DMA((2, 6)),
            pltpu.SemaphoreType.DMA((2, 8)),
            pltpu.SemaphoreType.DMA((2, 8)),
        ],
        compiler_params=pltpu.CompilerParams(collective_id=0, has_side_effects=True),
    )(*operands)
    return pl.pallas_call(
        flow_kernel,
        name="flow",
        out_shape=(
            jax.ShapeDtypeStruct(block, F32),
            jax.ShapeDtypeStruct((3,) + block[1:], F32),
        ),
        in_specs=[vmem],
        out_specs=(pl.BlockSpec(memory_space=pl.ANY),) * 2,
        scratch_shapes=[pltpu.VMEM((3,) + block[1:], F32), pltpu.SemaphoreType.DMA((2,))],
    )(pltpu.with_memory_space_constraint(fields, pltpu.VMEM))


def solution(mesh):
    in_specs = (
        P(None, "slab", "cross", None),
        P("slab", "cross", None),
        P("slab", "cross", None),
        P(None, "slab", None),
        P(),
        P("slab", None),
        P(None, "slab"),
        P(None, ("slab", "cross")),
    )
    out_specs = (P(None, "slab", "cross", None), P(None, "slab", "cross", None))
    return jax.shard_map(
        functools.partial(on_device, mesh.shape["slab"], mesh.shape["cross"]),
        mesh=mesh, in_specs=in_specs, out_specs=out_specs, check_vma=False,
    )
```
